128 devices in a mesh: gx: 16 (over x, z), gy: 8 (over y, core).
Axes of the slice: x: 4, y: 4, z: 4, core: 2. Of those that a mesh axis runs over, the one named last changes fastest.
Arguments:
- velocity: float32 [3, 256, 256, 256], P(None, 'gx', 'gy'), may hold values from -6 to 6
- owner_block: int32 [262144, 1], P(('gx', 'gy')), may hold values from 0 to 127, as said below
- base_x: int32 [262144], P(('gx', 'gy')), may hold values from 0 to 16
- base_y: int32 [262144], P(('gx', 'gy')), may hold values from 0 to 32
- base_z: int32 [262144], P(('gx', 'gy')), may hold values from 0 to 255
- delta_weights: float32 [12, 262144], P(None, ('gx', 'gy')), may hold values from 0.1 to 1
- marker_offset: float32 [3, 262144], P(None, ('gx', 'gy')), may hold values from -4 to 4
- sphere_motion: float32 [6, 256], P(None, ('gx', 'gy')), may hold values from -6 to 6
- contact_sphere: int32 [512], P(('gx', 'gy')), may hold values from 0 to 255, as said below
- contact_partner: int32 [512], P(('gx', 'gy')), may hold values from 0 to 255
Outputs:
- velocity_star: float32 [3, 256, 256, 256], P(None, 'gx', 'gy')
- new_motion: float32 [6, 256], P(None, ('gx', 'gy'))
The draws below stay inside these ranges and needn't reach their ends.
Inputs may be any that keep to these rules, and one draw needn't show every extreme that they name: `owner_block`: block b stands at gx index b // 8 and gy index b % 8. Each marker's owner block is the block of the device that holds the marker or one of the eight blocks beside it (periodic along gx, none beyond the walls along gy). Among the markers of one device, at most 256 have any one owner block other than that device's own, and in every device exactly 256 have one such block. `contact_sphere`: entry k names one of the 2 spheres k // 4 * 2 and after, those of the device that holds entry k.
All inputs are finite; a program needn't handle non-finite values.
Results may differ from the reference program's by a relative error of at most 0.0003.
Values sent between devices are 32-bit elements; how exact they have to be, the bound alone decides.
No kernel may reach another device: no remote copies, remote signals or barrier semaphores. Data moves between devices by JAX's collectives and lax.ppermute only.
A program may use at most 64 MiB of HBM per device.

```python
import math
import jax
import jax.numpy as jnp
from jax import lax

CX = 16
CY = 32
NZ = 256
MK = 1024
S_DEV = 2
CT_DEV = 4
ITERS = 4
NX = 256
NY = 256
SPHERES = 256
MARKERS = 262144
CAP = 256
CONTACTS = 512
N_GX = 16
N_GY = 8


def draw_contact_sphere(key, part):
    entries = jnp.arange(CONTACTS, dtype=jnp.int32)
    picked = jax.random.randint(key, (CONTACTS,), 0, S_DEV, dtype=jnp.int32)
    return entries // CT_DEV * S_DEV + picked


def draw_owner_block(key, part):
    per_device = S_DEV * MK
    devices = N_GX * N_GY
    device = jnp.arange(devices, dtype=jnp.int32)
    column = device // N_GY
    row = device % N_GY
    shift_x = jnp.array([-1, -1, -1, 0, 0, 1, 1, 1], dtype=jnp.int32)
    shift_y = jnp.array([-1, 0, 1, -1, 1, -1, 0, 1], dtype=jnp.int32)
    counts = jax.random.randint(jax.random.fold_in(key, 11), (devices, 8), 1, CAP + 1, dtype=jnp.int32)
    coin = jax.random.randint(jax.random.fold_in(key, 12), (devices,), 0, 2, dtype=jnp.int32)
    full_lane = jnp.where(coin == 0, 1, 6).astype(jnp.int32)
    counts = jnp.where(jnp.arange(8, dtype=jnp.int32)[None, :] == full_lane[:, None], CAP, counts)
    device_keys = jax.random.split(jax.random.fold_in(key, 13), devices)
    position = jax.vmap(lambda one_key: jax.random.permutation(one_key, per_device))(device_keys).astype(jnp.int32)
    lane = jnp.minimum(position // CAP, 7)
    within = position % CAP
    count_here = jnp.take_along_axis(counts, lane, axis=1)
    away = within < count_here
    towards_x = (column[:, None] + shift_x[lane]) % N_GX
    towards_y = row[:, None] + shift_y[lane]
    inside = jnp.logical_and(towards_y >= 0, towards_y < N_GY)
    chosen = jnp.where(jnp.logical_and(away, inside), towards_x * N_GY + towards_y, device[:, None])
    return chosen.reshape(MARKERS, 1).astype(jnp.int32)


def plant(values, stream_key, low, largest):
    shape = values.shape
    index_at = [jax.random.randint(jax.random.fold_in(stream_key, axis), (), 0, shape[axis]) for axis in range(len(shape))]
    values = values.at[tuple(index_at)].set(low)
    longest = shape.index(max(shape))
    index_at[longest] = (index_at[longest] + 1) % shape[longest]
    return values.at[tuple(index_at)].set(largest)


def block_levels(key, extent, shards, smallest, high):
    gain = 1.0
    for axis_at, shards_of in shards:
        heights = jax.random.uniform(jax.random.fold_in(jax.random.fold_in(key, 6), axis_at), (shards_of,), jnp.float32, smallest / len(shards), high / len(shards))
        gain = gain * jnp.repeat(jnp.exp(heights), extent[axis_at] // shards_of).reshape((-1,) + (1,) * (len(extent) - 1 - axis_at))
    return gain


def noise(rng, dims, scale, limit, cuts=(), held_as=jnp.bfloat16):
    level = block_levels(rng, dims, cuts, -0.22, 0.18) if cuts else 1.0
    result = jax.random.normal(rng, dims, jnp.float32) * scale * level
    return jnp.minimum(jnp.maximum(result, -limit), limit).astype(held_as)


def setup_inputs(seed: int = 0) -> dict:
    seeds = jax.random.split(jax.random.key(seed), 11)
    return {
        "velocity": noise(seeds[0], (3, NX, NY, NZ), 1.0, 6.0, ((1, 16), (2, 8)), jnp.float32),
        "owner_block": draw_owner_block(jax.random.fold_in(seeds[10], 71), 0),
        "base_x": plant(jax.random.randint(seeds[2], (MARKERS,), 0, CX + 1), jax.random.fold_in(seeds[2], 1), 0, CX).astype(jnp.int32),
        "base_y": plant(jax.random.randint(seeds[3], (MARKERS,), 0, CY + 1), jax.random.fold_in(seeds[3], 1), 0, CY).astype(jnp.int32),
        "base_z": plant(jax.random.randint(seeds[4], (MARKERS,), 0, NZ), jax.random.fold_in(seeds[4], 1), 0, NZ - 1).astype(jnp.int32),
        "delta_weights": jnp.clip(jnp.exp(math.log(1.0) - 2.3025851 * jax.random.uniform(seeds[5], (12, MARKERS), jnp.float32) ** block_levels(seeds[5], (12, MARKERS), ((1, 128),), -0.2, 0.2)), 0.1, 1.0),
        "marker_offset": noise(seeds[6], (3, MARKERS), 1.0, 4.0, ((1, 128),), jnp.float32),
        "sphere_motion": noise(seeds[7], (6, SPHERES), 1.0, 6.0, ((1, 128),), jnp.float32),
        "contact_sphere": draw_contact_sphere(jax.random.fold_in(seeds[10], 71), 0),
        "contact_partner": plant(jax.random.randint(seeds[9], (CONTACTS,), 0, SPHERES), jax.random.fold_in(seeds[9], 1), 0, SPHERES - 1).astype(jnp.int32),
    }


DIFFUSION = 1.0
RESPONSE = 0.5
DASHPOT = 0.1


def support(start_x, start_y, start_z, weights, stride_y, extent_z):
    offsets = jnp.arange(4, dtype=jnp.int32)
    cells_x = start_x[None, :] + offsets[:, None]
    cells_y = start_y[None, :] + offsets[:, None]
    cells_z = (start_z[None, :] + offsets[:, None]) % extent_z
    where = ((cells_x[:, None, None, :] * stride_y + cells_y[None, :, None, :]) * extent_z + cells_z[None, None, :, :]).reshape(64, -1)
    product = (weights[0:4][:, None, None, :] * weights[4:8][None, :, None, :] * weights[8:12][None, None, :, :]).reshape(64, -1)
    return where, product


def reference(velocity, owner_block, base_x, base_y, base_z, delta_weights, marker_offset, sphere_motion, contact_sphere, contact_partner):
    padded = jnp.pad(velocity, ((0, 0), (2, 2), (0, 0), (0, 0)), mode="wrap")
    padded = jnp.pad(padded, ((0, 0), (0, 0), (2, 2), (0, 0)))
    flat_field = padded.reshape(3, -1)
    owner = owner_block[:, 0]
    start_x = (owner // N_GY) * CX + base_x
    start_y = (owner % N_GY) * CY + base_y
    linear = sphere_motion[0:3]
    angular = sphere_motion[3:6]
    marker_linear = jnp.repeat(linear, MK, axis=1)
    marker_angular = jnp.repeat(angular, MK, axis=1)
    target = marker_linear + jnp.cross(marker_angular, marker_offset, axis=0)
    block_x = start_x.reshape(SPHERES, MK)
    block_y = start_y.reshape(SPHERES, MK)
    block_z = base_z.reshape(SPHERES, MK)
    block_w = delta_weights.reshape(12, SPHERES, MK).transpose(1, 0, 2)
    block_t = target.reshape(3, SPHERES, MK).transpose(1, 0, 2)

    def sample(item):
        where, product = support(item[0], item[1], item[2], item[3], NY + 4, NZ)
        picked = flat_field[:, where]
        return jnp.sum(picked * product[None], axis=1)

    sampled = lax.map(sample, (block_x, block_y, block_z, block_w))
    block_force = block_t - sampled
    force = block_force.transpose(1, 0, 2).reshape(3, MARKERS)
    push = jnp.sum(block_force, axis=-1).T / MK
    twist = jnp.sum(jnp.cross(marker_offset, force, axis=0).reshape(3, SPHERES, MK), axis=-1) / MK
    moved = linear - RESPONSE * push
    turned = angular - RESPONSE * twist
    spring = moved[:, contact_partner] - moved[:, contact_sphere]
    settled = moved + DASHPOT * jax.ops.segment_sum(spring.T, contact_sphere, SPHERES).T
    new_motion = jnp.concatenate([settled, turned], axis=0)

    def deposit(field, item):
        where, product = support(item[0], item[1], item[2], item[3], NY + 4, NZ)
        return field.at[:, where.reshape(-1)].add((product[None] * item[4][:, None, :]).reshape(3, -1)), None

    spread, unused = lax.scan(deposit, jnp.zeros_like(flat_field), (block_x, block_y, block_z, block_w, block_force))
    spread = spread.reshape(padded.shape)
    folded = spread[:, 2:NX + 2]
    folded = folded.at[:, 0:2].add(spread[:, NX + 2:NX + 4])
    folded = folded.at[:, NX - 2:NX].add(spread[:, 0:2])
    source = folded[:, :, 2:NY + 2]
    rhs = velocity + source
    state = rhs
    for sweep in range(ITERS):
        walled = jnp.pad(state, ((0, 0), (0, 0), (1, 1), (0, 0)))
        beside_all = jnp.roll(state, -1, 1) + jnp.roll(state, 1, 1) + walled[:, :, 2:] + walled[:, :, :-2]
        beside_all = beside_all + jnp.roll(state, -1, 3) + jnp.roll(state, 1, 3)
        state = (rhs + DIFFUSION * beside_all) / (1.0 + 6.0 * DIFFUSION)
    return state, new_motion
```

```python
import functools

import jax
import jax.numpy as jnp
from jax import lax
from jax.experimental import pallas as pl
from jax.experimental.pallas import tpu as pltpu
from jax.sharding import PartitionSpec as P

F32 = jnp.float32
BF16 = jnp.bfloat16
I32 = jnp.int32

ITERS = 4
DIFFUSION = 1.0
RESPONSE = 0.5
DASHPOT = 0.1

ROWS = 24
TILE = 256
WIN = 8
CYR = 112


TRAVEL = ((0, 0), (-1, 0), (1, 0), (-1, -1), (0, -1), (1, -1), (-1, 1), (0, 1), (1, 1))

VMEM = pl.BlockSpec(memory_space=pltpu.VMEM)
SMEM = pl.BlockSpec(memory_space=pltpu.SMEM)
HBM = pl.BlockSpec(memory_space=pltpu.HBM)


def params(mib):
    return pltpu.CompilerParams(vmem_limit_bytes=mib * 1024 * 1024)


def split(value):
    high = value.astype(BF16)
    low = (value - high.astype(F32)).astype(BF16)
    return high, low


def counting_ranks(bin_of, start_of, bins_here):
    markers = bin_of.shape[1]
    bins = (lax.broadcasted_iota(I32, (32, markers), 0) == bin_of).astype(F32)
    bins16 = bins.astype(BF16)
    ramp_i = lax.broadcasted_iota(I32, (TILE, TILE), 0)
    ramp_j = lax.broadcasted_iota(I32, (TILE, TILE), 1)
    upper = (ramp_i < ramp_j).astype(F32).astype(BF16)
    totals = lax.dot_general(
        jnp.ones((8, markers), BF16), bins16, (((1,), (1,)), ((), ())), preferred_element_type=F32
    )
    row = lax.broadcasted_iota(I32, (32, 32), 0)
    col = lax.broadcasted_iota(I32, (32, 32), 1)
    before = jnp.where(jnp.logical_and(col < row, row < bins_here), totals[0:1, :], 0.0)
    bin_row = lax.broadcasted_iota(I32, (32, 1), 0)
    start = jnp.where(
        bin_row < bins_here, jnp.sum(before, axis=1, keepdims=True), start_of(bin_row).astype(F32)
    )
    slots = []
    for b in range(markers // TILE):
        mine = bins[:, b * TILE : (b + 1) * TILE]
        ranks = jnp.dot(bins16[:, b * TILE : (b + 1) * TILE], upper, preferred_element_type=F32)
        slots.append(jnp.sum(mine * (ranks + start), axis=0, keepdims=True))
        start = start + jnp.sum(mine, axis=1, keepdims=True)
    return jnp.concatenate(slots, axis=1).astype(I32)


def gather_tile(both, slot, tile):
    place = lax.broadcasted_iota(I32, (TILE, slot.shape[1]), 0)
    pick = (slot - tile * TILE == place).astype(F32).astype(BF16)
    out = lax.dot_general(both, pick, (((1,), (1,)), ((), ())), preferred_element_type=F32)
    return out[0:ROWS] + out[ROWS : 2 * ROWS]


def halves(value):
    high, low = split(value)
    return jnp.concatenate([high.astype(F32), low.astype(F32)], axis=0).astype(BF16)


def route_kernel(
    where, motion, owner_h, bx_h, by_h, bz_h, weights_h, offset_h, velocity_h,
    to_left, to_right, middle, to_down, to_up, slot_out, both_out, linear,
    owner, bx, by, bz, weights, offset, vel, rec, sems, edge_sem, *, gx, gy_shift
):
    markers = owner.shape[1]
    blocks = markers // TILE
    nx, ny = vel.shape[1:3]
    moves = []
    for k, (src, dst) in enumerate(
        ((owner_h, owner), (bx_h, bx), (by_h, by), (bz_h, bz), (weights_h, weights), (offset_h, offset))
    ):
        move = pltpu.make_async_copy(src, dst, sems.at[k])
        move.start()
        moves.append(move)
    whole = pltpu.make_async_copy(velocity_h, vel, edge_sem.at[0])
    whole.start()
    for move in moves:
        move.wait()
    own = owner[...]
    step_x = (lax.shift_right_logical(own, gy_shift) - where[0] + 1) & (gx - 1)
    step_y = (own & ((1 << gy_shift) - 1)) - where[1] + 1
    lane = step_x * 3 + step_y
    bin_of = jnp.where(lane == 4, bx[...], 17 + lane)
    slot = counting_ranks(bin_of, lambda b: markers + (b - 17) * TILE, 17)
    slot_out[...] = slot

    first = lax.broadcasted_iota(I32, (1, markers), 1) < markers // 2
    speed = [jnp.where(first, motion[0, c], motion[1, c]) for c in range(6)]
    off = [offset[c : c + 1, :] for c in range(3)]
    target = [
        speed[0] + (speed[4] * off[2] - speed[5] * off[1]),
        speed[1] + (speed[5] * off[0] - speed[3] * off[2]),
        speed[2] + (speed[3] * off[1] - speed[4] * off[0]),
    ]
    rec[0:12, :] = weights[...]
    rec[12:13, :] = bx[...].astype(F32)
    rec[13:14, :] = by[...].astype(F32)
    rec[14:15, :] = bz[...].astype(F32)
    for c in range(3):
        rec[15 + c : 16 + c, :] = target[c]
    rec[18:21, :] = offset[...]
    rec[21:22, :] = jnp.where(first, 0.0, 1.0)
    rec[22:23, :] = jnp.ones((1, markers), F32)
    rec[23:24, :] = jnp.zeros((1, markers), F32)
    both = halves(rec[...])
    both_out[...] = both
    base = 6 * ny
    for k in range(3):
        to_left[base + k * ROWS : base + (k + 1) * ROWS, :] = gather_tile(both, slot, blocks + k)
        to_right[base + k * ROWS : base + (k + 1) * ROWS, :] = gather_tile(both, slot, blocks + 6 + k)
    middle[0] = gather_tile(both, slot, blocks + 3)
    middle[1] = gather_tile(both, slot, blocks + 5)

    lane_row = lax.broadcasted_iota(I32, (1, 128), 1)
    line = jnp.zeros((1, 128), F32)
    for s in range(2):
        for c in range(3):
            line = jnp.where(lane_row == 108 + 6 * s + c, motion[s, c], line)
    linear[...] = line
    whole.wait()
    for c in range(3):
        for x in range(2):
            rows = pl.ds((c * 2 + x) * ny, ny)
            to_left[rows, :] = vel[c, x]
            to_right[rows, :] = vel[c, nx - 2 + x]

    for x in range(nx):
        for c in range(3):
            at = (x + 2) * 6 + c * 2
            to_down[at : at + 2, :] = vel[c, x, 0:2, :]
            to_up[at : at + 2, :] = vel[c, x, ny - 2 : ny, :]


def home_kernel(slot, both, home):
    count = jnp.sum((slot[...] < slot.shape[1]).astype(F32)).astype(I32)
    for t in range(home.shape[0]):
        home[t] = jnp.zeros((ROWS, TILE), F32)

    def tile(t, carry):
        home[t] = gather_tile(both[...], slot[...], t)
        return carry

    lax.fori_loop(0, (count + TILE - 1) // TILE, tile, 0)


def turn_kernel(got_left, got_right, middle, own_down, own_up, to_down, to_up, *, nx, ny):
    base = 6 * ny
    lists = (nx + 4) * 6
    for out, own, cut, pick, mid in (
        (to_down, own_down, 0, 0, 0),
        (to_up, own_up, ny - 2, 2, 1),
    ):
        out[0:lists, :] = own[0:lists, :]
        for x in range(2):
            for c in range(3):
                at = (c * 2 + x) * ny + cut
                to = x * 6 + c * 2
                out[to : to + 2, :] = got_right[at : at + 2, :]
                to = (nx + 2 + x) * 6 + c * 2
                out[to : to + 2, :] = got_left[at : at + 2, :]
        out[lists : lists + ROWS, :] = got_left[base + pick * ROWS : base + (pick + 1) * ROWS, :]
        out[lists + ROWS : lists + 2 * ROWS, :] = middle[mid]
        out[lists + 2 * ROWS : lists + 3 * ROWS, :] = (
            got_right[base + pick * ROWS : base + (pick + 1) * ROWS, :]
        )


def chain(distance, rows):
    value = jnp.where(distance == 3, rows[3], 0.0)
    for k in (2, 1, 0):
        value = jnp.where(distance == k, rows[k], value)
    return value


def couple_kernel(
    vel, got_left, got_right, got_down, got_up, home, linear,
    part, send_l, send_r, message,
    fcat, lists, arrived, tn, tt, sacc, scat, sums,
):
    nx = vel.shape[1] + 4
    cells = vel.shape[2]
    tall = cells + 4
    zero_pad = jnp.zeros((CYR - 3 * tall, vel.shape[3]), F32)

    def fill_own(x, carry):
        for c in range(3):
            part[x + 2, c * tall + 2 : c * tall + 2 + cells, :] = vel[c, x]
        return carry

    lax.fori_loop(0, nx - 4, fill_own, 0)
    for x in range(2):
        for c in range(3):
            rows = pl.ds((c * 2 + x) * cells, cells)
            part[x, c * tall + 2 : c * tall + 2 + cells, :] = got_right[rows, :]
            part[nx - 2 + x, c * tall + 2 : c * tall + 2 + cells, :] = got_left[rows, :]

    zero2 = jnp.zeros((2, vel.shape[3]), F32)
    for x in range(nx):
        for c in range(3):
            rows = pl.ds(x * 6 + c * 2, 2)
            part[x, c * tall : c * tall + 2, :] = got_up[rows, :]
            part[x, c * tall + 2 + cells : (c + 1) * tall, :] = got_down[rows, :]
        part[x, 3 * tall : CYR, :] = zero_pad

    def fill_rest(x, carry):
        high, low = split(part[x])
        fcat[x, :, 0:256] = high
        fcat[x, :, 256:512] = low
        fcat[x, :, 512:768] = high
        for c in range(3):
            part[x, c * tall : c * tall + 2, :] = zero2
            part[x, c * tall + 2 + cells : (c + 1) * tall, :] = zero2
        return carry

    lax.fori_loop(0, nx, fill_rest, 0)
    for x in (0, 1, nx - 2, nx - 1):
        part[x] = jnp.zeros((CYR, vel.shape[3]), F32)

    base = 6 * cells + ROWS
    after = nx * 6
    arrived[:, 0:TILE] = got_left[base : base + ROWS, :]
    arrived[:, TILE : 2 * TILE] = got_right[base : base + ROWS, :]
    for k in range(3):
        rows = pl.ds(after + k * ROWS, ROWS)
        arrived[:, (2 + k) * TILE : (3 + k) * TILE] = got_down[rows, :]
        arrived[:, (5 + k) * TILE : (6 + k) * TILE] = got_up[rows, :]
    total_lanes = arrived.shape[1]
    lane_at = lax.broadcasted_iota(I32, (1, total_lanes), 1)
    arrived[23:24, :] = (1 + lax.shift_right_logical(lane_at, 8)).astype(F32)
    valid_all = arrived[22:23, :] > 0.5
    count = jnp.sum(arrived[22:23, :]).astype(I32)
    bin_all = jnp.where(valid_all, arrived[12:13, :].astype(I32), 17)
    slot = counting_ranks(bin_all, lambda b: 0 * b + total_lanes, 17)
    both = halves(arrived[...])
    blocks = home.shape[0]
    for t in range(blocks):
        lists[t] = home[t]
        lists[blocks + t] = jnp.zeros((ROWS, TILE), F32)

    def gather_one(t, carry):
        lists[blocks + t] = gather_tile(both, slot, t)
        return carry

    lax.fori_loop(0, (count + TILE - 1) // TILE, gather_one, 0)
    sums[...] = jnp.zeros(sums.shape, F32)

    row = lax.broadcasted_iota(I32, (CYR, 1), 0)
    comp = (row >= tall).astype(I32) + (row >= 2 * tall).astype(I32)
    y_of = jnp.where(row < 3 * tall, row - comp * tall, -100)
    comp = jnp.where(row < 3 * tall, comp, 3)
    z_of = lax.broadcasted_iota(I32, (256, TILE), 0)
    win_row = lax.broadcasted_iota(I32, (WIN, TILE), 0)
    group_of = lax.broadcasted_iota(I32, (128, TILE), 0)

    def tile_body(t, carry):
        rec = lists[t]
        valid = rec[22:23] > 0.5
        bxf = rec[12:13]
        x_first = jnp.min(jnp.where(valid, bxf, 99.0)).astype(I32)
        x_last = jnp.max(jnp.where(valid, bxf, -9.0)).astype(I32)
        windows = jnp.where(x_last < 0, 0, (x_last - x_first + 4 + WIN - 1) // WIN)

        @pl.when(windows > 0)
        def _():
            bxi = bxf.astype(I32)
            byi = rec[13:14].astype(I32)
            bzi = rec[14:15].astype(I32)
            table_z = chain((z_of - bzi) & 255, [rec[8 + k : 9 + k] for k in range(4)])
            high, low = split(table_z)
            tn[0:256, :] = high
            tn[256:512, :] = high
            tn[512:768, :] = low
            tt[:, 0:256] = high
            tt[:, 256:512] = high
            tt[:, 512:768] = low
            table_y = chain(y_of - byi, [rec[4 + k : 5 + k] for k in range(4)])
            sacc[...] = jnp.zeros(sacc.shape, F32)

            def window(w):
                begin = x_first + w * WIN
                x0 = jnp.minimum(begin, nx - WIN)
                x_at = win_row + x0
                table_x = chain(x_at - bxi, [rec[k : k + 1] for k in range(4)])
                return x0, jnp.where(x_at >= begin, table_x, 0.0)

            def sample(w, c):
                x0, table_x = window(w)
                block = fcat[pl.ds(x0, WIN)].reshape(WIN * CYR, 768)
                got = jnp.dot(block, tn[...], preferred_element_type=F32)
                total = sacc[...]
                for i in range(WIN):
                    total = total + table_x[i : i + 1] * got[i * CYR : (i + 1) * CYR]
                sacc[...] = total
                return c

            lax.fori_loop(0, windows, sample, 0)
            weighted = sacc[...] * table_y
            force = [
                rec[15 + c : 16 + c]
                - jnp.sum(jnp.where(comp == c, weighted, 0.0), axis=0, keepdims=True)
                for c in range(3)
            ]
            by_row = jnp.where(comp == 0, force[0], jnp.where(comp == 1, force[1], force[2]))
            plane = table_y * by_row

            def deposit(w, c):
                x0, table_x = window(w)
                for i in range(WIN):
                    hi, lo = split(table_x[i : i + 1] * plane)
                    scat[i, :, 0:256] = hi
                    scat[i, :, 256:512] = lo
                    scat[i, :, 512:768] = hi
                made = lax.dot_general(
                    scat[...].reshape(WIN * CYR, 768),
                    tt[...],
                    (((1,), (1,)), ((), ())),
                    preferred_element_type=F32,
                )
                part[pl.ds(x0, WIN)] += made.reshape(WIN, CYR, 256)
                return c

            lax.fori_loop(0, windows, deposit, 0)
            off = [rec[18 + c : 19 + c] for c in range(3)]
            turn = [
                off[1] * force[2] - off[2] * force[1],
                off[2] * force[0] - off[0] * force[2],
                off[0] * force[1] - off[1] * force[0],
            ]
            stack = jnp.concatenate(force + turn + [jnp.zeros((2, TILE), F32)], axis=0)
            group = (2.0 * rec[23:24] + rec[21:22]).astype(I32)
            member = (group_of == group).astype(F32).astype(BF16)
            found = lax.dot_general(
                member, halves(stack), (((1,), (1,)), ((), ())), preferred_element_type=F32
            )
            sums[:, 0:16] += found

        return carry

    lax.fori_loop(0, 2 * blocks, tile_body, 0)
    lane_of = lax.broadcasted_iota(I32, (128, 128), 1)
    low_part = pltpu.roll(sums[...], 120, axis=1)
    joined = jnp.where(lane_of < 6, sums[...] + low_part, 0.0)
    line = linear[...] + joined[0:1]
    for k in range(1, 18):
        line = line + pltpu.roll(joined[k : k + 1], 6 * k, axis=1)
    message[...] = jnp.broadcast_to(line, message.shape)
    for x in range(6):
        send_l[x] = part[x]
        send_r[x] = part[nx - 6 + x]


def motion(where, contact_own, contact_other, got, out, moved, *, gx, gy, per_sphere):
    here = where[0] * gy + where[1]
    data = got[...]
    total = jnp.zeros(data.shape, F32)
    devices = gx * gy
    for k, (dx, dy) in enumerate(TRAVEL):
        piece = data
        shift = (-(gy * dx + dy)) % devices
        if shift:
            piece = pltpu.roll(piece, shift, axis=0)
        if k:
            piece = pltpu.roll(piece, 128 - 12 * k, axis=1)
        total = total + piece
    linear = pltpu.roll(data, 128 - 108, axis=1)
    moved[...] = linear - (RESPONSE / per_sphere) * total
    lane = lax.broadcasted_iota(I32, (1, 128), 1)
    mine = moved[pl.ds(here, 1), :]
    spring = jnp.zeros((1, 128), F32)
    for k in range(contact_own.shape[0]):
        partner = contact_other[k]
        line = moved[pl.ds(lax.shift_right_logical(partner, 1), 1), :]
        local = contact_own[k] - here * 2
        which = partner & 1
        same = jnp.where(which == local, line, 0.0)
        higher = jnp.where(which < local, pltpu.roll(line, 6, axis=1), 0.0)
        lower = jnp.where(which > local, pltpu.roll(line, 122, axis=1), 0.0)
        of_own = jnp.logical_and(lane >= local * 6, lane < local * 6 + 3)
        spring = spring + jnp.where(of_own, same + higher + lower - mine, 0.0)
    out[...] = mine + DASHPOT * spring


def edges_kernel(
    where, contact_own, contact_other, got, part, got_l, got_r, low, high, line, moved,
    *, tall, gx, gy, per_sphere
):
    motion(where, contact_own, contact_other, got, line, moved, gx=gx, gy=gy, per_sphere=per_sphere)
    nx = part.shape[0]
    for x in range(nx + 4):
        for c in range(3):
            for ref, at in ((low, c * tall), (high, (c + 1) * tall - 6)):
                rows = pl.ds(at, 6)
                pieces = []
                if 2 <= x < nx + 2:
                    pieces.append(part[x - 2, rows, :])
                if x < 6:
                    pieces.append(got_l[x, rows, :])
                if x >= nx - 2:
                    pieces.append(got_r[x - (nx - 2), rows, :])
                total = pieces[0]
                for piece in pieces[1:]:
                    total = total + piece
                ref[x * 18 + c * 6 : x * 18 + c * 6 + 6, :] = total


def relax_kernel(where, part, got_l, got_r, low, high, out, rhs, va, vb, *, tall, rows):
    nx = part.shape[0]
    long = nx + 4
    high_y = tall + 4
    y_at = lax.broadcasted_iota(I32, (high_y, 1), 0) - 4 + where[1] * (tall - 4)
    inside = jnp.logical_and(y_at >= 0, y_at < rows)
    mask = jnp.broadcast_to(inside.astype(F32), (high_y, 256))
    factor = jnp.broadcast_to(
        jnp.where(inside, 1.0 / (1.0 + 6.0 * DIFFUSION), 0.0), (high_y, 256)
    )
    zero2 = jnp.zeros((2, 256), F32)

    def fill(x, sources):
        for c in range(3):
            rows_of = pl.ds(c * tall, tall)
            total = sources[0][0][sources[0][1], rows_of, :]
            for ref, at in sources[1:]:
                total = total + ref[at, rows_of, :]
            rhs[c, x, 0:2, :] = zero2
            rhs[c, x, high_y - 2 : high_y, :] = zero2
            rhs[c, x, 2 : 2 + tall, :] = total

    for x in range(6):
        fill(x, [(got_l, x)] + ([(part, x - 2)] if x >= 2 else []))
        fill(long - 6 + x, [(got_r, x)] + ([(part, nx - 4 + x)] if x < 4 else []))

    def middle(x, carry):
        fill(x, [(part, x - 2)])
        return carry

    lax.fori_loop(6, long - 6, middle, 0)
    for x in range(long):
        for c in range(3):
            at = pl.ds(x * 18 + c * 6, 6)
            rhs[c, x, 0:6, :] += low[at, :]
            rhs[c, x, high_y - 6 : high_y, :] += high[at, :]

    def finish(x, carry):
        for c in range(3):
            rhs[c, x] = rhs[c, x] * mask
        return carry

    lax.fori_loop(0, long, finish, 0)

    state = rhs
    for sweep in range(ITERS):
        target = (va, vb)[sweep % 2]
        last = sweep == ITERS - 1

        def layer(x, carry, state=state, target=target, last=last):
            for c in range(3):
                here = state[c, x]
                near = state[c, x - 1] + state[c, x + 1]
                near = near + (pltpu.roll(here, 1, axis=1) + pltpu.roll(here, 255, axis=1))
                near = near + (pltpu.roll(here, 1, axis=0) + pltpu.roll(here, high_y - 1, axis=0))
                new = (rhs[c, x] + DIFFUSION * near) * factor
                if last:
                    out[c, x - 4] = new[4 : high_y - 4]
                else:
                    target[c, x] = new
            return carry

        lax.fori_loop(sweep + 1, long - 1 - sweep, layer, 0, unroll=2)
        state = target


def on_device(
    velocity,
    owner_block,
    base_x,
    base_y,
    base_z,
    delta_weights,
    marker_offset,
    sphere_motion,
    contact_sphere,
    contact_partner,
):
    nx, ny, nz = velocity.shape[1:]
    gx = lax.axis_size("gx")
    gy = lax.axis_size("gy")
    where = jnp.stack([lax.axis_index("gx"), lax.axis_index("gy")]).astype(I32)
    markers = base_x.shape[0]
    spheres = sphere_motion.shape[1]
    per_sphere = markers // spheres
    blocks = markers // TILE
    tall = ny + 4
    x_up = [(i, (i + 1) % gx) for i in range(gx)]
    x_down = [(j, i) for i, j in x_up]
    y_up = [(i, i + 1) for i in range(gy - 1)]
    y_down = [(j, i) for i, j in y_up]

    def array(*shape, dtype=F32):
        return jax.ShapeDtypeStruct(shape, dtype)

    x_rows = 6 * ny + 3 * ROWS
    y_rows = 6 * (nx + 4) + 3 * ROWS
    to_left, to_right, middle, own_down, own_up, slot, both, linear = pl.pallas_call(
        functools.partial(route_kernel, gx=gx, gy_shift=gy.bit_length() - 1),
        out_shape=(
            array(x_rows, nz),
            array(x_rows, nz),
            array(2, ROWS, TILE),
            array(y_rows, nz),
            array(y_rows, nz),
            array(1, markers, dtype=I32),
            array(2 * ROWS, markers, dtype=BF16),
            array(1, 128),
        ),
        in_specs=[SMEM, SMEM] + [HBM] * 7,
        out_specs=(VMEM,) * 8,
        scratch_shapes=[
            pltpu.VMEM((1, markers), I32),
            pltpu.VMEM((1, markers), I32),
            pltpu.VMEM((1, markers), I32),
            pltpu.VMEM((1, markers), I32),
            pltpu.VMEM((12, markers), F32),
            pltpu.VMEM((3, markers), F32),
            pltpu.VMEM((3, nx, ny, nz), F32),
            pltpu.VMEM((ROWS, markers), F32),
            pltpu.SemaphoreType.DMA((6,)),
            pltpu.SemaphoreType.DMA((1,)),
        ],
        compiler_params=params(16),
        name="route",
    )(
        where,
        sphere_motion.T,
        owner_block.reshape(1, markers),
        base_x.reshape(1, markers),
        base_y.reshape(1, markers),
        base_z.reshape(1, markers),
        delta_weights,
        marker_offset,
        velocity,
    )
    got_left = lax.ppermute(to_left, "gx", x_down)
    got_right = lax.ppermute(to_right, "gx", x_up)
    home = pl.pallas_call(
        home_kernel,
        out_shape=array(blocks, ROWS, TILE),
        in_specs=[VMEM] * 2,
        out_specs=VMEM,
        compiler_params=params(8),
        cost_estimate=pl.CostEstimate(flops=2_000_000_000, bytes_accessed=0, transcendentals=0),
        name="home",
    )(slot, both)
    to_down, to_up = pl.pallas_call(
        functools.partial(turn_kernel, nx=nx, ny=ny),
        out_shape=(array(y_rows, nz),) * 2,
        in_specs=[VMEM] * 5,
        out_specs=(VMEM,) * 2,
        compiler_params=params(4),
        name="turn",
    )(got_left, got_right, middle, own_down, own_up)
    got_down = lax.ppermute(to_down, "gy", y_down)
    got_up = lax.ppermute(to_up, "gy", y_up)

    devices = gx * gy
    slab = array(6, CYR, nz)
    part, send_l, send_r, message = pl.pallas_call(
        couple_kernel,
        out_shape=(array(nx + 4, CYR, nz), slab, slab, array(devices, 128)),
        in_specs=[VMEM] * 7,
        out_specs=(VMEM,) * 4,
        scratch_shapes=[
            pltpu.VMEM((nx + 4, CYR, 768), BF16),
            pltpu.VMEM((2 * blocks, ROWS, TILE), F32),
            pltpu.VMEM((ROWS, markers), F32),
            pltpu.VMEM((768, 256), BF16),
            pltpu.VMEM((256, 768), BF16),
            pltpu.VMEM((CYR, TILE), F32),
            pltpu.VMEM((WIN, CYR, 768), BF16),
            pltpu.VMEM((128, 128), F32),
        ],
        compiler_params=params(24),
        name="couple",
    )(velocity, got_left, got_right, got_down, got_up, home, linear)

    got_r = lax.ppermute(send_l, "gx", x_down)
    got_l = lax.ppermute(send_r, "gx", x_up)
    everyone = lax.all_to_all(message, ("gx", "gy"), 0, 0, tiled=True)
    strip = array((nx + 8) * 18, nz)
    low, high, line = pl.pallas_call(
        functools.partial(edges_kernel, tall=tall, gx=gx, gy=gy, per_sphere=per_sphere),
        out_shape=(strip, strip, array(1, 128)),
        in_specs=[SMEM] * 3 + [VMEM] * 4,
        out_specs=(VMEM,) * 3,
        scratch_shapes=[pltpu.VMEM((devices, 128), F32)],
        compiler_params=params(4),
        name="edges",
    )(where, contact_sphere, contact_partner, everyone, part, got_l, got_r)
    found = line[0, 0 : 6 * spheres].reshape(spheres, 6).T
    new_motion = found + jnp.concatenate([jnp.zeros((3, spheres), F32), sphere_motion[3:6]], axis=0)

    got_high = lax.ppermute(low, "gy", y_down)
    got_low = lax.ppermute(high, "gy", y_up)
    grown = pltpu.VMEM((3, nx + 8, tall + 4, nz), F32)
    state = pl.pallas_call(
        functools.partial(relax_kernel, tall=tall, rows=ny * gy),
        out_shape=array(3, nx, ny, nz),
        in_specs=[SMEM] + [VMEM] * 5,
        out_specs=VMEM,
        scratch_shapes=[grown, grown, grown],
        compiler_params=params(16),
        name="relax",
    )(where, part, got_l, got_r, got_low, got_high)
    return (state, new_motion)


def solution(mesh):
    placed = (
        P(None, "gx", "gy", None),
        P(("gx", "gy"), None),
        P(("gx", "gy")),
        P(("gx", "gy")),
        P(("gx", "gy")),
        P(None, ("gx", "gy")),
        P(None, ("gx", "gy")),
        P(None, ("gx", "gy")),
        P(("gx", "gy")),
        P(("gx", "gy")),
    )
    return jax.shard_map(
        on_device,
        mesh=mesh,
        in_specs=placed,
        out_specs=(P(None, "gx", "gy", None), P(None, ("gx", "gy"))),
        check_vma=False,
    )
```

```python
import functools

import jax
import jax.numpy as jnp
from jax import lax
from jax.experimental import pallas as pl
from jax.experimental.pallas import tpu as pltpu
from jax.sharding import PartitionSpec as P

F32 = jnp.float32
BF16 = jnp.bfloat16
I32 = jnp.int32

ITERS = 4
DIFFUSION = 1.0
RESPONSE = 0.5
DASHPOT = 0.1

ROWS = 24
TILE = 256
UNROLL = 4
WIN = 8
CYR = 112


TRAVEL = ((0, 0), (-1, 0), (1, 0), (-1, -1), (0, -1), (1, -1), (-1, 1), (0, 1), (1, 1))

VMEM = pl.BlockSpec(memory_space=pltpu.VMEM)
SMEM = pl.BlockSpec(memory_space=pltpu.SMEM)
HBM = pl.BlockSpec(memory_space=pltpu.HBM)


def params(mib):
    return pltpu.CompilerParams(vmem_limit_bytes=mib * 1024 * 1024)


def split(value):
    high = value.astype(BF16)
    low = (value - high.astype(F32)).astype(BF16)
    return high, low


def counting_ranks(bin_of, start_of, bins_here):
    markers = bin_of.shape[1]
    bins = (lax.broadcasted_iota(I32, (32, markers), 0) == bin_of).astype(F32)
    bins16 = bins.astype(BF16)
    ramp_i = lax.broadcasted_iota(I32, (TILE, TILE), 0)
    ramp_j = lax.broadcasted_iota(I32, (TILE, TILE), 1)
    upper = (ramp_i < ramp_j).astype(F32).astype(BF16)
    totals = lax.dot_general(
        jnp.ones((8, markers), BF16), bins16, (((1,), (1,)), ((), ())), preferred_element_type=F32
    )
    row = lax.broadcasted_iota(I32, (32, 32), 0)
    col = lax.broadcasted_iota(I32, (32, 32), 1)
    before = jnp.where(jnp.logical_and(col < row, row < bins_here), totals[0:1, :], 0.0)
    bin_row = lax.broadcasted_iota(I32, (32, 1), 0)
    start = jnp.where(
        bin_row < bins_here, jnp.sum(before, axis=1, keepdims=True), start_of(bin_row).astype(F32)
    )
    slots = []
    for b in range(markers // TILE):
        mine = bins[:, b * TILE : (b + 1) * TILE]
        ranks = jnp.dot(bins16[:, b * TILE : (b + 1) * TILE], upper, preferred_element_type=F32)
        slots.append(jnp.sum(mine * (ranks + start), axis=0, keepdims=True))
        start = start + jnp.sum(mine, axis=1, keepdims=True)
    return jnp.concatenate(slots, axis=1).astype(I32)


def gather_tile(both, slot, tile):
    place = lax.broadcasted_iota(I32, (TILE, slot.shape[1]), 0)
    pick = (slot - tile * TILE == place).astype(F32).astype(BF16)
    out = lax.dot_general(both, pick, (((1,), (1,)), ((), ())), preferred_element_type=F32)
    return out[0:ROWS] + out[ROWS : 2 * ROWS]


def sort_out(index, first, second, out_first, out_second):
    even = (index & 1) == 0
    out_first[...] = jnp.where(even, first[...], second[...])
    out_second[...] = jnp.where(even, second[...], first[...])


def halves(value):
    high, low = split(value)
    return jnp.concatenate([high.astype(F32), low.astype(F32)], axis=0).astype(BF16)


def route_kernel(
    where, motion_h, owner_h, bx_h, by_h, bz_h, weights_h, offset_h, velocity_h,
    to_a, to_b, middle, to_down, to_up, slot_out, both_out, linear,
    motion, owner, bx, by, bz, weights, offset, vel, rec, sems, edge_sem, *, gx, gy_shift
):
    markers = owner.shape[1]
    blocks = markers // TILE
    nx, ny = vel.shape[1:3]
    moves = []
    for k, (src, dst) in enumerate(
        (
            (owner_h, owner),
            (bx_h, bx),
            (by_h, by),
            (bz_h, bz),
            (weights_h, weights),
            (offset_h, offset),
            (motion_h, motion),
        )
    ):
        move = pltpu.make_async_copy(src, dst, sems.at[k])
        move.start()
        moves.append(move)
    whole = pltpu.make_async_copy(velocity_h, vel, edge_sem.at[0])
    whole.start()
    for move in moves:
        move.wait()
    own = owner[...]
    step_x = (lax.shift_right_logical(own, gy_shift) - where[0] + 1) & (gx - 1)
    step_y = (own & ((1 << gy_shift) - 1)) - where[1] + 1
    lane = step_x * 3 + step_y
    bin_of = jnp.where(lane == 4, bx[...], 17 + lane)
    slot = counting_ranks(bin_of, lambda b: markers + (b - 17) * TILE, 17)
    slot_out[...] = slot

    first = lax.broadcasted_iota(I32, (1, markers), 1) < markers // 2
    speed = [jnp.where(first, motion[0, c], motion[1, c]) for c in range(6)]
    off = [offset[c : c + 1, :] for c in range(3)]
    target = [
        speed[0] + (speed[4] * off[2] - speed[5] * off[1]),
        speed[1] + (speed[5] * off[0] - speed[3] * off[2]),
        speed[2] + (speed[3] * off[1] - speed[4] * off[0]),
    ]
    rec[0:12, :] = weights[...]
    rec[12:13, :] = bx[...].astype(F32)
    rec[13:14, :] = by[...].astype(F32)
    rec[14:15, :] = bz[...].astype(F32)
    for c in range(3):
        rec[15 + c : 16 + c, :] = target[c]
    rec[18:21, :] = offset[...]
    rec[21:22, :] = jnp.where(first, 0.0, 1.0)
    rec[22:23, :] = jnp.ones((1, markers), F32)
    rec[23:24, :] = jnp.zeros((1, markers), F32)
    both = halves(rec[...])
    both_out[...] = both
    base = 6 * ny
    even = (where[0] & 1) == 0
    for ref, up in ((to_a, even), (to_b, jnp.logical_not(even))):
        tile = blocks + jnp.where(up, 6, 0)
        for k in range(3):
            ref[base + k * ROWS : base + (k + 1) * ROWS, :] = gather_tile(both, slot, tile + k)
    middle[0] = gather_tile(both, slot, blocks + 3)
    middle[1] = gather_tile(both, slot, blocks + 5)

    lane_row = lax.broadcasted_iota(I32, (1, 128), 1)
    line = jnp.zeros((1, 128), F32)
    for s in range(2):
        for c in range(3):
            line = jnp.where(lane_row == 108 + 6 * s + c, motion[s, c], line)
    linear[...] = line
    whole.wait()
    for c in range(3):
        for x in range(2):
            rows = pl.ds((c * 2 + x) * ny, ny)
            to_a[rows, :] = vel[c, jnp.where(even, nx - 2, 0) + x]
            to_b[rows, :] = vel[c, jnp.where(even, 0, nx - 2) + x]

    for x in range(nx):
        for c in range(3):
            at = (x + 2) * 6 + c * 2
            to_down[at : at + 2, :] = vel[c, x, 0:2, :]
            to_up[at : at + 2, :] = vel[c, x, ny - 2 : ny, :]


def home_kernel(slot, both, home):
    count = jnp.sum((slot[...] < slot.shape[1]).astype(F32)).astype(I32)
    for t in range(home.shape[0]):
        home[t] = jnp.zeros((ROWS, TILE), F32)

    def tile(t, carry):
        home[t] = gather_tile(both[...], slot[...], t)
        return carry

    lax.fori_loop(0, (count + TILE - 1) // TILE, tile, 0)


def turn_kernel(
    where, got_a, got_b, middle, own_down, own_up, to_a, to_b, got_left, got_right, down, up, *, nx, ny
):
    sort_out(where[0], got_a, got_b, got_left, got_right)
    base = 6 * ny
    lists = (nx + 4) * 6
    for out, own, cut, pick, mid in (
        (down, own_down, 0, 0, 0),
        (up, own_up, ny - 2, 2, 1),
    ):
        out[0:lists, :] = own[0:lists, :]
        for x in range(2):
            for c in range(3):
                at = (c * 2 + x) * ny + cut
                to = x * 6 + c * 2
                out[to : to + 2, :] = got_right[at : at + 2, :]
                to = (nx + 2 + x) * 6 + c * 2
                out[to : to + 2, :] = got_left[at : at + 2, :]
        out[lists : lists + ROWS, :] = got_left[base + pick * ROWS : base + (pick + 1) * ROWS, :]
        out[lists + ROWS : lists + 2 * ROWS, :] = middle[mid]
        out[lists + 2 * ROWS : lists + 3 * ROWS, :] = (
            got_right[base + pick * ROWS : base + (pick + 1) * ROWS, :]
        )
    sort_out(where[1], up, down, to_a, to_b)


def chain(distance, rows):
    value = jnp.where(distance == 3, rows[3], 0.0)
    for k in (2, 1, 0):
        value = jnp.where(distance == k, rows[k], value)
    return value


def couple_kernel(
    where, vel, got_xa, got_xb, got_ya, got_yb, home, linear,
    part, send_a, send_b, message,
    got_left, got_right, got_down, got_up, fcat, lists, arrived, tn, tt, sacc, scat, sums,
):
    nx = vel.shape[1] + 4
    cells = vel.shape[2]
    tall = cells + 4
    sort_out(where[0], got_xa, got_xb, got_left, got_right)
    sort_out(where[1], got_ya, got_yb, got_down, got_up)
    zero_pad = jnp.zeros((CYR - 3 * tall, vel.shape[3]), F32)

    def fill_own(x, carry):
        for c in range(3):
            part[x + 2, c * tall + 2 : c * tall + 2 + cells, :] = vel[c, x]
        return carry

    lax.fori_loop(0, nx - 4, fill_own, 0)
    for x in range(2):
        for c in range(3):
            rows = pl.ds((c * 2 + x) * cells, cells)
            part[x, c * tall + 2 : c * tall + 2 + cells, :] = got_right[rows, :]
            part[nx - 2 + x, c * tall + 2 : c * tall + 2 + cells, :] = got_left[rows, :]

    zero2 = jnp.zeros((2, vel.shape[3]), F32)
    for x in range(nx):
        for c in range(3):
            rows = pl.ds(x * 6 + c * 2, 2)
            part[x, c * tall : c * tall + 2, :] = got_up[rows, :]
            part[x, c * tall + 2 + cells : (c + 1) * tall, :] = got_down[rows, :]
        part[x, 3 * tall : CYR, :] = zero_pad

    def fill_rest(x, carry):
        high, low = split(part[x])
        fcat[x, :, 0:256] = high
        fcat[x, :, 256:512] = low
        fcat[x, :, 512:768] = high
        for c in range(3):
            part[x, c * tall : c * tall + 2, :] = zero2
            part[x, c * tall + 2 + cells : (c + 1) * tall, :] = zero2
        return carry

    lax.fori_loop(0, nx, fill_rest, 0)
    for x in (0, 1, nx - 2, nx - 1):
        part[x] = jnp.zeros((CYR, vel.shape[3]), F32)

    base = 6 * cells + ROWS
    after = nx * 6
    arrived[:, 0:TILE] = got_left[base : base + ROWS, :]
    arrived[:, TILE : 2 * TILE] = got_right[base : base + ROWS, :]
    for k in range(3):
        rows = pl.ds(after + k * ROWS, ROWS)
        arrived[:, (2 + k) * TILE : (3 + k) * TILE] = got_down[rows, :]
        arrived[:, (5 + k) * TILE : (6 + k) * TILE] = got_up[rows, :]
    total_lanes = arrived.shape[1]
    lane_at = lax.broadcasted_iota(I32, (1, total_lanes), 1)
    arrived[23:24, :] = (1 + lax.shift_right_logical(lane_at, 8)).astype(F32)
    valid_all = arrived[22:23, :] > 0.5
    count = jnp.sum(arrived[22:23, :]).astype(I32)
    bin_all = jnp.where(valid_all, arrived[12:13, :].astype(I32), 17)
    slot = counting_ranks(bin_all, lambda b: 0 * b + total_lanes, 17)
    both = halves(arrived[...])
    blocks = home.shape[0]
    for t in range(blocks):
        lists[t] = home[t]
        lists[blocks + t] = jnp.zeros((ROWS, TILE), F32)

    def gather_one(t, carry):
        lists[blocks + t] = gather_tile(both, slot, t)
        return carry

    lax.fori_loop(0, (count + TILE - 1) // TILE, gather_one, 0)
    sums[...] = jnp.zeros(sums.shape, F32)

    row = lax.broadcasted_iota(I32, (CYR, 1), 0)
    comp = (row >= tall).astype(I32) + (row >= 2 * tall).astype(I32)
    y_of = jnp.where(row < 3 * tall, row - comp * tall, -100)
    comp = jnp.where(row < 3 * tall, comp, 3)
    z_of = lax.broadcasted_iota(I32, (256, TILE), 0)
    win_row = lax.broadcasted_iota(I32, (WIN, TILE), 0)
    group_of = lax.broadcasted_iota(I32, (128, TILE), 0)

    def tile_body(t, carry):
        rec = lists[t]
        valid = rec[22:23] > 0.5
        bxf = rec[12:13]
        x_first = jnp.min(jnp.where(valid, bxf, 99.0)).astype(I32)
        x_last = jnp.max(jnp.where(valid, bxf, -9.0)).astype(I32)
        windows = jnp.where(x_last < 0, 0, (x_last - x_first + 4 + WIN - 1) // WIN)

        @pl.when(windows > 0)
        def _():
            bxi = bxf.astype(I32)
            byi = rec[13:14].astype(I32)
            bzi = rec[14:15].astype(I32)
            table_z = chain((z_of - bzi) & 255, [rec[8 + k : 9 + k] for k in range(4)])
            high, low = split(table_z)
            tn[0:256, :] = high
            tn[256:512, :] = high
            tn[512:768, :] = low
            tt[:, 0:256] = high
            tt[:, 256:512] = high
            tt[:, 512:768] = low
            table_y = chain(y_of - byi, [rec[4 + k : 5 + k] for k in range(4)])
            sacc[...] = jnp.zeros(sacc.shape, F32)

            def window(w):
                begin = x_first + w * WIN
                x0 = jnp.minimum(begin, nx - WIN)
                x_at = win_row + x0
                table_x = chain(x_at - bxi, [rec[k : k + 1] for k in range(4)])
                return x0, jnp.where(x_at >= begin, table_x, 0.0)

            def sample(w, c):
                x0, table_x = window(w)
                block = fcat[pl.ds(x0, WIN)].reshape(WIN * CYR, 768)
                got = jnp.dot(block, tn[...], preferred_element_type=F32)
                total = sacc[...]
                for i in range(WIN):
                    total = total + table_x[i : i + 1] * got[i * CYR : (i + 1) * CYR]
                sacc[...] = total
                return c

            lax.fori_loop(0, windows, sample, 0)
            weighted = sacc[...] * table_y
            force = [
                rec[15 + c : 16 + c]
                - jnp.sum(jnp.where(comp == c, weighted, 0.0), axis=0, keepdims=True)
                for c in range(3)
            ]
            by_row = jnp.where(comp == 0, force[0], jnp.where(comp == 1, force[1], force[2]))
            plane = table_y * by_row

            def deposit(w, c):
                x0, table_x = window(w)
                for i in range(WIN):
                    hi, lo = split(table_x[i : i + 1] * plane)
                    scat[i, :, 0:256] = hi
                    scat[i, :, 256:512] = lo
                    scat[i, :, 512:768] = hi
                made = lax.dot_general(
                    scat[...].reshape(WIN * CYR, 768),
                    tt[...],
                    (((1,), (1,)), ((), ())),
                    preferred_element_type=F32,
                )
                part[pl.ds(x0, WIN)] += made.reshape(WIN, CYR, 256)
                return c

            lax.fori_loop(0, windows, deposit, 0)
            off = [rec[18 + c : 19 + c] for c in range(3)]
            turn = [
                off[1] * force[2] - off[2] * force[1],
                off[2] * force[0] - off[0] * force[2],
                off[0] * force[1] - off[1] * force[0],
            ]
            stack = jnp.concatenate(force + turn + [jnp.zeros((2, TILE), F32)], axis=0)
            group = (2.0 * rec[23:24] + rec[21:22]).astype(I32)
            member = (group_of == group).astype(F32).astype(BF16)
            found = lax.dot_general(
                member, halves(stack), (((1,), (1,)), ((), ())), preferred_element_type=F32
            )
            sums[:, 0:16] += found

        return carry

    lax.fori_loop(0, 2 * blocks, tile_body, 0)
    lane_of = lax.broadcasted_iota(I32, (128, 128), 1)
    low_part = pltpu.roll(sums[...], 120, axis=1)
    joined = jnp.where(lane_of < 6, sums[...] + low_part, 0.0)
    line = linear[...] + joined[0:1]
    for k in range(1, 18):
        line = line + pltpu.roll(joined[k : k + 1], 6 * k, axis=1)
    message[...] = jnp.broadcast_to(line, message.shape)
    even = (where[0] & 1) == 0
    for x in range(6):
        send_a[x] = part[jnp.where(even, nx - 6, 0) + x]
        send_b[x] = part[jnp.where(even, 0, nx - 6) + x]


def motion(where, contact_own, contact_other, got, out, moved, *, gx, gy, per_sphere):
    here = where[0] * gy + where[1]
    data = got[...]
    total = jnp.zeros(data.shape, F32)
    devices = gx * gy
    for k, (dx, dy) in enumerate(TRAVEL):
        piece = data
        shift = (-(gy * dx + dy)) % devices
        if shift:
            piece = pltpu.roll(piece, shift, axis=0)
        if k:
            piece = pltpu.roll(piece, 128 - 12 * k, axis=1)
        total = total + piece
    linear = pltpu.roll(data, 128 - 108, axis=1)
    moved[...] = linear - (RESPONSE / per_sphere) * total
    lane = lax.broadcasted_iota(I32, (1, 128), 1)
    mine = moved[pl.ds(here, 1), :]
    spring = jnp.zeros((1, 128), F32)
    for k in range(contact_own.shape[0]):
        partner = contact_other[k]
        line = moved[pl.ds(lax.shift_right_logical(partner, 1), 1), :]
        local = contact_own[k] - here * 2
        which = partner & 1
        same = jnp.where(which == local, line, 0.0)
        higher = jnp.where(which < local, pltpu.roll(line, 6, axis=1), 0.0)
        lower = jnp.where(which > local, pltpu.roll(line, 122, axis=1), 0.0)
        of_own = jnp.logical_and(lane >= local * 6, lane < local * 6 + 3)
        spring = spring + jnp.where(of_own, same + higher + lower - mine, 0.0)
    out[...] = mine + DASHPOT * spring


def edges_kernel(
    where, contact_own, contact_other, got, part, got_a, got_b, to_a, to_b, line,
    moved, low, high, *, tall, gx, gy, per_sphere
):
    motion(where, contact_own, contact_other, got, line, moved, gx=gx, gy=gy, per_sphere=per_sphere)
    nx = part.shape[0]
    even = (where[0] & 1) == 0
    for x in range(nx + 4):
        for c in range(3):
            for ref, at in ((low, c * tall), (high, (c + 1) * tall - 6)):
                rows = pl.ds(at, 6)
                pieces = []
                if 2 <= x < nx + 2:
                    pieces.append(part[x - 2, rows, :])
                if x < 6:
                    pieces.append(jnp.where(even, got_b[x, rows, :], got_a[x, rows, :]))
                if x >= nx - 2:
                    y = x - (nx - 2)
                    pieces.append(jnp.where(even, got_a[y, rows, :], got_b[y, rows, :]))
                total = pieces[0]
                for piece in pieces[1:]:
                    total = total + piece
                ref[x * 18 + c * 6 : x * 18 + c * 6 + 6, :] = total
    sort_out(where[1], high, low, to_a, to_b)


def middle_kernel(where, part, got_a, got_b, rhs, *, tall):
    nx = part.shape[0]
    long = nx + 4
    high_y = tall + 4
    even = (where[0] & 1) == 0
    zero2 = jnp.zeros((2, 256), F32)

    def fill(x, sources):
        for c in range(3):
            rows_of = pl.ds(c * tall, tall)
            total = sources[0](rows_of)
            for source in sources[1:]:
                total = total + source(rows_of)
            rhs[c, x, 0:2, :] = zero2
            rhs[c, x, high_y - 2 : high_y, :] = zero2
            rhs[c, x, 2 : 2 + tall, :] = total

    def from_part(at):
        return lambda rows_of: part[at, rows_of, :]

    def chosen(at, first, second):
        return lambda rows_of: jnp.where(even, first[at, rows_of, :], second[at, rows_of, :])

    for x in range(6):
        fill(x, [chosen(x, got_b, got_a)] + ([from_part(x - 2)] if x >= 2 else []))
        fill(
            long - 6 + x,
            [chosen(x, got_a, got_b)] + ([from_part(nx - 4 + x)] if x < 4 else []),
        )

    def centre(x, carry):
        fill(x, [from_part(x - 2)])
        return carry

    lax.fori_loop(6, long - 6, centre, 0)


def relax_kernel(where, grown, got_a, got_b, out_h, rhs, va, vb, low, high, out, sems, *, rows):
    long, high_y = grown.shape[1:3]
    span = high_y - 8
    nx = long - 8
    sort_out(where[1], got_b, got_a, low, high)
    y_at = lax.broadcasted_iota(I32, (high_y, 1), 0) - 4 + where[1] * span
    inside = jnp.logical_and(y_at >= 0, y_at < rows)
    mask = jnp.broadcast_to(inside.astype(F32), (high_y, 256))
    factor = jnp.broadcast_to(
        jnp.where(inside, 1.0 / (1.0 + 6.0 * DIFFUSION), 0.0), (high_y, 256)
    )
    gap = jnp.zeros((high_y - 12, 256), F32)
    for x in range(long):
        for c in range(3):
            at = pl.ds(x * 18 + c * 6, 6)
            edge = jnp.concatenate([low[at, :], gap, high[at, :]], axis=0)
            rhs[c, x] = (grown[c, x] + edge) * mask

    state = rhs
    for sweep in range(ITERS):
        target = (va, vb)[sweep % 2]
        last = sweep == ITERS - 1

        def layer(x, state=state, target=target, last=last):
            for c in range(3):
                here = state[c, x]
                near = state[c, x - 1] + state[c, x + 1]
                near = near + (pltpu.roll(here, 1, axis=1) + pltpu.roll(here, 255, axis=1))
                near = near + (pltpu.roll(here, 1, axis=0) + pltpu.roll(here, high_y - 1, axis=0))
                new = (rhs[c, x] + DIFFUSION * near) * factor
                if last:
                    out[c, x - 4] = new[4 : high_y - 4]
                else:
                    target[c, x] = new

        def group(g, carry, sweep=sweep, layer=layer, last=last):
            for k in range(UNROLL):
                layer(jnp.minimum(sweep + 1 + g * UNROLL + k, long - 2 - sweep))
            if last:
                for c in range(3):
                    part = pl.ds(g * UNROLL, UNROLL)
                    pltpu.make_async_copy(out.at[c, part], out_h.at[c, part], sems.at[g * 3 + c]).start()
            return carry

        lax.fori_loop(0, (long - 2 - 2 * sweep + UNROLL - 1) // UNROLL, group, 0)
        state = target
    for g in range(nx // UNROLL):
        for c in range(3):
            part = pl.ds(g * UNROLL, UNROLL)
            pltpu.make_async_copy(out.at[c, part], out_h.at[c, part], sems.at[g * 3 + c]).wait()


def on_device(
    velocity,
    owner_block,
    base_x,
    base_y,
    base_z,
    delta_weights,
    marker_offset,
    sphere_motion,
    contact_sphere,
    contact_partner,
):
    nx, ny, nz = velocity.shape[1:]
    gx = lax.axis_size("gx")
    gy = lax.axis_size("gy")
    where = jnp.stack([lax.axis_index("gx"), lax.axis_index("gy")]).astype(I32)
    markers = base_x.shape[0]
    spheres = sphere_motion.shape[1]
    per_sphere = markers // spheres
    blocks = markers // TILE
    tall = ny + 4

    def pairs(size, first, wrap):
        both_ways = []
        for i in range(first, size, 2):
            j = (i + 1) % size
            if j or wrap:
                both_ways += [(i, j), (j, i)]
        return both_ways

    def swap_x(first, second):
        return (
            lax.ppermute(first, "gx", pairs(gx, 0, True)),
            lax.ppermute(second, "gx", pairs(gx, 1, True)),
        )

    def swap_y(first, second):
        return (
            lax.ppermute(first, "gy", pairs(gy, 0, False)),
            lax.ppermute(second, "gy", pairs(gy, 1, False)),
        )


    def array(*shape, dtype=F32):
        return jax.ShapeDtypeStruct(shape, dtype)

    x_rows = 6 * ny + 3 * ROWS
    y_rows = 6 * (nx + 4) + 3 * ROWS
    to_a, to_b, middle, own_down, own_up, slot, both, linear = pl.pallas_call(
        functools.partial(route_kernel, gx=gx, gy_shift=gy.bit_length() - 1),
        out_shape=(
            array(x_rows, nz),
            array(x_rows, nz),
            array(2, ROWS, TILE),
            array(y_rows, nz),
            array(y_rows, nz),
            array(1, markers, dtype=I32),
            array(2 * ROWS, markers, dtype=BF16),
            array(1, 128),
        ),
        in_specs=[SMEM] + [HBM] * 8,
        out_specs=(VMEM,) * 8,
        scratch_shapes=[
            pltpu.SMEM((spheres, 6), F32),
            pltpu.VMEM((1, markers), I32),
            pltpu.VMEM((1, markers), I32),
            pltpu.VMEM((1, markers), I32),
            pltpu.VMEM((1, markers), I32),
            pltpu.VMEM((12, markers), F32),
            pltpu.VMEM((3, markers), F32),
            pltpu.VMEM((3, nx, ny, nz), F32),
            pltpu.VMEM((ROWS, markers), F32),
            pltpu.SemaphoreType.DMA((7,)),
            pltpu.SemaphoreType.DMA((1,)),
        ],
        compiler_params=params(16),
        name="route",
    )(
        where,
        *(
            pltpu.with_memory_space_constraint(a, pltpu.HBM)
            for a in (
                sphere_motion.T,
                owner_block.reshape(1, markers),
                base_x.reshape(1, markers),
                base_y.reshape(1, markers),
                base_z.reshape(1, markers),
                delta_weights,
                marker_offset,
                velocity,
            )
        ),
    )
    got_xa, got_xb = swap_x(to_a, to_b)
    home = pl.pallas_call(
        home_kernel,
        out_shape=array(blocks, ROWS, TILE),
        in_specs=[VMEM] * 2,
        out_specs=VMEM,
        compiler_params=params(8),
        cost_estimate=pl.CostEstimate(flops=2_000_000_000, bytes_accessed=0, transcendentals=0),
        name="home",
    )(slot, both)
    x_buffer = pltpu.VMEM((x_rows, nz), F32)
    y_buffer = pltpu.VMEM((y_rows, nz), F32)
    got_ya, got_yb = swap_y(
        *pl.pallas_call(
            functools.partial(turn_kernel, nx=nx, ny=ny),
            out_shape=(array(y_rows, nz),) * 2,
            in_specs=[SMEM] + [VMEM] * 5,
            out_specs=(VMEM,) * 2,
            scratch_shapes=[x_buffer, x_buffer, y_buffer, y_buffer],
            compiler_params=params(4),
            name="turn",
        )(where, got_xa, got_xb, middle, own_down, own_up)
    )

    devices = gx * gy
    slab = array(6, CYR, nz)
    part, send_a, send_b, message = pl.pallas_call(
        couple_kernel,
        out_shape=(array(nx + 4, CYR, nz), slab, slab, array(devices, 128)),
        in_specs=[SMEM] + [VMEM] * 7,
        out_specs=(VMEM,) * 4,
        scratch_shapes=[
            x_buffer,
            x_buffer,
            y_buffer,
            y_buffer,
            pltpu.VMEM((nx + 4, CYR, 768), BF16),
            pltpu.VMEM((2 * blocks, ROWS, TILE), F32),
            pltpu.VMEM((ROWS, markers), F32),
            pltpu.VMEM((768, 256), BF16),
            pltpu.VMEM((256, 768), BF16),
            pltpu.VMEM((CYR, TILE), F32),
            pltpu.VMEM((WIN, CYR, 768), BF16),
            pltpu.VMEM((128, 128), F32),
        ],
        compiler_params=params(24),
        name="couple",
    )(where, velocity, got_xa, got_xb, got_ya, got_yb, home, linear)

    got_a, got_b = swap_x(send_a, send_b)
    everyone = lax.all_to_all(message, ("gx", "gy"), 0, 0, tiled=True)
    strip = array((nx + 8) * 18, nz)
    strip_buffer = pltpu.VMEM(strip.shape, F32)
    to_ya, to_yb, line = pl.pallas_call(
        functools.partial(edges_kernel, tall=tall, gx=gx, gy=gy, per_sphere=per_sphere),
        out_shape=(strip, strip, array(1, 128)),
        in_specs=[SMEM] * 3 + [VMEM] * 4,
        out_specs=(VMEM,) * 3,
        scratch_shapes=[pltpu.VMEM((devices, 128), F32), strip_buffer, strip_buffer],
        compiler_params=params(4),
        name="edges",
    )(where, contact_sphere, contact_partner, everyone, part, got_a, got_b)
    found = line[0, 0 : 6 * spheres].reshape(spheres, 6).T
    new_motion = found + jnp.concatenate([jnp.zeros((3, spheres), F32), sphere_motion[3:6]], axis=0)
    got_ea, got_eb = swap_y(to_ya, to_yb)
    grown = pl.pallas_call(
        functools.partial(middle_kernel, tall=tall),
        out_shape=array(3, nx + 8, tall + 4, nz),
        in_specs=[SMEM] + [VMEM] * 3,
        out_specs=VMEM,
        compiler_params=params(4),
        cost_estimate=pl.CostEstimate(flops=2_000_000_000, bytes_accessed=0, transcendentals=0),
        name="middle",
    )(where, part, got_a, got_b)
    buffer = pltpu.VMEM(grown.shape, F32)
    state = pl.pallas_call(
        functools.partial(relax_kernel, rows=ny * gy),
        out_shape=array(3, nx, ny, nz),
        in_specs=[SMEM] + [VMEM] * 3,
        out_specs=HBM,
        scratch_shapes=[
            buffer,
            buffer,
            buffer,
            strip_buffer,
            strip_buffer,
            pltpu.VMEM((3, nx, ny, nz), F32),
            pltpu.SemaphoreType.DMA((3 * (nx // UNROLL),)),
        ],
        compiler_params=params(20),
        name="relax",
    )(where, grown, got_ea, got_eb)
    return (state, new_motion)


def solution(mesh):
    placed = (
        P(None, "gx", "gy", None),
        P(("gx", "gy"), None),
        P(("gx", "gy")),
        P(("gx", "gy")),
        P(("gx", "gy")),
        P(None, ("gx", "gy")),
        P(None, ("gx", "gy")),
        P(None, ("gx", "gy")),
        P(("gx", "gy")),
        P(("gx", "gy")),
    )
    return jax.shard_map(
        on_device,
        mesh=mesh,
        in_specs=placed,
        out_specs=(P(None, "gx", "gy", None), P(None, ("gx", "gy"))),
        check_vma=False,
    )
```

```python
import functools

import jax
import jax.numpy as jnp
from jax import lax
from jax.experimental import pallas as pl
from jax.experimental.pallas import tpu as pltpu
from jax.sharding import PartitionSpec as P

F32 = jnp.float32
BF16 = jnp.bfloat16
I32 = jnp.int32

ITERS = 4
DIFFUSION = 1.0
RESPONSE = 0.5
DASHPOT = 0.1

ROWS = 24
TILE = 256
UNROLL = 4
SIZES = (7, 8, 9)
WIN = 10
CYR = 112


TRAVEL = ((0, 0), (-1, 0), (1, 0), (-1, -1), (0, -1), (1, -1), (-1, 1), (0, 1), (1, 1))

VMEM = pl.BlockSpec(memory_space=pltpu.VMEM)
SMEM = pl.BlockSpec(memory_space=pltpu.SMEM)
HBM = pl.BlockSpec(memory_space=pltpu.HBM)


def params(mib):
    return pltpu.CompilerParams(vmem_limit_bytes=mib * 1024 * 1024)


def split(value):
    high = value.astype(BF16)
    low = (value - high.astype(F32)).astype(BF16)
    return high, low


def counting_ranks(bin_of, start_of, bins_here):
    markers = bin_of.shape[1]
    bins = (lax.broadcasted_iota(I32, (32, markers), 0) == bin_of).astype(F32)
    bins16 = bins.astype(BF16)
    ramp_i = lax.broadcasted_iota(I32, (TILE, TILE), 0)
    ramp_j = lax.broadcasted_iota(I32, (TILE, TILE), 1)
    upper = (ramp_i < ramp_j).astype(F32).astype(BF16)
    totals = lax.dot_general(
        jnp.ones((8, markers), BF16), bins16, (((1,), (1,)), ((), ())), preferred_element_type=F32
    )
    row = lax.broadcasted_iota(I32, (32, 32), 0)
    col = lax.broadcasted_iota(I32, (32, 32), 1)
    before = jnp.where(jnp.logical_and(col < row, row < bins_here), totals[0:1, :], 0.0)
    bin_row = lax.broadcasted_iota(I32, (32, 1), 0)
    start = jnp.where(
        bin_row < bins_here, jnp.sum(before, axis=1, keepdims=True), start_of(bin_row).astype(F32)
    )
    slots = []
    for b in range(markers // TILE):
        mine = bins[:, b * TILE : (b + 1) * TILE]
        ranks = jnp.dot(bins16[:, b * TILE : (b + 1) * TILE], upper, preferred_element_type=F32)
        slots.append(jnp.sum(mine * (ranks + start), axis=0, keepdims=True))
        start = start + jnp.sum(mine, axis=1, keepdims=True)
    return jnp.concatenate(slots, axis=1).astype(I32)


def gather_tile(both, slot, tile):
    place = lax.broadcasted_iota(I32, (TILE, slot.shape[1]), 0)
    pick = (slot - tile * TILE == place).astype(F32).astype(BF16)
    out = lax.dot_general(both, pick, (((1,), (1,)), ((), ())), preferred_element_type=F32)
    return out[0:ROWS] + out[ROWS : 2 * ROWS]


def sort_out(index, first, second, out_first, out_second):
    even = (index & 1) == 0
    out_first[...] = jnp.where(even, first[...], second[...])
    out_second[...] = jnp.where(even, second[...], first[...])


def halves(value):
    high, low = split(value)
    return jnp.concatenate([high.astype(F32), low.astype(F32)], axis=0).astype(BF16)


def route_kernel(
    where, motion_h, owner_h, bx_h, by_h, bz_h, weights_h, offset_h, velocity_h,
    to_a, to_b, middle, to_down, to_up, slot_out, both_out, linear,
    motion, owner, bx, by, bz, weights, offset, vel, rec, sems, edge_sem, *, gx, gy_shift
):
    markers = owner.shape[1]
    blocks = markers // TILE
    nx, ny = vel.shape[1:3]
    moves = []
    for k, (src, dst) in enumerate(
        (
            (owner_h, owner),
            (bx_h, bx),
            (by_h, by),
            (bz_h, bz),
            (weights_h, weights),
            (offset_h, offset),
            (motion_h, motion),
        )
    ):
        move = pltpu.make_async_copy(src, dst, sems.at[k])
        move.start()
        moves.append(move)
    whole = pltpu.make_async_copy(velocity_h, vel, edge_sem.at[0])
    whole.start()
    for move in moves:
        move.wait()
    own = owner[...]
    step_x = (lax.shift_right_logical(own, gy_shift) - where[0] + 1) & (gx - 1)
    step_y = (own & ((1 << gy_shift) - 1)) - where[1] + 1
    lane = step_x * 3 + step_y
    x_in = jnp.logical_and(bx[...] >= 2, bx[...] <= nx - 2)
    y_in = jnp.logical_and(by[...] >= 2, by[...] <= ny - 2)
    at_home = jnp.where(jnp.logical_and(x_in, y_in), bx[...], 17)
    bin_of = jnp.where(lane == 4, at_home, 18 + lane)
    slot = counting_ranks(
        bin_of, lambda b: jnp.where(b == 17, markers, 2 * markers + (b - 18) * TILE), 17
    )
    slot_out[...] = slot

    first = lax.broadcasted_iota(I32, (1, markers), 1) < markers // 2
    speed = [jnp.where(first, motion[0, c], motion[1, c]) for c in range(6)]
    off = [offset[c : c + 1, :] for c in range(3)]
    target = [
        speed[0] + (speed[4] * off[2] - speed[5] * off[1]),
        speed[1] + (speed[5] * off[0] - speed[3] * off[2]),
        speed[2] + (speed[3] * off[1] - speed[4] * off[0]),
    ]
    rec[0:12, :] = weights[...]
    rec[12:13, :] = bx[...].astype(F32)
    rec[13:14, :] = by[...].astype(F32)
    rec[14:15, :] = bz[...].astype(F32)
    for c in range(3):
        rec[15 + c : 16 + c, :] = target[c]
    rec[18:21, :] = offset[...]
    rec[21:22, :] = jnp.where(first, 0.0, 1.0)
    rec[22:23, :] = jnp.ones((1, markers), F32)
    rec[23:24, :] = jnp.zeros((1, markers), F32)
    both = halves(rec[...])
    both_out[...] = both
    base = 6 * ny
    even = (where[0] & 1) == 0
    for ref, up in ((to_a, even), (to_b, jnp.logical_not(even))):
        tile = 2 * blocks + jnp.where(up, 6, 0)
        for k in range(3):
            ref[base + k * ROWS : base + (k + 1) * ROWS, :] = gather_tile(both, slot, tile + k)
    middle[0] = gather_tile(both, slot, 2 * blocks + 3)
    middle[1] = gather_tile(both, slot, 2 * blocks + 5)

    lane_row = lax.broadcasted_iota(I32, (1, 128), 1)
    line = jnp.zeros((1, 128), F32)
    for s in range(2):
        for c in range(3):
            line = jnp.where(lane_row == 108 + 6 * s + c, motion[s, c], line)
    linear[...] = line
    whole.wait()
    for c in range(3):
        for x in range(2):
            rows = pl.ds((c * 2 + x) * ny, ny)
            to_a[rows, :] = vel[c, jnp.where(even, nx - 2, 0) + x]
            to_b[rows, :] = vel[c, jnp.where(even, 0, nx - 2) + x]

    for x in range(nx):
        for c in range(3):
            at = (x + 2) * 6 + c * 2
            to_down[at : at + 2, :] = vel[c, x, 0:2, :]
            to_up[at : at + 2, :] = vel[c, x, ny - 2 : ny, :]


def home_kernel(slot, both, vel, inner, rim, part, fcat):
    markers = slot.shape[1]
    blocks = inner.shape[0]
    below = (slot[...] < markers).astype(F32)
    upto = (slot[...] < 2 * markers).astype(F32)
    count_inner = jnp.sum(below).astype(I32)
    count_rim = jnp.sum(upto - below).astype(I32)
    for t in range(blocks):
        inner[t] = jnp.zeros((ROWS, TILE), F32)
        rim[t] = jnp.zeros((ROWS, TILE), F32)

    def inner_tile(t, carry):
        inner[t] = gather_tile(both[...], slot[...], t)
        return carry

    def rim_tile(t, carry):
        rim[t] = gather_tile(both[...], slot[...], blocks + t)
        return carry

    lax.fori_loop(0, (count_inner + TILE - 1) // TILE, inner_tile, 0)
    lax.fori_loop(0, (count_rim + TILE - 1) // TILE, rim_tile, 0)

    nx = part.shape[0]
    cells = vel.shape[2]
    tall = cells + 4
    blank = jnp.zeros(part.shape[1:], F32)
    for x in range(nx):
        part[x] = blank
    fill_own(vel, part)

    def halve(x, carry):
        to_halves(part, fcat, x)
        return carry

    lax.fori_loop(0, nx, halve, 0)


def fill_own(vel, field):
    cells = vel.shape[2]

    def layer(x, carry):
        for c in range(3):
            field[x + 2, c * (cells + 4) + 2 : c * (cells + 4) + 2 + cells, :] = vel[c, x]
        return carry

    lax.fori_loop(0, vel.shape[1], layer, 0)


def to_halves(field, fcat, x):
    high, low = split(field[x])
    fcat[x, :, 0:256] = high
    fcat[x, :, 256:512] = low


def turn_kernel(
    where, got_a, got_b, middle, own_down, own_up, to_a, to_b, got_left, got_right, down, up, *, nx, ny
):
    sort_out(where[0], got_a, got_b, got_left, got_right)
    base = 6 * ny
    lists = (nx + 4) * 6
    for out, own, cut, pick, mid in (
        (down, own_down, 0, 0, 0),
        (up, own_up, ny - 2, 2, 1),
    ):
        out[0:lists, :] = own[0:lists, :]
        for x in range(2):
            for c in range(3):
                at = (c * 2 + x) * ny + cut
                to = x * 6 + c * 2
                out[to : to + 2, :] = got_right[at : at + 2, :]
                to = (nx + 2 + x) * 6 + c * 2
                out[to : to + 2, :] = got_left[at : at + 2, :]
        out[lists : lists + ROWS, :] = got_left[base + pick * ROWS : base + (pick + 1) * ROWS, :]
        out[lists + ROWS : lists + 2 * ROWS, :] = middle[mid]
        out[lists + 2 * ROWS : lists + 3 * ROWS, :] = (
            got_right[base + pick * ROWS : base + (pick + 1) * ROWS, :]
        )
    sort_out(where[1], up, down, to_a, to_b)


def chain(distance, rows):
    value = jnp.where(distance == 3, rows[3], 0.0)
    for k in (2, 1, 0):
        value = jnp.where(distance == k, rows[k], value)
    return value


def process_tiles(count, lists, fcat, part, sums, tn, tt, sacc, *, tall):
    nx = part.shape[0]
    row = lax.broadcasted_iota(I32, (CYR, 1), 0)
    comp = (row >= tall).astype(I32) + (row >= 2 * tall).astype(I32)
    y_of = jnp.where(row < 3 * tall, row - comp * tall, -100)
    comp = jnp.where(row < 3 * tall, comp, 3)
    z_of = lax.broadcasted_iota(I32, (256, TILE), 0)
    win_row = lax.broadcasted_iota(I32, (16, TILE), 0)
    group_of = lax.broadcasted_iota(I32, (128, TILE), 0)

    def tile_body(t, carry):
        rec = lists[t]
        valid = rec[22:23] > 0.5
        bxf = rec[12:13]
        x_first = jnp.min(jnp.where(valid, bxf, 99.0)).astype(I32)
        x_last = jnp.max(jnp.where(valid, bxf, -9.0)).astype(I32)
        layers = x_last - x_first + 4
        windows = jnp.where(x_last < 0, 0, (layers + WIN - 1) // WIN)

        @pl.when(windows > 0)
        def _():
            bxi = bxf.astype(I32)
            byi = rec[13:14].astype(I32)
            bzi = rec[14:15].astype(I32)
            table_z = chain((z_of - bzi) & 255, [rec[8 + k : 9 + k] for k in range(4)])
            high, low = split(table_z)
            tn[0:256, :] = high
            tn[256:512, :] = low
            tt[:, 0:256] = high
            tt[:, 256:512] = low
            table_y = chain(y_of - byi, [rec[4 + k : 5 + k] for k in range(4)])
            sacc[...] = jnp.zeros(sacc.shape, F32)

            def window(w, size):
                begin = x_first + w * size
                x0 = jnp.minimum(begin, nx - size)
                x_at = win_row + x0
                table_x = chain(x_at - bxi, [rec[k : k + 1] for k in range(4)])
                return x0, jnp.where(x_at >= begin, table_x, 0.0)

            def sample(w, size):
                x0, table_x = window(w, size)
                block_h = fcat[pl.ds(x0, size), :, 0:256].reshape(size * CYR, 256)
                block_l = fcat[pl.ds(x0, size), :, 256:512].reshape(size * CYR, 256)
                got = (
                    jnp.dot(block_h, tn[0:256], preferred_element_type=F32)
                    + jnp.dot(block_l, tn[0:256], preferred_element_type=F32)
                    + jnp.dot(block_h, tn[256:512], preferred_element_type=F32)
                )
                total = sacc[...]
                for i in range(size):
                    total = total + table_x[i : i + 1] * got[i * CYR : (i + 1) * CYR]
                sacc[...] = total

            def by_size(step):
                for size in SIZES:
                    fits = layers <= size
                    if size > SIZES[0]:
                        fits = jnp.logical_and(fits, layers > size - 1)
                    pl.when(fits)(functools.partial(step, 0, size))

                @pl.when(layers > SIZES[-1])
                def _():
                    def loop(w, c):
                        step(w, WIN)
                        return c

                    lax.fori_loop(0, windows, loop, 0)

            by_size(sample)
            weighted = sacc[...] * table_y
            force = [
                rec[15 + c : 16 + c]
                - jnp.sum(jnp.where(comp == c, weighted, 0.0), axis=0, keepdims=True)
                for c in range(3)
            ]
            by_row = jnp.where(comp == 0, force[0], jnp.where(comp == 1, force[1], force[2]))
            plane = table_y * by_row

            def deposit(w, size):
                x0, table_x = window(w, size)
                pieces = [split(table_x[i : i + 1] * plane) for i in range(size)]
                high_s = jnp.concatenate([p[0] for p in pieces], axis=0)
                low_s = jnp.concatenate([p[1] for p in pieces], axis=0)
                nt = (((1,), (1,)), ((), ()))
                made = (
                    lax.dot_general(high_s, tt[:, 0:256], nt, preferred_element_type=F32)
                    + lax.dot_general(low_s, tt[:, 0:256], nt, preferred_element_type=F32)
                    + lax.dot_general(high_s, tt[:, 256:512], nt, preferred_element_type=F32)
                )
                part[pl.ds(x0, size)] += made.reshape(size, CYR, 256)

            by_size(deposit)
            off = [rec[18 + c : 19 + c] for c in range(3)]
            turn = [
                off[1] * force[2] - off[2] * force[1],
                off[2] * force[0] - off[0] * force[2],
                off[0] * force[1] - off[1] * force[0],
            ]
            stack = jnp.concatenate(force + turn + [jnp.zeros((2, TILE), F32)], axis=0)
            group = (2.0 * rec[23:24] + rec[21:22]).astype(I32)
            member = (group_of == group).astype(F32).astype(BF16)
            found = lax.dot_general(
                member, halves(stack), (((1,), (1,)), ((), ())), preferred_element_type=F32
            )
            sums[:, 0:16] += found

        return carry

    lax.fori_loop(0, count, tile_body, 0)


def inner_kernel(lists, fcat, part_in, part, sums, tn, tt, sacc, *, tall):
    del part_in
    sums[...] = jnp.zeros(sums.shape, F32)
    process_tiles(lists.shape[0], lists, fcat, part, sums, tn, tt, sacc, tall=tall)


def couple_kernel(
    where, vel, got_xa, got_xb, got_ya, got_yb, rim, linear, sums_in, part_in,
    part, send_a, send_b, message,
    got_left, got_right, got_down, got_up, field, fcat, lists, arrived, tn, tt, sacc, sums,
):
    del part_in
    nx = vel.shape[1] + 4
    cells = vel.shape[2]
    tall = cells + 4
    sort_out(where[0], got_xa, got_xb, got_left, got_right)
    sort_out(where[1], got_ya, got_yb, got_down, got_up)
    zero_pad = jnp.zeros((CYR - 3 * tall, vel.shape[3]), F32)
    fill_own(vel, field)
    for x in range(2):
        for c in range(3):
            rows = pl.ds((c * 2 + x) * cells, cells)
            field[x, c * tall + 2 : c * tall + 2 + cells, :] = got_right[rows, :]
            field[nx - 2 + x, c * tall + 2 : c * tall + 2 + cells, :] = got_left[rows, :]
    for x in range(nx):
        for c in range(3):
            rows = pl.ds(x * 6 + c * 2, 2)
            field[x, c * tall : c * tall + 2, :] = got_up[rows, :]
            field[x, c * tall + 2 + cells : (c + 1) * tall, :] = got_down[rows, :]
        field[x, 3 * tall : CYR, :] = zero_pad

    def halve(x, carry):
        to_halves(field, fcat, x)
        return carry

    lax.fori_loop(0, nx, halve, 0)

    base = 6 * cells + ROWS
    after = nx * 6
    blocks = rim.shape[0]
    arrived[:, 0:TILE] = got_left[base : base + ROWS, :]
    arrived[:, TILE : 2 * TILE] = got_right[base : base + ROWS, :]
    for k in range(3):
        rows = pl.ds(after + k * ROWS, ROWS)
        arrived[:, (2 + k) * TILE : (3 + k) * TILE] = got_down[rows, :]
        arrived[:, (5 + k) * TILE : (6 + k) * TILE] = got_up[rows, :]
    for t in range(blocks):
        arrived[:, (8 + t) * TILE : (9 + t) * TILE] = rim[t]
    total_lanes = arrived.shape[1]
    lane_at = lax.broadcasted_iota(I32, (1, total_lanes), 1)
    list_at = 1 + lax.shift_right_logical(lane_at, TILE.bit_length() - 1)
    arrived[23:24, :] = jnp.where(list_at > 8, 0, list_at).astype(F32)
    valid_all = arrived[22:23, :] > 0.5
    count = jnp.sum(arrived[22:23, :]).astype(I32)
    few = 10 * TILE
    beyond = jnp.sum(arrived[22:23, few:total_lanes])
    bin_all = jnp.where(valid_all, arrived[12:13, :].astype(I32), 17)
    slot = counting_ranks(bin_all, lambda b: 0 * b + total_lanes, 17)
    both = halves(arrived[...])
    for t in range(lists.shape[0]):
        lists[t] = jnp.zeros((ROWS, TILE), F32)
    tiles = (count + TILE - 1) // TILE

    def gather_few(t, carry):
        lists[t] = gather_tile(both[:, 0:few], slot[:, 0:few], t)
        return carry

    def gather_all(t, carry):
        lists[t] = gather_tile(both, slot, t)
        return carry

    lax.fori_loop(0, jnp.where(beyond > 0.5, 0, tiles), gather_few, 0)
    lax.fori_loop(0, jnp.where(beyond > 0.5, tiles, 0), gather_all, 0)
    sums[...] = sums_in[...]
    process_tiles(tiles, lists, fcat, part, sums, tn, tt, sacc, tall=tall)
    lane_of = lax.broadcasted_iota(I32, (128, 128), 1)
    low_part = pltpu.roll(sums[...], 120, axis=1)
    joined = jnp.where(lane_of < 6, sums[...] + low_part, 0.0)
    line = linear[...] + joined[0:1]
    for k in range(1, 18):
        line = line + pltpu.roll(joined[k : k + 1], 6 * k, axis=1)
    message[...] = jnp.broadcast_to(line, message.shape)
    even = (where[0] & 1) == 0
    for x in range(6):
        send_a[x] = part[jnp.where(even, nx - 6, 0) + x]
        send_b[x] = part[jnp.where(even, 0, nx - 6) + x]


def motion_kernel(
    where, contact_own, contact_other, angular, got, out, moved, *, gx, gy, per_sphere
):
    here = where[0] * gy + where[1]
    data = got[...]
    total = jnp.zeros(data.shape, F32)
    devices = gx * gy
    for k, (dx, dy) in enumerate(TRAVEL):
        piece = data
        shift = (-(gy * dx + dy)) % devices
        if shift:
            piece = pltpu.roll(piece, shift, axis=0)
        if k:
            piece = pltpu.roll(piece, 128 - 12 * k, axis=1)
        total = total + piece
    linear = pltpu.roll(data, 128 - 108, axis=1)
    moved[...] = linear - (RESPONSE / per_sphere) * total
    lane = lax.broadcasted_iota(I32, (1, 128), 1)
    mine = moved[pl.ds(here, 1), :]
    spring = jnp.zeros((1, 128), F32)
    for k in range(contact_own.shape[0]):
        partner = contact_other[k]
        line = moved[pl.ds(lax.shift_right_logical(partner, 1), 1), :]
        local = contact_own[k] - here * 2
        which = partner & 1
        same = jnp.where(which == local, line, 0.0)
        higher = jnp.where(which < local, pltpu.roll(line, 6, axis=1), 0.0)
        lower = jnp.where(which > local, pltpu.roll(line, 122, axis=1), 0.0)
        of_own = jnp.logical_and(lane >= local * 6, lane < local * 6 + 3)
        spring = spring + jnp.where(of_own, same + higher + lower - mine, 0.0)
    result = mine + DASHPOT * spring
    out[0:1, :] = result[:, 0:6] + angular[0:1, :]
    out[1:2, :] = pltpu.roll(result, 122, axis=1)[:, 0:6] + angular[1:2, :]


def edges_kernel(where, part, got_a, got_b, to_a, to_b, *, tall):
    nx = part.shape[0]
    even = (where[0] & 1) == 0
    even_y = (where[1] & 1) == 0
    for x in range(nx + 4):
        for c in range(3):
            values = []
            for at in (c * tall, (c + 1) * tall - 6):
                rows = pl.ds(at, 6)
                pieces = []
                if 2 <= x < nx + 2:
                    pieces.append(part[x - 2, rows, :])
                if x < 6:
                    pieces.append(jnp.where(even, got_b[x, rows, :], got_a[x, rows, :]))
                if x >= nx - 2:
                    y = x - (nx - 2)
                    pieces.append(jnp.where(even, got_a[y, rows, :], got_b[y, rows, :]))
                total = pieces[0]
                for piece in pieces[1:]:
                    total = total + piece
                values.append(total)
            to = pl.ds(x * 18 + c * 6, 6)
            to_a[to, :] = jnp.where(even_y, values[1], values[0])
            to_b[to, :] = jnp.where(even_y, values[0], values[1])


def middle_kernel(where, part, got_a, got_b, rhs, *, tall):
    nx = part.shape[0]
    long = nx + 4
    high_y = tall + 4
    even = (where[0] & 1) == 0
    zero2 = jnp.zeros((2, 256), F32)

    def fill(x, sources):
        for c in range(3):
            rows_of = pl.ds(c * tall, tall)
            total = sources[0](rows_of)
            for source in sources[1:]:
                total = total + source(rows_of)
            rhs[c, x, 0:2, :] = zero2
            rhs[c, x, high_y - 2 : high_y, :] = zero2
            rhs[c, x, 2 : 2 + tall, :] = total

    def from_part(at):
        return lambda rows_of: part[at, rows_of, :]

    def chosen(at, first, second):
        return lambda rows_of: jnp.where(even, first[at, rows_of, :], second[at, rows_of, :])

    for x in range(6):
        fill(x, [chosen(x, got_b, got_a)] + ([from_part(x - 2)] if x >= 2 else []))
        fill(
            long - 6 + x,
            [chosen(x, got_a, got_b)] + ([from_part(nx - 4 + x)] if x < 4 else []),
        )

    def centre(x, carry):
        fill(x, [from_part(x - 2)])
        return carry

    lax.fori_loop(6, long - 6, centre, 0)


def relax_kernel(where, grown, got_a, got_b, out_h, rhs, va, vb, low, high, out, sems, *, rows):
    long, high_y = grown.shape[1:3]
    span = high_y - 8
    nx = long - 8
    sort_out(where[1], got_b, got_a, low, high)
    y_at = lax.broadcasted_iota(I32, (high_y, 1), 0) - 4 + where[1] * span
    inside = jnp.logical_and(y_at >= 0, y_at < rows)
    mask = jnp.broadcast_to(inside.astype(F32), (high_y, 256))
    factor = jnp.broadcast_to(
        jnp.where(inside, 1.0 / (1.0 + 6.0 * DIFFUSION), 0.0), (high_y, 256)
    )
    gap = jnp.zeros((high_y - 12, 256), F32)
    for x in range(long):
        for c in range(3):
            at = pl.ds(x * 18 + c * 6, 6)
            edge = jnp.concatenate([low[at, :], gap, high[at, :]], axis=0)
            rhs[c, x] = (grown[c, x] + edge) * mask

    state = rhs
    for sweep in range(ITERS):
        target = (va, vb)[sweep % 2]
        last = sweep == ITERS - 1

        def layer(x, state=state, target=target, last=last):
            for c in range(3):
                here = state[c, x]
                near = state[c, x - 1] + state[c, x + 1]
                near = near + (pltpu.roll(here, 1, axis=1) + pltpu.roll(here, 255, axis=1))
                near = near + (pltpu.roll(here, 1, axis=0) + pltpu.roll(here, high_y - 1, axis=0))
                new = (rhs[c, x] + DIFFUSION * near) * factor
                if last:
                    out[c, x - 4] = new[4 : high_y - 4]
                else:
                    target[c, x] = new

        def group(g, carry, sweep=sweep, layer=layer, last=last):
            for k in range(UNROLL):
                layer(jnp.minimum(sweep + 1 + g * UNROLL + k, long - 2 - sweep))
            if last:
                for c in range(3):
                    part = pl.ds(g * UNROLL, UNROLL)
                    pltpu.make_async_copy(out.at[c, part], out_h.at[c, part], sems.at[g * 3 + c]).start()
            return carry

        lax.fori_loop(0, (long - 2 - 2 * sweep + UNROLL - 1) // UNROLL, group, 0)
        state = target
    for g in range(nx // UNROLL):
        for c in range(3):
            part = pl.ds(g * UNROLL, UNROLL)
            pltpu.make_async_copy(out.at[c, part], out_h.at[c, part], sems.at[g * 3 + c]).wait()


def on_device(
    velocity,
    owner_block,
    base_x,
    base_y,
    base_z,
    delta_weights,
    marker_offset,
    sphere_motion,
    contact_sphere,
    contact_partner,
):
    nx, ny, nz = velocity.shape[1:]
    gx = lax.axis_size("gx")
    gy = lax.axis_size("gy")
    where = jnp.stack([lax.axis_index("gx"), lax.axis_index("gy")]).astype(I32)
    markers = base_x.shape[0]
    spheres = sphere_motion.shape[1]
    per_sphere = markers // spheres
    blocks = markers // TILE
    tall = ny + 4

    def pairs(size, first, wrap):
        both_ways = []
        for i in range(first, size, 2):
            j = (i + 1) % size
            if j or wrap:
                both_ways += [(i, j), (j, i)]
        return both_ways

    def swap_x(first, second):
        return (
            lax.ppermute(first, "gx", pairs(gx, 0, True)),
            lax.ppermute(second, "gx", pairs(gx, 1, True)),
        )

    def swap_y(first, second):
        return (
            lax.ppermute(first, "gy", pairs(gy, 0, False)),
            lax.ppermute(second, "gy", pairs(gy, 1, False)),
        )


    def array(*shape, dtype=F32):
        return jax.ShapeDtypeStruct(shape, dtype)

    x_rows = 6 * ny + 3 * ROWS
    y_rows = 6 * (nx + 4) + 3 * ROWS
    to_a, to_b, middle, own_down, own_up, slot, both, linear = pl.pallas_call(
        functools.partial(route_kernel, gx=gx, gy_shift=gy.bit_length() - 1),
        out_shape=(
            array(x_rows, nz),
            array(x_rows, nz),
            array(2, ROWS, TILE),
            array(y_rows, nz),
            array(y_rows, nz),
            array(1, markers, dtype=I32),
            array(2 * ROWS, markers, dtype=BF16),
            array(1, 128),
        ),
        in_specs=[SMEM] + [HBM] * 8,
        out_specs=(VMEM,) * 8,
        scratch_shapes=[
            pltpu.SMEM((spheres, 6), F32),
            pltpu.VMEM((1, markers), I32),
            pltpu.VMEM((1, markers), I32),
            pltpu.VMEM((1, markers), I32),
            pltpu.VMEM((1, markers), I32),
            pltpu.VMEM((12, markers), F32),
            pltpu.VMEM((3, markers), F32),
            pltpu.VMEM((3, nx, ny, nz), F32),
            pltpu.VMEM((ROWS, markers), F32),
            pltpu.SemaphoreType.DMA((7,)),
            pltpu.SemaphoreType.DMA((1,)),
        ],
        compiler_params=params(16),
        name="route",
    )(
        where,
        *(
            pltpu.with_memory_space_constraint(a, pltpu.HBM)
            for a in (
                sphere_motion.T,
                owner_block.reshape(1, markers),
                base_x.reshape(1, markers),
                base_y.reshape(1, markers),
                base_z.reshape(1, markers),
                delta_weights,
                marker_offset,
                velocity,
            )
        ),
    )
    got_xa, got_xb = swap_x(to_a, to_b)
    field = array(nx + 4, CYR, nz)
    halved = array(nx + 4, CYR, 2 * nz, dtype=BF16)
    lists = array(blocks, ROWS, TILE)
    inner, rim, part, fcat = pl.pallas_call(
        home_kernel,
        out_shape=(lists, lists, field, halved),
        in_specs=[VMEM] * 3,
        out_specs=(VMEM,) * 4,
        compiler_params=params(8),
        cost_estimate=pl.CostEstimate(flops=2_000_000_000, bytes_accessed=0, transcendentals=0),
        name="home",
    )(slot, both, velocity)
    tile_scratch = [
        pltpu.VMEM((2 * nz, TILE), BF16),
        pltpu.VMEM((nz, 2 * TILE), BF16),
        pltpu.VMEM((CYR, TILE), F32),
    ]
    part, sums = pl.pallas_call(
        functools.partial(inner_kernel, tall=tall),
        out_shape=(field, array(128, 128)),
        in_specs=[VMEM] * 3,
        out_specs=(VMEM,) * 2,
        input_output_aliases={2: 0},
        scratch_shapes=tile_scratch,
        compiler_params=params(8),
        cost_estimate=pl.CostEstimate(flops=4_000_000_000, bytes_accessed=0, transcendentals=0),
        name="inner",
    )(inner, fcat, part)
    x_buffer = pltpu.VMEM((x_rows, nz), F32)
    y_buffer = pltpu.VMEM((y_rows, nz), F32)
    got_ya, got_yb = swap_y(
        *pl.pallas_call(
            functools.partial(turn_kernel, nx=nx, ny=ny),
            out_shape=(array(y_rows, nz),) * 2,
            in_specs=[SMEM] + [VMEM] * 5,
            out_specs=(VMEM,) * 2,
            scratch_shapes=[x_buffer, x_buffer, y_buffer, y_buffer],
            compiler_params=params(4),
            name="turn",
        )(where, got_xa, got_xb, middle, own_down, own_up)
    )

    devices = gx * gy
    slab = array(6, CYR, nz)
    part, send_a, send_b, message = pl.pallas_call(
        couple_kernel,
        out_shape=(field, slab, slab, array(devices, 128)),
        in_specs=[SMEM] + [VMEM] * 9,
        out_specs=(VMEM,) * 4,
        input_output_aliases={9: 0},
        scratch_shapes=[
            x_buffer,
            x_buffer,
            y_buffer,
            y_buffer,
            pltpu.VMEM(field.shape, F32),
            pltpu.VMEM(halved.shape, BF16),
            pltpu.VMEM((2 * blocks, ROWS, TILE), F32),
            pltpu.VMEM((ROWS, 2 * markers), F32),
            *tile_scratch,
            pltpu.VMEM((128, 128), F32),
        ],
        compiler_params=params(16),
        name="couple",
    )(where, velocity, got_xa, got_xb, got_ya, got_yb, rim, linear, sums, part)

    got_a, got_b = swap_x(send_a, send_b)
    everyone = lax.all_to_all(message, ("gx", "gy"), 0, 0, tiled=True)
    strip = array((nx + 8) * 18, nz)
    everyone, part = lax.optimization_barrier((everyone, part))
    strip_buffer = pltpu.VMEM(strip.shape, F32)
    to_ya, to_yb = pl.pallas_call(
        functools.partial(edges_kernel, tall=tall),
        out_shape=(strip, strip),
        in_specs=[SMEM] + [VMEM] * 3,
        out_specs=(VMEM,) * 2,
        compiler_params=params(4),
        name="edges",
    )(where, part, got_a, got_b)
    angular = jnp.concatenate([jnp.zeros((3, spheres), F32), sphere_motion[3:6]], axis=0).T
    new_motion = pl.pallas_call(
        functools.partial(motion_kernel, gx=gx, gy=gy, per_sphere=per_sphere),
        out_shape=array(spheres, 6),
        in_specs=[SMEM] * 3 + [VMEM] * 2,
        out_specs=VMEM,
        scratch_shapes=[pltpu.VMEM((devices, 128), F32)],
        compiler_params=params(4),
        name="motion",
    )(where, contact_sphere, contact_partner, angular, everyone).T
    got_ea, got_eb = swap_y(to_ya, to_yb)
    grown = pl.pallas_call(
        functools.partial(middle_kernel, tall=tall),
        out_shape=array(3, nx + 8, tall + 4, nz),
        in_specs=[SMEM] + [VMEM] * 3,
        out_specs=VMEM,
        compiler_params=params(4),
        cost_estimate=pl.CostEstimate(flops=2_000_000_000, bytes_accessed=0, transcendentals=0),
        name="middle",
    )(where, part, got_a, got_b)
    buffer = pltpu.VMEM(grown.shape, F32)
    state = pl.pallas_call(
        functools.partial(relax_kernel, rows=ny * gy),
        out_shape=array(3, nx, ny, nz),
        in_specs=[SMEM] + [VMEM] * 3,
        out_specs=HBM,
        scratch_shapes=[
            buffer,
            buffer,
            buffer,
            strip_buffer,
            strip_buffer,
            pltpu.VMEM((3, nx, ny, nz), F32),
            pltpu.SemaphoreType.DMA((3 * (nx // UNROLL),)),
        ],
        compiler_params=params(20),
        name="relax",
    )(where, grown, got_ea, got_eb)
    return (state, new_motion)


def solution(mesh):
    placed = (
        P(None, "gx", "gy", None),
        P(("gx", "gy"), None),
        P(("gx", "gy")),
        P(("gx", "gy")),
        P(("gx", "gy")),
        P(None, ("gx", "gy")),
        P(None, ("gx", "gy")),
        P(None, ("gx", "gy")),
        P(("gx", "gy")),
        P(("gx", "gy")),
    )
    return jax.shard_map(
        on_device,
        mesh=mesh,
        in_specs=placed,
        out_specs=(P(None, "gx", "gy", None), P(None, ("gx", "gy"))),
        check_vma=False,
    )
```

```python
import functools

import jax
import jax.numpy as jnp
from jax import lax
from jax.experimental import pallas as pl
from jax.experimental.pallas import tpu as pltpu
from jax.sharding import PartitionSpec as P

F32 = jnp.float32
BF16 = jnp.bfloat16
I32 = jnp.int32

ITERS = 4
DIFFUSION = 1.0
RESPONSE = 0.5
DASHPOT = 0.1

ROWS = 24
TILE = 256
UNROLL = 4
EARLY = 2
SIZES = (6, 7, 8, 9)
WIN = 10
CYR = 112


TRAVEL = ((0, 0), (-1, 0), (1, 0), (-1, -1), (0, -1), (1, -1), (-1, 1), (0, 1), (1, 1))

VMEM = pl.BlockSpec(memory_space=pltpu.VMEM)
SMEM = pl.BlockSpec(memory_space=pltpu.SMEM)
HBM = pl.BlockSpec(memory_space=pltpu.HBM)


def params(mib):
    return pltpu.CompilerParams(vmem_limit_bytes=mib * 1024 * 1024)


def split(value):
    high = value.astype(BF16)
    low = (value - high.astype(F32)).astype(BF16)
    return high, low


def counting_ranks(bin_of, start_of, bins_here):
    markers = bin_of.shape[1]
    bins = (lax.broadcasted_iota(I32, (32, markers), 0) == bin_of).astype(F32)
    bins16 = bins.astype(BF16)
    ramp_i = lax.broadcasted_iota(I32, (TILE, TILE), 0)
    ramp_j = lax.broadcasted_iota(I32, (TILE, TILE), 1)
    upper = (ramp_i < ramp_j).astype(F32).astype(BF16)
    totals = lax.dot_general(
        jnp.ones((8, markers), BF16), bins16, (((1,), (1,)), ((), ())), preferred_element_type=F32
    )
    row = lax.broadcasted_iota(I32, (32, 32), 0)
    col = lax.broadcasted_iota(I32, (32, 32), 1)
    before = jnp.where(jnp.logical_and(col < row, row < bins_here), totals[0:1, :], 0.0)
    bin_row = lax.broadcasted_iota(I32, (32, 1), 0)
    start = jnp.where(
        bin_row < bins_here, jnp.sum(before, axis=1, keepdims=True), start_of(bin_row).astype(F32)
    )
    slots = []
    for b in range(markers // TILE):
        mine = bins[:, b * TILE : (b + 1) * TILE]
        ranks = jnp.dot(bins16[:, b * TILE : (b + 1) * TILE], upper, preferred_element_type=F32)
        slots.append(jnp.sum(mine * (ranks + start), axis=0, keepdims=True))
        start = start + jnp.sum(mine, axis=1, keepdims=True)
    return jnp.concatenate(slots, axis=1).astype(I32)


def gather_tile(both, slot, tile):
    place = lax.broadcasted_iota(I32, (TILE, slot.shape[1]), 0).astype(F32).astype(BF16)
    local = jnp.clip(slot - tile * TILE, -1, TILE).astype(F32).astype(BF16)
    pick = jnp.where(place == local, jnp.ones((), BF16), jnp.zeros((), BF16))
    out = lax.dot_general(both, pick, (((1,), (1,)), ((), ())), preferred_element_type=F32)
    return out[0:ROWS] + out[ROWS : 2 * ROWS]


def sort_out(index, first, second, out_first, out_second):
    even = (index & 1) == 0
    out_first[...] = jnp.where(even, first[...], second[...])
    out_second[...] = jnp.where(even, second[...], first[...])


def halves(value):
    high, low = split(value)
    return jnp.concatenate([high.astype(F32), low.astype(F32)], axis=0).astype(BF16)


def route_kernel(
    where, motion_h, owner_h, bx_h, by_h, bz_h, weights_h, offset_h, velocity_h,
    to_a, to_b, middle, to_down, to_up, slot_out, both_out, linear, vel,
    motion, owner, bx, by, bz, weights, offset, rec, sems, edge_sem, *, gx, gy_shift
):
    markers = owner.shape[1]
    blocks = markers // TILE
    nx, ny = vel.shape[1:3]
    moves = []
    for k, (src, dst) in enumerate(
        (
            (owner_h, owner),
            (bx_h, bx),
            (by_h, by),
            (bz_h, bz),
            (weights_h, weights),
            (offset_h, offset),
            (motion_h, motion),
        )
    ):
        move = pltpu.make_async_copy(src, dst, sems.at[k])
        move.start()
        moves.append(move)
    whole = pltpu.make_async_copy(velocity_h, vel, edge_sem.at[0])
    whole.start()
    for move in moves:
        move.wait()
    own = owner[...]
    step_x = (lax.shift_right_logical(own, gy_shift) - where[0] + 1) & (gx - 1)
    step_y = (own & ((1 << gy_shift) - 1)) - where[1] + 1
    lane = step_x * 3 + step_y
    x_in = jnp.logical_and(bx[...] >= 2, bx[...] <= nx - 2)
    y_in = jnp.logical_and(by[...] >= 2, by[...] <= ny - 2)
    at_home = jnp.where(jnp.logical_and(x_in, y_in), bx[...], 17)
    bin_of = jnp.where(lane == 4, at_home, 18 + lane)
    slot = counting_ranks(
        bin_of, lambda b: jnp.where(b == 17, markers, 2 * markers + (b - 18) * TILE), 17
    )
    slot_out[...] = slot

    first = lax.broadcasted_iota(I32, (1, markers), 1) < markers // 2
    speed = [jnp.where(first, motion[0, c], motion[1, c]) for c in range(6)]
    off = [offset[c : c + 1, :] for c in range(3)]
    target = [
        speed[0] + (speed[4] * off[2] - speed[5] * off[1]),
        speed[1] + (speed[5] * off[0] - speed[3] * off[2]),
        speed[2] + (speed[3] * off[1] - speed[4] * off[0]),
    ]
    rec[0:12, :] = weights[...]
    rec[12:13, :] = bx[...].astype(F32)
    rec[13:14, :] = by[...].astype(F32)
    rec[14:15, :] = bz[...].astype(F32)
    for c in range(3):
        rec[15 + c : 16 + c, :] = target[c]
    rec[18:21, :] = offset[...]
    rec[21:22, :] = jnp.where(first, 0.0, 1.0)
    rec[22:23, :] = jnp.ones((1, markers), F32)
    rec[23:24, :] = jnp.zeros((1, markers), F32)
    both = halves(rec[...])
    both_out[...] = both
    base = 6 * ny
    even = (where[0] & 1) == 0
    for ref, up in ((to_a, even), (to_b, jnp.logical_not(even))):
        tile = 2 * blocks + jnp.where(up, 6, 0)
        for k in range(3):
            ref[base + k * ROWS : base + (k + 1) * ROWS, :] = gather_tile(both, slot, tile + k)
    middle[0] = gather_tile(both, slot, 2 * blocks + 3)
    middle[1] = gather_tile(both, slot, 2 * blocks + 5)

    lane_row = lax.broadcasted_iota(I32, (1, 128), 1)
    line = jnp.zeros((1, 128), F32)
    for s in range(2):
        for c in range(3):
            line = jnp.where(lane_row == 108 + 6 * s + c, motion[s, c], line)
    linear[...] = line
    whole.wait()
    for c in range(3):
        for x in range(2):
            rows = pl.ds((c * 2 + x) * ny, ny)
            to_a[rows, :] = vel[c, jnp.where(even, nx - 2, 0) + x]
            to_b[rows, :] = vel[c, jnp.where(even, 0, nx - 2) + x]

    for x in range(nx):
        for c in range(3):
            at = (x + 2) * 6 + c * 2
            to_down[at : at + 2, :] = vel[c, x, 0:2, :]
            to_up[at : at + 2, :] = vel[c, x, ny - 2 : ny, :]


def home_kernel(slot, both, vel, inner, rim, part, fcat, sums, tn, tt, sacc):
    markers = slot.shape[1]
    blocks = inner.shape[0]
    below = (slot[...] < markers).astype(F32)
    upto = (slot[...] < 2 * markers).astype(F32)
    count_inner = jnp.sum(below).astype(I32)
    count_rim = jnp.sum(upto - below).astype(I32)
    for t in range(blocks):
        inner[t] = jnp.zeros((ROWS, TILE), F32)
        rim[t] = jnp.zeros((ROWS, TILE), F32)

    def inner_tile(t, carry):
        inner[t] = gather_tile(both[...], slot[...], t)
        return carry

    def rim_tile(t, carry):
        rim[t] = gather_tile(both[...], slot[...], blocks + t)
        return carry

    lax.fori_loop(0, (count_inner + TILE - 1) // TILE, inner_tile, 0)
    lax.fori_loop(0, (count_rim + TILE - 1) // TILE, rim_tile, 0)

    nx = part.shape[0]
    cells = vel.shape[2]
    tall = cells + 4
    blank = jnp.zeros(part.shape[1:], F32)
    for x in range(nx):
        part[x] = blank
    fill_own(vel, part)

    def halve(x, carry):
        to_halves(part, fcat, x)
        return carry

    lax.fori_loop(0, nx, halve, 0)
    sums[...] = jnp.zeros(sums.shape, F32)
    process_tiles(0, EARLY, inner, fcat, part, sums, tn, tt, sacc, tall=tall)


def fill_own(vel, field):
    cells = vel.shape[2]

    def layer(x, carry):
        for c in range(3):
            field[x + 2, c * (cells + 4) + 2 : c * (cells + 4) + 2 + cells, :] = vel[c, x]
        return carry

    lax.fori_loop(0, vel.shape[1], layer, 0)


def to_halves(field, fcat, x):
    high, low = split(field[x])
    fcat[x, :, 0:256] = high
    fcat[x, :, 256:512] = low


def turn_kernel(
    where, got_a, got_b, middle, own_down, own_up, to_a, to_b, got_left, got_right, down, up, *, nx, ny
):
    sort_out(where[0], got_a, got_b, got_left, got_right)
    base = 6 * ny
    lists = (nx + 4) * 6
    for out, own, cut, pick, mid in (
        (down, own_down, 0, 0, 0),
        (up, own_up, ny - 2, 2, 1),
    ):
        out[0:lists, :] = own[0:lists, :]
        for x in range(2):
            for c in range(3):
                at = (c * 2 + x) * ny + cut
                to = x * 6 + c * 2
                out[to : to + 2, :] = got_right[at : at + 2, :]
                to = (nx + 2 + x) * 6 + c * 2
                out[to : to + 2, :] = got_left[at : at + 2, :]
        out[lists : lists + ROWS, :] = got_left[base + pick * ROWS : base + (pick + 1) * ROWS, :]
        out[lists + ROWS : lists + 2 * ROWS, :] = middle[mid]
        out[lists + 2 * ROWS : lists + 3 * ROWS, :] = (
            got_right[base + pick * ROWS : base + (pick + 1) * ROWS, :]
        )
    sort_out(where[1], up, down, to_a, to_b)


def chain(distance, rows):
    value = jnp.where(distance == 3, rows[3], jnp.zeros((), rows[3].dtype))
    for k in (2, 1, 0):
        value = jnp.where(distance == k, rows[k], value)
    return value


def process_tiles(first_tile, stop, lists, fcat, part, sums, tn, tt, sacc, *, tall):
    nx = part.shape[0]
    row = lax.broadcasted_iota(I32, (CYR, 1), 0)
    comp = (row >= tall).astype(I32) + (row >= 2 * tall).astype(I32)
    y_of = jnp.where(row < 3 * tall, row - comp * tall, -100)
    comp = jnp.where(row < 3 * tall, comp, 3)
    z_of = lax.broadcasted_iota(I32, (256, TILE), 0).astype(F32).astype(BF16)
    win_row = lax.broadcasted_iota(I32, (16, TILE), 0)
    group_of = lax.broadcasted_iota(I32, (128, TILE), 0)

    def tile_body(t, carry):
        rec = lists[t]
        valid = rec[22:23] > 0.5
        bxf = rec[12:13]
        x_first = jnp.min(jnp.where(valid, bxf, 99.0)).astype(I32)
        x_last = jnp.max(jnp.where(valid, bxf, -9.0)).astype(I32)
        layers = x_last - x_first + 4
        windows = jnp.where(x_last < 0, 0, (layers + WIN - 1) // WIN)

        @pl.when(windows > 0)
        def _():
            bxi = bxf.astype(I32)
            byi = rec[13:14].astype(I32)
            ahead = z_of - rec[14:15].astype(BF16)
            ahead = jnp.where(ahead < 0, ahead + 256, ahead)
            parts = [split(rec[8 + k : 9 + k]) for k in range(4)]
            high = chain(ahead, [p[0] for p in parts])
            low = chain(ahead, [p[1] for p in parts])
            tn[0:256, :] = high
            tn[256:512, :] = low
            tt[:, 0:256] = high
            tt[:, 256:512] = low
            table_y = chain(y_of - byi, [rec[4 + k : 5 + k] for k in range(4)])
            sacc[...] = jnp.zeros(sacc.shape, F32)

            def window(w, size):
                begin = x_first + w * size
                x0 = jnp.minimum(begin, nx - size)
                x_at = win_row + x0
                table_x = chain(x_at - bxi, [rec[k : k + 1] for k in range(4)])
                return x0, jnp.where(x_at >= begin, table_x, 0.0)

            def sample(w, size):
                x0, table_x = window(w, size)
                block_h = fcat[pl.ds(x0, size), :, 0:256].reshape(size * CYR, 256)
                block_l = fcat[pl.ds(x0, size), :, 256:512].reshape(size * CYR, 256)
                got = (
                    jnp.dot(block_h, tn[0:256], preferred_element_type=F32)
                    + jnp.dot(block_l, tn[0:256], preferred_element_type=F32)
                    + jnp.dot(block_h, tn[256:512], preferred_element_type=F32)
                )
                total = sacc[...]
                for i in range(size):
                    total = total + table_x[i : i + 1] * got[i * CYR : (i + 1) * CYR]
                sacc[...] = total

            def by_size(step):
                for size in SIZES:
                    fits = layers <= size
                    if size > SIZES[0]:
                        fits = jnp.logical_and(fits, layers > size - 1)
                    pl.when(fits)(functools.partial(step, 0, size))

                @pl.when(layers > SIZES[-1])
                def _():
                    def loop(w, c):
                        step(w, WIN)
                        return c

                    lax.fori_loop(0, windows, loop, 0)

            by_size(sample)
            weighted = sacc[...] * table_y
            force = [
                rec[15 + c : 16 + c]
                - jnp.sum(jnp.where(comp == c, weighted, 0.0), axis=0, keepdims=True)
                for c in range(3)
            ]
            by_row = jnp.where(comp == 0, force[0], jnp.where(comp == 1, force[1], force[2]))
            plane = table_y * by_row

            def deposit(w, size):
                x0, table_x = window(w, size)
                pieces = [split(table_x[i : i + 1] * plane) for i in range(size)]
                high_s = jnp.concatenate([p[0] for p in pieces], axis=0)
                low_s = jnp.concatenate([p[1] for p in pieces], axis=0)
                nt = (((1,), (1,)), ((), ()))
                made = (
                    lax.dot_general(high_s, tt[:, 0:256], nt, preferred_element_type=F32)
                    + lax.dot_general(low_s, tt[:, 0:256], nt, preferred_element_type=F32)
                    + lax.dot_general(high_s, tt[:, 256:512], nt, preferred_element_type=F32)
                )
                part[pl.ds(x0, size)] += made.reshape(size, CYR, 256)

            by_size(deposit)
            off = [rec[18 + c : 19 + c] for c in range(3)]
            turn = [
                off[1] * force[2] - off[2] * force[1],
                off[2] * force[0] - off[0] * force[2],
                off[0] * force[1] - off[1] * force[0],
            ]
            stack = jnp.concatenate(force + turn + [jnp.zeros((2, TILE), F32)], axis=0)
            group = (2.0 * rec[23:24] + rec[21:22]).astype(I32)
            member = (group_of == group).astype(F32).astype(BF16)
            found = lax.dot_general(
                member, halves(stack), (((1,), (1,)), ((), ())), preferred_element_type=F32
            )
            sums[:, 0:16] += found

        return carry

    lax.fori_loop(first_tile, stop, tile_body, 0)


def inner_kernel(lists, fcat, part_in, sums_in, part, sums, tn, tt, sacc, *, tall):
    del part_in
    del sums_in
    process_tiles(EARLY, lists.shape[0], lists, fcat, part, sums, tn, tt, sacc, tall=tall)


def couple_kernel(
    where, vel, got_xa, got_xb, got_ya, got_yb, rim, linear, sums_in, part_in,
    part, send_a, send_b, message,
    got_left, got_right, got_down, got_up, field, fcat, lists, arrived, tn, tt, sacc, sums,
):
    del part_in
    nx = vel.shape[1] + 4
    cells = vel.shape[2]
    tall = cells + 4
    sort_out(where[0], got_xa, got_xb, got_left, got_right)
    sort_out(where[1], got_ya, got_yb, got_down, got_up)
    zero_pad = jnp.zeros((CYR - 3 * tall, vel.shape[3]), F32)
    fill_own(vel, field)
    for x in range(2):
        for c in range(3):
            rows = pl.ds((c * 2 + x) * cells, cells)
            field[x, c * tall + 2 : c * tall + 2 + cells, :] = got_right[rows, :]
            field[nx - 2 + x, c * tall + 2 : c * tall + 2 + cells, :] = got_left[rows, :]
    for x in range(nx):
        for c in range(3):
            rows = pl.ds(x * 6 + c * 2, 2)
            field[x, c * tall : c * tall + 2, :] = got_up[rows, :]
            field[x, c * tall + 2 + cells : (c + 1) * tall, :] = got_down[rows, :]
        field[x, 3 * tall : CYR, :] = zero_pad

    def halve(x, carry):
        to_halves(field, fcat, x)
        return carry

    lax.fori_loop(0, nx, halve, 0)

    base = 6 * cells + ROWS
    after = nx * 6
    blocks = rim.shape[0]
    arrived[:, 0:TILE] = got_left[base : base + ROWS, :]
    arrived[:, TILE : 2 * TILE] = got_right[base : base + ROWS, :]
    for k in range(3):
        rows = pl.ds(after + k * ROWS, ROWS)
        arrived[:, (2 + k) * TILE : (3 + k) * TILE] = got_down[rows, :]
        arrived[:, (5 + k) * TILE : (6 + k) * TILE] = got_up[rows, :]
    for t in range(blocks):
        arrived[:, (8 + t) * TILE : (9 + t) * TILE] = rim[t]
    total_lanes = arrived.shape[1]
    lane_at = lax.broadcasted_iota(I32, (1, total_lanes), 1)
    list_at = 1 + lax.shift_right_logical(lane_at, TILE.bit_length() - 1)
    arrived[23:24, :] = jnp.where(list_at > 8, 0, list_at).astype(F32)
    valid_all = arrived[22:23, :] > 0.5
    count = jnp.sum(arrived[22:23, :]).astype(I32)
    used = 8 + (jnp.sum(arrived[22:23, 8 * TILE : total_lanes]).astype(I32) + TILE - 1) // TILE
    bin_all = jnp.where(valid_all, arrived[12:13, :].astype(I32), 17)
    slot = counting_ranks(bin_all, lambda b: 0 * b + total_lanes, 17)
    both = halves(arrived[...])
    for t in range(lists.shape[0]):
        lists[t] = jnp.zeros((ROWS, TILE), F32)
    tiles = (count + TILE - 1) // TILE

    reach = 0
    for size in (9, 10, 11, 12, 16):
        wanted = jnp.logical_and(used > reach, used <= size)
        reach = size

        def gather_some(t, carry, lanes=size * TILE):
            lists[t] = gather_tile(both[:, 0:lanes], slot[:, 0:lanes], t)
            return carry

        lax.fori_loop(0, jnp.where(wanted, tiles, 0), gather_some, 0)
    sums[...] = sums_in[...]
    process_tiles(0, tiles, lists, fcat, part, sums, tn, tt, sacc, tall=tall)
    lane_of = lax.broadcasted_iota(I32, (128, 128), 1)
    low_part = pltpu.roll(sums[...], 120, axis=1)
    joined = jnp.where(lane_of < 6, sums[...] + low_part, 0.0)
    line = linear[...] + joined[0:1]
    for k in range(1, 18):
        line = line + pltpu.roll(joined[k : k + 1], 6 * k, axis=1)
    message[...] = jnp.broadcast_to(line, message.shape)
    even = (where[0] & 1) == 0
    for x in range(6):
        send_a[x] = part[jnp.where(even, nx - 6, 0) + x]
        send_b[x] = part[jnp.where(even, 0, nx - 6) + x]


def motion_kernel(
    where, contact_own, contact_other, angular, got, out, moved, *, gx, gy, per_sphere
):
    here = where[0] * gy + where[1]
    data = got[...]
    total = jnp.zeros(data.shape, F32)
    devices = gx * gy
    for k, (dx, dy) in enumerate(TRAVEL):
        piece = data
        shift = (-(gy * dx + dy)) % devices
        if shift:
            piece = pltpu.roll(piece, shift, axis=0)
        if k:
            piece = pltpu.roll(piece, 128 - 12 * k, axis=1)
        total = total + piece
    linear = pltpu.roll(data, 128 - 108, axis=1)
    moved[...] = linear - (RESPONSE / per_sphere) * total
    lane = lax.broadcasted_iota(I32, (1, 128), 1)
    mine = moved[pl.ds(here, 1), :]
    spring = jnp.zeros((1, 128), F32)
    for k in range(contact_own.shape[0]):
        partner = contact_other[k]
        line = moved[pl.ds(lax.shift_right_logical(partner, 1), 1), :]
        local = contact_own[k] - here * 2
        which = partner & 1
        same = jnp.where(which == local, line, 0.0)
        higher = jnp.where(which < local, pltpu.roll(line, 6, axis=1), 0.0)
        lower = jnp.where(which > local, pltpu.roll(line, 122, axis=1), 0.0)
        of_own = jnp.logical_and(lane >= local * 6, lane < local * 6 + 3)
        spring = spring + jnp.where(of_own, same + higher + lower - mine, 0.0)
    result = mine + DASHPOT * spring
    out[0:1, :] = result[:, 0:6] + angular[0:1, :]
    out[1:2, :] = pltpu.roll(result, 122, axis=1)[:, 0:6] + angular[1:2, :]


def edges_kernel(where, part, got_a, got_b, to_a, to_b, *, tall):
    nx = part.shape[0]
    even = (where[0] & 1) == 0
    even_y = (where[1] & 1) == 0
    for x in range(nx + 4):
        for c in range(3):
            values = []
            for at in (c * tall, (c + 1) * tall - 6):
                rows = pl.ds(at, 6)
                pieces = []
                if 2 <= x < nx + 2:
                    pieces.append(part[x - 2, rows, :])
                if x < 6:
                    pieces.append(jnp.where(even, got_b[x, rows, :], got_a[x, rows, :]))
                if x >= nx - 2:
                    y = x - (nx - 2)
                    pieces.append(jnp.where(even, got_a[y, rows, :], got_b[y, rows, :]))
                total = pieces[0]
                for piece in pieces[1:]:
                    total = total + piece
                values.append(total)
            to = pl.ds(x * 18 + c * 6, 6)
            to_a[to, :] = jnp.where(even_y, values[1], values[0])
            to_b[to, :] = jnp.where(even_y, values[0], values[1])


def middle_kernel(where, part, got_a, got_b, rhs, *, tall):
    nx = part.shape[0]
    long = nx + 4
    high_y = tall + 4
    even = (where[0] & 1) == 0
    zero2 = jnp.zeros((2, 256), F32)

    def fill(x, sources):
        for c in range(3):
            rows_of = pl.ds(c * tall, tall)
            total = sources[0](rows_of)
            for source in sources[1:]:
                total = total + source(rows_of)
            rhs[c, x, 0:2, :] = zero2
            rhs[c, x, high_y - 2 : high_y, :] = zero2
            rhs[c, x, 2 : 2 + tall, :] = total

    def from_part(at):
        return lambda rows_of: part[at, rows_of, :]

    def chosen(at, first, second):
        return lambda rows_of: jnp.where(even, first[at, rows_of, :], second[at, rows_of, :])

    for x in range(6):
        fill(x, [chosen(x, got_b, got_a)] + ([from_part(x - 2)] if x >= 2 else []))
        fill(
            long - 6 + x,
            [chosen(x, got_a, got_b)] + ([from_part(nx - 4 + x)] if x < 4 else []),
        )

    def centre(x, carry):
        fill(x, [from_part(x - 2)])
        return carry

    lax.fori_loop(6, long - 6, centre, 0)


def relax_kernel(where, grown, got_a, got_b, out_h, rhs, va, vb, low, high, out, sems, *, rows):
    long, high_y = grown.shape[1:3]
    span = high_y - 8
    nx = long - 8
    sort_out(where[1], got_b, got_a, low, high)
    y_at = lax.broadcasted_iota(I32, (high_y, 1), 0) - 4 + where[1] * span
    inside = jnp.logical_and(y_at >= 0, y_at < rows)
    mask = jnp.broadcast_to(inside.astype(F32), (high_y, 256))
    factor = jnp.broadcast_to(
        jnp.where(inside, 1.0 / (1.0 + 6.0 * DIFFUSION), 0.0), (high_y, 256)
    )
    gap = jnp.zeros((high_y - 12, 256), F32)
    for x in range(long):
        for c in range(3):
            at = pl.ds(x * 18 + c * 6, 6)
            edge = jnp.concatenate([low[at, :], gap, high[at, :]], axis=0)
            rhs[c, x] = (grown[c, x] + edge) * mask

    state = rhs
    for sweep in range(ITERS):
        target = (va, vb)[sweep % 2]
        last = sweep == ITERS - 1

        def layer(x, state=state, target=target, last=last):
            for c in range(3):
                here = state[c, x]
                near = state[c, x - 1] + state[c, x + 1]
                near = near + (pltpu.roll(here, 1, axis=1) + pltpu.roll(here, 255, axis=1))
                near = near + (pltpu.roll(here, 1, axis=0) + pltpu.roll(here, high_y - 1, axis=0))
                new = (rhs[c, x] + DIFFUSION * near) * factor
                if last:
                    out[c, x - 4] = new[4 : high_y - 4]
                else:
                    target[c, x] = new

        def group(g, carry, sweep=sweep, layer=layer, last=last):
            for k in range(UNROLL):
                layer(jnp.minimum(sweep + 1 + g * UNROLL + k, long - 2 - sweep))
            if last:
                for c in range(3):
                    part = pl.ds(g * UNROLL, UNROLL)
                    pltpu.make_async_copy(out.at[c, part], out_h.at[c, part], sems.at[g * 3 + c]).start()
            return carry

        lax.fori_loop(0, (long - 2 - 2 * sweep + UNROLL - 1) // UNROLL, group, 0)
        state = target
    for g in range(nx // UNROLL):
        for c in range(3):
            part = pl.ds(g * UNROLL, UNROLL)
            pltpu.make_async_copy(out.at[c, part], out_h.at[c, part], sems.at[g * 3 + c]).wait()


def on_device(
    velocity,
    owner_block,
    base_x,
    base_y,
    base_z,
    delta_weights,
    marker_offset,
    sphere_motion,
    contact_sphere,
    contact_partner,
):
    nx, ny, nz = velocity.shape[1:]
    gx = lax.axis_size("gx")
    gy = lax.axis_size("gy")
    where = jnp.stack([lax.axis_index("gx"), lax.axis_index("gy")]).astype(I32)
    markers = base_x.shape[0]
    spheres = sphere_motion.shape[1]
    per_sphere = markers // spheres
    blocks = markers // TILE
    tall = ny + 4

    def pairs(size, first, wrap):
        both_ways = []
        for i in range(first, size, 2):
            j = (i + 1) % size
            if j or wrap:
                both_ways += [(i, j), (j, i)]
        return both_ways

    def swap_x(first, second):
        return (
            lax.ppermute(first, "gx", pairs(gx, 0, True)),
            lax.ppermute(second, "gx", pairs(gx, 1, True)),
        )

    def swap_y(first, second):
        return (
            lax.ppermute(first, "gy", pairs(gy, 0, False)),
            lax.ppermute(second, "gy", pairs(gy, 1, False)),
        )


    def array(*shape, dtype=F32):
        return jax.ShapeDtypeStruct(shape, dtype)

    x_rows = 6 * ny + 3 * ROWS
    y_rows = 6 * (nx + 4) + 3 * ROWS
    to_a, to_b, middle, own_down, own_up, slot, both, linear, vel = pl.pallas_call(
        functools.partial(route_kernel, gx=gx, gy_shift=gy.bit_length() - 1),
        out_shape=(
            array(x_rows, nz),
            array(x_rows, nz),
            array(2, ROWS, TILE),
            array(y_rows, nz),
            array(y_rows, nz),
            array(1, markers, dtype=I32),
            array(2 * ROWS, markers, dtype=BF16),
            array(1, 128),
            array(3, nx, ny, nz),
        ),
        in_specs=[SMEM] + [HBM] * 8,
        out_specs=(VMEM,) * 9,
        scratch_shapes=[
            pltpu.SMEM((spheres, 6), F32),
            pltpu.VMEM((1, markers), I32),
            pltpu.VMEM((1, markers), I32),
            pltpu.VMEM((1, markers), I32),
            pltpu.VMEM((1, markers), I32),
            pltpu.VMEM((12, markers), F32),
            pltpu.VMEM((3, markers), F32),
            pltpu.VMEM((ROWS, markers), F32),
            pltpu.SemaphoreType.DMA((7,)),
            pltpu.SemaphoreType.DMA((1,)),
        ],
        compiler_params=params(16),
        name="route",
    )(
        where,
        *(
            pltpu.with_memory_space_constraint(a, pltpu.HBM)
            for a in (
                sphere_motion.T,
                owner_block.reshape(1, markers),
                base_x.reshape(1, markers),
                base_y.reshape(1, markers),
                base_z.reshape(1, markers),
                delta_weights,
                marker_offset,
                velocity,
            )
        ),
    )
    got_xa, got_xb = swap_x(to_a, to_b)
    field = array(nx + 4, CYR, nz)
    halved = array(nx + 4, CYR, 2 * nz, dtype=BF16)
    lists = array(blocks, ROWS, TILE)
    tile_scratch = [
        pltpu.VMEM((2 * nz, TILE), BF16),
        pltpu.VMEM((nz, 2 * TILE), BF16),
        pltpu.VMEM((CYR, TILE), F32),
    ]
    inner, rim, part, fcat, sums = pl.pallas_call(
        home_kernel,
        out_shape=(lists, lists, field, halved, array(128, 128)),
        in_specs=[VMEM] * 3,
        out_specs=(VMEM,) * 5,
        scratch_shapes=tile_scratch,
        compiler_params=params(8),
        cost_estimate=pl.CostEstimate(flops=2_000_000_000, bytes_accessed=0, transcendentals=0),
        name="home",
    )(slot, both, vel)
    part, sums = pl.pallas_call(
        functools.partial(inner_kernel, tall=tall),
        out_shape=(field, array(128, 128)),
        in_specs=[VMEM] * 4,
        out_specs=(VMEM,) * 2,
        input_output_aliases={2: 0, 3: 1},
        scratch_shapes=tile_scratch,
        compiler_params=params(8),
        cost_estimate=pl.CostEstimate(flops=4_000_000_000, bytes_accessed=0, transcendentals=0),
        name="inner",
    )(inner, fcat, part, sums)
    x_buffer = pltpu.VMEM((x_rows, nz), F32)
    y_buffer = pltpu.VMEM((y_rows, nz), F32)
    got_ya, got_yb = swap_y(
        *pl.pallas_call(
            functools.partial(turn_kernel, nx=nx, ny=ny),
            out_shape=(array(y_rows, nz),) * 2,
            in_specs=[SMEM] + [VMEM] * 5,
            out_specs=(VMEM,) * 2,
            scratch_shapes=[x_buffer, x_buffer, y_buffer, y_buffer],
            compiler_params=params(4),
            name="turn",
        )(where, got_xa, got_xb, middle, own_down, own_up)
    )

    devices = gx * gy
    slab = array(6, CYR, nz)
    part, send_a, send_b, message = pl.pallas_call(
        couple_kernel,
        out_shape=(field, slab, slab, array(devices, 128)),
        in_specs=[SMEM] + [VMEM] * 9,
        out_specs=(VMEM,) * 4,
        input_output_aliases={9: 0},
        scratch_shapes=[
            x_buffer,
            x_buffer,
            y_buffer,
            y_buffer,
            pltpu.VMEM(field.shape, F32),
            pltpu.VMEM(halved.shape, BF16),
            pltpu.VMEM((2 * blocks, ROWS, TILE), F32),
            pltpu.VMEM((ROWS, 2 * markers), F32),
            *tile_scratch,
            pltpu.VMEM((128, 128), F32),
        ],
        compiler_params=params(16),
        name="couple",
    )(where, vel, got_xa, got_xb, got_ya, got_yb, rim, linear, sums, part)

    got_a, got_b = swap_x(send_a, send_b)
    everyone = lax.all_to_all(message, ("gx", "gy"), 0, 0, tiled=True)
    strip = array((nx + 8) * 18, nz)
    everyone, part = lax.optimization_barrier((everyone, part))
    strip_buffer = pltpu.VMEM(strip.shape, F32)
    to_ya, to_yb = pl.pallas_call(
        functools.partial(edges_kernel, tall=tall),
        out_shape=(strip, strip),
        in_specs=[SMEM] + [VMEM] * 3,
        out_specs=(VMEM,) * 2,
        compiler_params=params(4),
        name="edges",
    )(where, part, got_a, got_b)
    angular = jnp.concatenate([jnp.zeros((3, spheres), F32), sphere_motion[3:6]], axis=0).T
    new_motion = pl.pallas_call(
        functools.partial(motion_kernel, gx=gx, gy=gy, per_sphere=per_sphere),
        out_shape=array(spheres, 6),
        in_specs=[SMEM] * 3 + [VMEM] * 2,
        out_specs=VMEM,
        scratch_shapes=[pltpu.VMEM((devices, 128), F32)],
        compiler_params=params(4),
        name="motion",
    )(where, contact_sphere, contact_partner, angular, everyone).T
    got_ea, got_eb = swap_y(to_ya, to_yb)
    grown = pl.pallas_call(
        functools.partial(middle_kernel, tall=tall),
        out_shape=array(3, nx + 8, tall + 4, nz),
        in_specs=[SMEM] + [VMEM] * 3,
        out_specs=VMEM,
        compiler_params=params(4),
        cost_estimate=pl.CostEstimate(flops=2_000_000_000, bytes_accessed=0, transcendentals=0),
        name="middle",
    )(where, part, got_a, got_b)
    buffer = pltpu.VMEM(grown.shape, F32)
    state = pl.pallas_call(
        functools.partial(relax_kernel, rows=ny * gy),
        out_shape=array(3, nx, ny, nz),
        in_specs=[SMEM] + [VMEM] * 3,
        out_specs=HBM,
        scratch_shapes=[
            buffer,
            buffer,
            buffer,
            strip_buffer,
            strip_buffer,
            pltpu.VMEM((3, nx, ny, nz), F32),
            pltpu.SemaphoreType.DMA((3 * (nx // UNROLL),)),
        ],
        compiler_params=params(20),
        name="relax",
    )(where, grown, got_ea, got_eb)
    return (state, new_motion)


def solution(mesh):
    placed = (
        P(None, "gx", "gy", None),
        P(("gx", "gy"), None),
        P(("gx", "gy")),
        P(("gx", "gy")),
        P(("gx", "gy")),
        P(None, ("gx", "gy")),
        P(None, ("gx", "gy")),
        P(None, ("gx", "gy")),
        P(("gx", "gy")),
        P(("gx", "gy")),
    )
    return jax.shard_map(
        on_device,
        mesh=mesh,
        in_specs=placed,
        out_specs=(P(None, "gx", "gy", None), P(None, ("gx", "gy"))),
        check_vma=False,
    )
```

```python
import functools

import jax
import jax.numpy as jnp
from jax import lax
from jax.experimental import pallas as pl
from jax.experimental.pallas import tpu as pltpu
from jax.sharding import PartitionSpec as P

F32 = jnp.float32
BF16 = jnp.bfloat16
I32 = jnp.int32

ITERS = 4
DIFFUSION = 1.0
RESPONSE = 0.5
DASHPOT = 0.1

ROWS = 24
TILE = 256
UNROLLS = (11, 10, 9, 4)
UNROLL = UNROLLS[-1]
EARLY = 2
SIZES = (6, 7, 8, 9)
WIN = 10
CYR = 112


TRAVEL = ((0, 0), (-1, 0), (1, 0), (-1, -1), (0, -1), (1, -1), (-1, 1), (0, 1), (1, 1))

VMEM = pl.BlockSpec(memory_space=pltpu.VMEM)
SMEM = pl.BlockSpec(memory_space=pltpu.SMEM)
HBM = pl.BlockSpec(memory_space=pltpu.HBM)


def params(mib):
    return pltpu.CompilerParams(vmem_limit_bytes=mib * 1024 * 1024)


def split(value):
    high = value.astype(BF16)
    low = (value - high.astype(F32)).astype(BF16)
    return high, low


def counting_ranks(bin_of, start_of, bins_here):
    markers = bin_of.shape[1]
    bins = (lax.broadcasted_iota(I32, (32, markers), 0) == bin_of).astype(F32)
    bins16 = bins.astype(BF16)
    ramp_i = lax.broadcasted_iota(I32, (TILE, TILE), 0)
    ramp_j = lax.broadcasted_iota(I32, (TILE, TILE), 1)
    upper = (ramp_i < ramp_j).astype(F32).astype(BF16)
    totals = lax.dot_general(
        jnp.ones((8, markers), BF16), bins16, (((1,), (1,)), ((), ())), preferred_element_type=F32
    )
    row = lax.broadcasted_iota(I32, (32, 32), 0)
    col = lax.broadcasted_iota(I32, (32, 32), 1)
    before = jnp.where(jnp.logical_and(col < row, row < bins_here), totals[0:1, :], 0.0)
    bin_row = lax.broadcasted_iota(I32, (32, 1), 0)
    start = jnp.where(
        bin_row < bins_here, jnp.sum(before, axis=1, keepdims=True), start_of(bin_row).astype(F32)
    )
    slots = []
    for b in range(markers // TILE):
        mine = bins[:, b * TILE : (b + 1) * TILE]
        ranks = jnp.dot(bins16[:, b * TILE : (b + 1) * TILE], upper, preferred_element_type=F32)
        slots.append(jnp.sum(mine * (ranks + start), axis=0, keepdims=True))
        start = start + jnp.sum(mine, axis=1, keepdims=True)
    return jnp.concatenate(slots, axis=1).astype(I32)


def gather_tile(both, slot, tile):
    place = lax.broadcasted_iota(I32, (TILE, slot.shape[1]), 0).astype(F32).astype(BF16)
    local = jnp.clip(slot - tile * TILE, -1, TILE).astype(F32).astype(BF16)
    pick = jnp.where(place == local, jnp.ones((), BF16), jnp.zeros((), BF16))
    out = lax.dot_general(both, pick, (((1,), (1,)), ((), ())), preferred_element_type=F32)
    return out[0:ROWS] + out[ROWS : 2 * ROWS]


def sort_out(index, first, second, out_first, out_second):
    even = (index & 1) == 0
    out_first[...] = jnp.where(even, first[...], second[...])
    out_second[...] = jnp.where(even, second[...], first[...])


def halves(value):
    high, low = split(value)
    return jnp.concatenate([high.astype(F32), low.astype(F32)], axis=0).astype(BF16)


def route_kernel(
    where, motion_h, owner_h, bx_h, by_h, bz_h, weights_h, offset_h, velocity_h,
    to_a, to_b, middle, to_down, to_up, slot_out, both_out, linear, vel,
    motion, owner, bx, by, bz, weights, offset, rec, sems, edge_sem, *, gx, gy_shift
):
    markers = owner.shape[1]
    blocks = markers // TILE
    nx, ny = vel.shape[1:3]
    moves = []
    for k, (src, dst) in enumerate(
        (
            (owner_h, owner),
            (bx_h, bx),
            (by_h, by),
            (bz_h, bz),
            (weights_h, weights),
            (offset_h, offset),
            (motion_h, motion),
        )
    ):
        move = pltpu.make_async_copy(src, dst, sems.at[k])
        move.start()
        moves.append(move)
    whole = pltpu.make_async_copy(velocity_h, vel, edge_sem.at[0])
    whole.start()
    for move in moves:
        move.wait()
    own = owner[...]
    step_x = (lax.shift_right_logical(own, gy_shift) - where[0] + 1) & (gx - 1)
    step_y = (own & ((1 << gy_shift) - 1)) - where[1] + 1
    lane = step_x * 3 + step_y
    x_in = jnp.logical_and(bx[...] >= 2, bx[...] <= nx - 2)
    y_in = jnp.logical_and(by[...] >= 2, by[...] <= ny - 2)
    at_home = jnp.where(jnp.logical_and(x_in, y_in), bx[...], 17)
    bin_of = jnp.where(lane == 4, at_home, 18 + lane)
    slot = counting_ranks(
        bin_of, lambda b: jnp.where(b == 17, markers, 2 * markers + (b - 18) * TILE), 17
    )
    slot_out[...] = slot

    first = lax.broadcasted_iota(I32, (1, markers), 1) < markers // 2
    speed = [jnp.where(first, motion[0, c], motion[1, c]) for c in range(6)]
    off = [offset[c : c + 1, :] for c in range(3)]
    target = [
        speed[0] + (speed[4] * off[2] - speed[5] * off[1]),
        speed[1] + (speed[5] * off[0] - speed[3] * off[2]),
        speed[2] + (speed[3] * off[1] - speed[4] * off[0]),
    ]
    rec[0:12, :] = weights[...]
    rec[12:13, :] = bx[...].astype(F32)
    rec[13:14, :] = by[...].astype(F32)
    rec[14:15, :] = bz[...].astype(F32)
    for c in range(3):
        rec[15 + c : 16 + c, :] = target[c]
    rec[18:21, :] = offset[...]
    rec[21:22, :] = jnp.where(first, 0.0, 1.0)
    rec[22:23, :] = jnp.ones((1, markers), F32)
    rec[23:24, :] = jnp.zeros((1, markers), F32)
    both = halves(rec[...])
    both_out[...] = both
    base = 6 * ny
    even = (where[0] & 1) == 0
    for ref, up in ((to_a, even), (to_b, jnp.logical_not(even))):
        tile = 2 * blocks + jnp.where(up, 6, 0)
        for k in range(3):
            ref[base + k * ROWS : base + (k + 1) * ROWS, :] = gather_tile(both, slot, tile + k)
    middle[0] = gather_tile(both, slot, 2 * blocks + 3)
    middle[1] = gather_tile(both, slot, 2 * blocks + 5)

    lane_row = lax.broadcasted_iota(I32, (1, 128), 1)
    line = jnp.zeros((1, 128), F32)
    for s in range(2):
        for c in range(3):
            line = jnp.where(lane_row == 108 + 6 * s + c, motion[s, c], line)
    linear[...] = line
    whole.wait()
    for c in range(3):
        for x in range(2):
            rows = pl.ds((c * 2 + x) * ny, ny)
            to_a[rows, :] = vel[c, jnp.where(even, nx - 2, 0) + x]
            to_b[rows, :] = vel[c, jnp.where(even, 0, nx - 2) + x]

    for x in range(nx):
        for c in range(3):
            at = (x + 2) * 6 + c * 2
            to_down[at : at + 2, :] = vel[c, x, 0:2, :]
            to_up[at : at + 2, :] = vel[c, x, ny - 2 : ny, :]


def home_kernel(slot, both, vel, inner, rim, part, fcat, sums, tn, tt, sacc):
    markers = slot.shape[1]
    blocks = inner.shape[0]
    below = (slot[...] < markers).astype(F32)
    upto = (slot[...] < 2 * markers).astype(F32)
    count_inner = jnp.sum(below).astype(I32)
    count_rim = jnp.sum(upto - below).astype(I32)
    for t in range(blocks):
        inner[t] = jnp.zeros((ROWS, TILE), F32)
        rim[t] = jnp.zeros((ROWS, TILE), F32)

    def inner_tile(t, carry):
        inner[t] = gather_tile(both[...], slot[...], t)
        return carry

    def rim_tile(t, carry):
        rim[t] = gather_tile(both[...], slot[...], blocks + t)
        return carry

    lax.fori_loop(0, (count_inner + TILE - 1) // TILE, inner_tile, 0)
    lax.fori_loop(0, (count_rim + TILE - 1) // TILE, rim_tile, 0)

    nx = part.shape[0]
    cells = vel.shape[2]
    tall = cells + 4
    blank = jnp.zeros(part.shape[1:], F32)
    for x in range(nx):
        part[x] = blank
    fill_own(vel, part)

    def halve(x, carry):
        to_halves(part, fcat, x)
        return carry

    lax.fori_loop(0, nx, halve, 0)
    sums[...] = jnp.zeros(sums.shape, F32)
    process_tiles(0, EARLY, inner, fcat, part, sums, tn, tt, sacc, tall=tall)


def fill_own(vel, field):
    cells = vel.shape[2]

    def layer(x, carry):
        for c in range(3):
            field[x + 2, c * (cells + 4) + 2 : c * (cells + 4) + 2 + cells, :] = vel[c, x]
        return carry

    lax.fori_loop(0, vel.shape[1], layer, 0)


def to_halves(field, fcat, x):
    high, low = split(field[x])
    fcat[x, :, 0:256] = high
    fcat[x, :, 256:512] = low


def turn_kernel(
    where, got_a, got_b, middle, own_down, own_up, to_a, to_b, got_left, got_right, down, up, *, nx, ny
):
    sort_out(where[0], got_a, got_b, got_left, got_right)
    base = 6 * ny
    lists = (nx + 4) * 6
    for out, own, cut, pick, mid in (
        (down, own_down, 0, 0, 0),
        (up, own_up, ny - 2, 2, 1),
    ):
        out[0:lists, :] = own[0:lists, :]
        for x in range(2):
            for c in range(3):
                at = (c * 2 + x) * ny + cut
                to = x * 6 + c * 2
                out[to : to + 2, :] = got_right[at : at + 2, :]
                to = (nx + 2 + x) * 6 + c * 2
                out[to : to + 2, :] = got_left[at : at + 2, :]
        out[lists : lists + ROWS, :] = got_left[base + pick * ROWS : base + (pick + 1) * ROWS, :]
        out[lists + ROWS : lists + 2 * ROWS, :] = middle[mid]
        out[lists + 2 * ROWS : lists + 3 * ROWS, :] = (
            got_right[base + pick * ROWS : base + (pick + 1) * ROWS, :]
        )
    sort_out(where[1], up, down, to_a, to_b)


def chain(distance, rows):
    value = jnp.where(distance == 3, rows[3], jnp.zeros((), rows[3].dtype))
    for k in (2, 1, 0):
        value = jnp.where(distance == k, rows[k], value)
    return value


def process_tiles(first_tile, stop, lists, fcat, part, sums, tn, tt, sacc, *, tall):
    nx = part.shape[0]
    row = lax.broadcasted_iota(I32, (CYR, 1), 0)
    comp = (row >= tall).astype(I32) + (row >= 2 * tall).astype(I32)
    y_of = jnp.where(row < 3 * tall, row - comp * tall, -100)
    comp = jnp.where(row < 3 * tall, comp, 3)
    z_of = lax.broadcasted_iota(I32, (256, TILE), 0).astype(F32).astype(BF16)
    win_row = lax.broadcasted_iota(I32, (16, TILE), 0)
    group_of = lax.broadcasted_iota(I32, (128, TILE), 0)

    def tile_body(t, carry):
        rec = lists[t]
        valid = rec[22:23] > 0.5
        bxf = rec[12:13]
        x_first = jnp.min(jnp.where(valid, bxf, 99.0)).astype(I32)
        x_last = jnp.max(jnp.where(valid, bxf, -9.0)).astype(I32)
        layers = x_last - x_first + 4
        windows = jnp.where(x_last < 0, 0, (layers + WIN - 1) // WIN)

        @pl.when(windows > 0)
        def _():
            bxi = bxf.astype(I32)
            byi = rec[13:14].astype(I32)
            ahead = z_of - rec[14:15].astype(BF16)
            ahead = jnp.where(ahead < 0, ahead + 256, ahead)
            parts = [split(rec[8 + k : 9 + k]) for k in range(4)]
            high = chain(ahead, [p[0] for p in parts])
            low = chain(ahead, [p[1] for p in parts])
            tn[0:256, :] = high
            tn[256:512, :] = low
            tt[:, 0:256] = high
            tt[:, 256:512] = low
            table_y = chain(y_of - byi, [rec[4 + k : 5 + k] for k in range(4)])
            sacc[...] = jnp.zeros(sacc.shape, F32)

            def window(w, size):
                begin = x_first + w * size
                x0 = jnp.minimum(begin, nx - size)
                x_at = win_row + x0
                table_x = chain(x_at - bxi, [rec[k : k + 1] for k in range(4)])
                return x0, jnp.where(x_at >= begin, table_x, 0.0)

            def sample(w, size):
                x0, table_x = window(w, size)
                block_h = fcat[pl.ds(x0, size), :, 0:256].reshape(size * CYR, 256)
                block_l = fcat[pl.ds(x0, size), :, 256:512].reshape(size * CYR, 256)
                got = (
                    jnp.dot(block_h, tn[0:256], preferred_element_type=F32)
                    + jnp.dot(block_l, tn[0:256], preferred_element_type=F32)
                    + jnp.dot(block_h, tn[256:512], preferred_element_type=F32)
                )
                total = sacc[...]
                for i in range(size):
                    total = total + table_x[i : i + 1] * got[i * CYR : (i + 1) * CYR]
                sacc[...] = total

            def by_size(step):
                for size in SIZES:
                    fits = layers <= size
                    if size > SIZES[0]:
                        fits = jnp.logical_and(fits, layers > size - 1)
                    pl.when(fits)(functools.partial(step, 0, size))

                @pl.when(layers > SIZES[-1])
                def _():
                    def loop(w, c):
                        step(w, WIN)
                        return c

                    lax.fori_loop(0, windows, loop, 0)

            by_size(sample)
            weighted = sacc[...] * table_y
            force = [
                rec[15 + c : 16 + c]
                - jnp.sum(jnp.where(comp == c, weighted, 0.0), axis=0, keepdims=True)
                for c in range(3)
            ]
            by_row = jnp.where(comp == 0, force[0], jnp.where(comp == 1, force[1], force[2]))
            plane = table_y * by_row

            def deposit(w, size):
                x0, table_x = window(w, size)
                pieces = [split(table_x[i : i + 1] * plane) for i in range(size)]
                high_s = jnp.concatenate([p[0] for p in pieces], axis=0)
                low_s = jnp.concatenate([p[1] for p in pieces], axis=0)
                nt = (((1,), (1,)), ((), ()))
                made = (
                    lax.dot_general(high_s, tt[:, 0:256], nt, preferred_element_type=F32)
                    + lax.dot_general(low_s, tt[:, 0:256], nt, preferred_element_type=F32)
                    + lax.dot_general(high_s, tt[:, 256:512], nt, preferred_element_type=F32)
                )
                part[pl.ds(x0, size)] += made.reshape(size, CYR, 256)

            by_size(deposit)
            off = [rec[18 + c : 19 + c] for c in range(3)]
            turn = [
                off[1] * force[2] - off[2] * force[1],
                off[2] * force[0] - off[0] * force[2],
                off[0] * force[1] - off[1] * force[0],
            ]
            stack = jnp.concatenate(force + turn + [jnp.zeros((2, TILE), F32)], axis=0)
            group = (2.0 * rec[23:24] + rec[21:22]).astype(I32)
            member = (group_of == group).astype(F32).astype(BF16)
            found = lax.dot_general(
                member, halves(stack), (((1,), (1,)), ((), ())), preferred_element_type=F32
            )
            sums[:, 0:16] += found

        return carry

    lax.fori_loop(first_tile, stop, tile_body, 0)


def inner_kernel(lists, fcat, part_in, sums_in, part, sums, tn, tt, sacc, *, tall):
    del part_in
    del sums_in
    process_tiles(EARLY, lists.shape[0], lists, fcat, part, sums, tn, tt, sacc, tall=tall)


def couple_kernel(
    where, vel, got_xa, got_xb, got_ya, got_yb, rim, linear, sums_in, part_in,
    part, send_a, send_b, message,
    got_left, got_right, got_down, got_up, field, fcat, lists, arrived, tn, tt, sacc, sums,
):
    del part_in
    nx = vel.shape[1] + 4
    cells = vel.shape[2]
    tall = cells + 4
    sort_out(where[0], got_xa, got_xb, got_left, got_right)
    sort_out(where[1], got_ya, got_yb, got_down, got_up)
    zero_pad = jnp.zeros((CYR - 3 * tall, vel.shape[3]), F32)
    fill_own(vel, field)
    for x in range(2):
        for c in range(3):
            rows = pl.ds((c * 2 + x) * cells, cells)
            field[x, c * tall + 2 : c * tall + 2 + cells, :] = got_right[rows, :]
            field[nx - 2 + x, c * tall + 2 : c * tall + 2 + cells, :] = got_left[rows, :]
    for x in range(nx):
        for c in range(3):
            rows = pl.ds(x * 6 + c * 2, 2)
            field[x, c * tall : c * tall + 2, :] = got_up[rows, :]
            field[x, c * tall + 2 + cells : (c + 1) * tall, :] = got_down[rows, :]
        field[x, 3 * tall : CYR, :] = zero_pad

    def halve(x, carry):
        to_halves(field, fcat, x)
        return carry

    lax.fori_loop(0, nx, halve, 0)

    base = 6 * cells + ROWS
    after = nx * 6
    blocks = rim.shape[0]
    arrived[:, 0:TILE] = got_left[base : base + ROWS, :]
    arrived[:, TILE : 2 * TILE] = got_right[base : base + ROWS, :]
    for k in range(3):
        rows = pl.ds(after + k * ROWS, ROWS)
        arrived[:, (2 + k) * TILE : (3 + k) * TILE] = got_down[rows, :]
        arrived[:, (5 + k) * TILE : (6 + k) * TILE] = got_up[rows, :]
    for t in range(blocks):
        arrived[:, (8 + t) * TILE : (9 + t) * TILE] = rim[t]
    total_lanes = arrived.shape[1]
    lane_at = lax.broadcasted_iota(I32, (1, total_lanes), 1)
    list_at = 1 + lax.shift_right_logical(lane_at, TILE.bit_length() - 1)
    arrived[23:24, :] = jnp.where(list_at > 8, 0, list_at).astype(F32)
    valid_all = arrived[22:23, :] > 0.5
    count = jnp.sum(arrived[22:23, :]).astype(I32)
    used = 8 + (jnp.sum(arrived[22:23, 8 * TILE : total_lanes]).astype(I32) + TILE - 1) // TILE
    bin_all = jnp.where(valid_all, arrived[12:13, :].astype(I32), 17)
    slot = counting_ranks(bin_all, lambda b: 0 * b + total_lanes, 17)
    both = halves(arrived[...])
    for t in range(lists.shape[0]):
        lists[t] = jnp.zeros((ROWS, TILE), F32)
    tiles = (count + TILE - 1) // TILE

    reach = 0
    for size in (9, 10, 11, 12, 16):
        wanted = jnp.logical_and(used > reach, used <= size)
        reach = size

        def gather_some(t, carry, lanes=size * TILE):
            lists[t] = gather_tile(both[:, 0:lanes], slot[:, 0:lanes], t)
            return carry

        lax.fori_loop(0, jnp.where(wanted, tiles, 0), gather_some, 0)
    sums[...] = sums_in[...]
    process_tiles(0, tiles, lists, fcat, part, sums, tn, tt, sacc, tall=tall)
    lane_of = lax.broadcasted_iota(I32, (128, 128), 1)
    low_part = pltpu.roll(sums[...], 120, axis=1)
    joined = jnp.where(lane_of < 6, sums[...] + low_part, 0.0)
    line = linear[...] + joined[0:1]
    for k in range(1, 18):
        line = line + pltpu.roll(joined[k : k + 1], 6 * k, axis=1)
    message[...] = jnp.broadcast_to(line, message.shape)
    even = (where[0] & 1) == 0
    for x in range(6):
        rows = pl.ds(x * 3 * tall, 3 * tall)
        send_a[rows, :] = part[jnp.where(even, nx - 6, 0) + x, 0 : 3 * tall, :]
        send_b[rows, :] = part[jnp.where(even, 0, nx - 6) + x, 0 : 3 * tall, :]


def motion_kernel(
    where, contact_own, contact_other, angular, got, out, moved, *, gx, gy, per_sphere
):
    here = where[0] * gy + where[1]
    data = got[...]
    total = jnp.zeros(data.shape, F32)
    devices = gx * gy
    for k, (dx, dy) in enumerate(TRAVEL):
        piece = data
        shift = (-(gy * dx + dy)) % devices
        if shift:
            piece = pltpu.roll(piece, shift, axis=0)
        if k:
            piece = pltpu.roll(piece, 128 - 12 * k, axis=1)
        total = total + piece
    linear = pltpu.roll(data, 128 - 108, axis=1)
    moved[...] = linear - (RESPONSE / per_sphere) * total
    lane = lax.broadcasted_iota(I32, (1, 128), 1)
    mine = moved[pl.ds(here, 1), :]
    spring = jnp.zeros((1, 128), F32)
    for k in range(contact_own.shape[0]):
        partner = contact_other[k]
        line = moved[pl.ds(lax.shift_right_logical(partner, 1), 1), :]
        local = contact_own[k] - here * 2
        which = partner & 1
        same = jnp.where(which == local, line, 0.0)
        higher = jnp.where(which < local, pltpu.roll(line, 6, axis=1), 0.0)
        lower = jnp.where(which > local, pltpu.roll(line, 122, axis=1), 0.0)
        of_own = jnp.logical_and(lane >= local * 6, lane < local * 6 + 3)
        spring = spring + jnp.where(of_own, same + higher + lower - mine, 0.0)
    result = mine + DASHPOT * spring
    out[0:1, :] = result[:, 0:6] + angular[0:1, :]
    out[1:2, :] = pltpu.roll(result, 122, axis=1)[:, 0:6] + angular[1:2, :]


def edges_kernel(where, part, got_a, got_b, to_a, to_b, *, tall):
    nx = part.shape[0]
    even = (where[0] & 1) == 0
    even_y = (where[1] & 1) == 0
    for x in range(nx + 4):
        for c in range(3):
            values = []
            for at in (c * tall, (c + 1) * tall - 6):
                rows = pl.ds(at, 6)
                pieces = []
                if 2 <= x < nx + 2:
                    pieces.append(part[x - 2, rows, :])
                if x < 6:
                    slab = pl.ds(x * 3 * tall + at, 6)
                    pieces.append(jnp.where(even, got_b[slab, :], got_a[slab, :]))
                if x >= nx - 2:
                    slab = pl.ds((x - (nx - 2)) * 3 * tall + at, 6)
                    pieces.append(jnp.where(even, got_a[slab, :], got_b[slab, :]))
                total = pieces[0]
                for piece in pieces[1:]:
                    total = total + piece
                values.append(total)
            to = pl.ds(x * 18 + c * 6, 6)
            to_a[to, :] = jnp.where(even_y, values[1], values[0])
            to_b[to, :] = jnp.where(even_y, values[0], values[1])


def middle_kernel(where, part, got_a, got_b, rhs, *, tall):
    nx = part.shape[0]
    long = nx + 4
    high_y = tall + 4
    even = (where[0] & 1) == 0
    zero2 = jnp.zeros((2, 256), F32)

    def fill(x, sources):
        for c in range(3):
            rows_of = pl.ds(c * tall, tall)
            total = sources[0](rows_of)
            for source in sources[1:]:
                total = total + source(rows_of)
            rhs[c, x, 0:2, :] = zero2
            rhs[c, x, high_y - 2 : high_y, :] = zero2
            rhs[c, x, 2 : 2 + tall, :] = total

    def from_part(at):
        return lambda rows_of: part[at, rows_of, :]

    def chosen(at, first, second):
        def source(rows_of):
            slab = pl.ds(at * 3 * tall + rows_of.start, tall)
            return jnp.where(even, first[slab, :], second[slab, :])

        return source

    for x in range(6):
        fill(x, [chosen(x, got_b, got_a)] + ([from_part(x - 2)] if x >= 2 else []))
        fill(
            long - 6 + x,
            [chosen(x, got_a, got_b)] + ([from_part(nx - 4 + x)] if x < 4 else []),
        )

    def centre(x, carry):
        fill(x, [from_part(x - 2)])
        return carry

    lax.fori_loop(6, long - 6, centre, 0)


def relax_kernel(where, grown, got_a, got_b, out_h, rhs, va, vb, low, high, out, sems, *, rows):
    long, high_y = grown.shape[1:3]
    span = high_y - 8
    nx = long - 8
    sort_out(where[1], got_b, got_a, low, high)
    y_at = lax.broadcasted_iota(I32, (high_y, 1), 0) - 4 + where[1] * span
    inside = jnp.logical_and(y_at >= 0, y_at < rows)
    mask = jnp.broadcast_to(inside.astype(F32), (high_y, 256))
    factor = jnp.broadcast_to(
        jnp.where(inside, 1.0 / (1.0 + 6.0 * DIFFUSION), 0.0), (high_y, 256)
    )
    gap = jnp.zeros((high_y - 12, 256), F32)
    for x in range(long):
        for c in range(3):
            at = pl.ds(x * 18 + c * 6, 6)
            edge = jnp.concatenate([low[at, :], gap, high[at, :]], axis=0)
            rhs[c, x] = (grown[c, x] + edge) * mask

    state = rhs
    for sweep in range(ITERS):
        target = (va, vb)[sweep % 2]
        last = sweep == ITERS - 1
        size = UNROLLS[sweep]

        def layer(x, state=state, target=target, last=last):
            for c in range(3):
                here = state[c, x]
                near = state[c, x - 1] + state[c, x + 1]
                near = near + (pltpu.roll(here, 1, axis=1) + pltpu.roll(here, 255, axis=1))
                near = near + (pltpu.roll(here, 1, axis=0) + pltpu.roll(here, high_y - 1, axis=0))
                new = (rhs[c, x] + DIFFUSION * near) * factor
                if last:
                    out[c, x - 4] = new[4 : high_y - 4]
                else:
                    target[c, x] = new

        def group(g, carry, sweep=sweep, layer=layer, last=last, size=size):
            for k in range(size):
                layer(jnp.minimum(sweep + 1 + g * size + k, long - 2 - sweep))
            if last:
                for c in range(3):
                    part = pl.ds(g * UNROLL, UNROLL)
                    pltpu.make_async_copy(out.at[c, part], out_h.at[c, part], sems.at[g * 3 + c]).start()
            return carry

        lax.fori_loop(0, (long - 2 - 2 * sweep + size - 1) // size, group, 0)
        state = target
    for g in range(nx // UNROLL):
        for c in range(3):
            part = pl.ds(g * UNROLL, UNROLL)
            pltpu.make_async_copy(out.at[c, part], out_h.at[c, part], sems.at[g * 3 + c]).wait()


def on_device(
    velocity,
    owner_block,
    base_x,
    base_y,
    base_z,
    delta_weights,
    marker_offset,
    sphere_motion,
    contact_sphere,
    contact_partner,
):
    nx, ny, nz = velocity.shape[1:]
    gx = lax.axis_size("gx")
    gy = lax.axis_size("gy")
    where = jnp.stack([lax.axis_index("gx"), lax.axis_index("gy")]).astype(I32)
    markers = base_x.shape[0]
    spheres = sphere_motion.shape[1]
    per_sphere = markers // spheres
    blocks = markers // TILE
    tall = ny + 4

    def pairs(size, first, wrap):
        both_ways = []
        for i in range(first, size, 2):
            j = (i + 1) % size
            if j or wrap:
                both_ways += [(i, j), (j, i)]
        return both_ways

    def swap_x(first, second):
        return (
            lax.ppermute(first, "gx", pairs(gx, 0, True)),
            lax.ppermute(second, "gx", pairs(gx, 1, True)),
        )

    def swap_y(first, second):
        return (
            lax.ppermute(first, "gy", pairs(gy, 0, False)),
            lax.ppermute(second, "gy", pairs(gy, 1, False)),
        )


    def array(*shape, dtype=F32):
        return jax.ShapeDtypeStruct(shape, dtype)

    x_rows = 6 * ny + 3 * ROWS
    y_rows = 6 * (nx + 4) + 3 * ROWS
    to_a, to_b, middle, own_down, own_up, slot, both, linear, vel = pl.pallas_call(
        functools.partial(route_kernel, gx=gx, gy_shift=gy.bit_length() - 1),
        out_shape=(
            array(x_rows, nz),
            array(x_rows, nz),
            array(2, ROWS, TILE),
            array(y_rows, nz),
            array(y_rows, nz),
            array(1, markers, dtype=I32),
            array(2 * ROWS, markers, dtype=BF16),
            array(1, 128),
            array(3, nx, ny, nz),
        ),
        in_specs=[SMEM] + [HBM] * 8,
        out_specs=(VMEM,) * 9,
        scratch_shapes=[
            pltpu.SMEM((spheres, 6), F32),
            pltpu.VMEM((1, markers), I32),
            pltpu.VMEM((1, markers), I32),
            pltpu.VMEM((1, markers), I32),
            pltpu.VMEM((1, markers), I32),
            pltpu.VMEM((12, markers), F32),
            pltpu.VMEM((3, markers), F32),
            pltpu.VMEM((ROWS, markers), F32),
            pltpu.SemaphoreType.DMA((7,)),
            pltpu.SemaphoreType.DMA((1,)),
        ],
        compiler_params=params(16),
        name="route",
    )(
        where,
        *(
            pltpu.with_memory_space_constraint(a, pltpu.HBM)
            for a in (
                sphere_motion.T,
                owner_block.reshape(1, markers),
                base_x.reshape(1, markers),
                base_y.reshape(1, markers),
                base_z.reshape(1, markers),
                delta_weights,
                marker_offset,
                velocity,
            )
        ),
    )
    got_xa, got_xb = swap_x(to_a, to_b)
    field = array(nx + 4, CYR, nz)
    halved = array(nx + 4, CYR, 2 * nz, dtype=BF16)
    lists = array(blocks, ROWS, TILE)
    tile_scratch = [
        pltpu.VMEM((2 * nz, TILE), BF16),
        pltpu.VMEM((nz, 2 * TILE), BF16),
        pltpu.VMEM((CYR, TILE), F32),
    ]
    inner, rim, part, fcat, sums = pl.pallas_call(
        home_kernel,
        out_shape=(lists, lists, field, halved, array(128, 128)),
        in_specs=[VMEM] * 3,
        out_specs=(VMEM,) * 5,
        scratch_shapes=tile_scratch,
        compiler_params=params(8),
        cost_estimate=pl.CostEstimate(flops=2_000_000_000, bytes_accessed=0, transcendentals=0),
        name="home",
    )(slot, both, vel)
    part, sums = pl.pallas_call(
        functools.partial(inner_kernel, tall=tall),
        out_shape=(field, array(128, 128)),
        in_specs=[VMEM] * 4,
        out_specs=(VMEM,) * 2,
        input_output_aliases={2: 0, 3: 1},
        scratch_shapes=tile_scratch,
        compiler_params=params(8),
        cost_estimate=pl.CostEstimate(flops=4_000_000_000, bytes_accessed=0, transcendentals=0),
        name="inner",
    )(inner, fcat, part, sums)
    x_buffer = pltpu.VMEM((x_rows, nz), F32)
    y_buffer = pltpu.VMEM((y_rows, nz), F32)
    got_ya, got_yb = swap_y(
        *pl.pallas_call(
            functools.partial(turn_kernel, nx=nx, ny=ny),
            out_shape=(array(y_rows, nz),) * 2,
            in_specs=[SMEM] + [VMEM] * 5,
            out_specs=(VMEM,) * 2,
            scratch_shapes=[x_buffer, x_buffer, y_buffer, y_buffer],
            compiler_params=params(4),
            name="turn",
        )(where, got_xa, got_xb, middle, own_down, own_up)
    )

    devices = gx * gy
    slab = array(6 * 3 * tall, nz)
    part, send_a, send_b, message = pl.pallas_call(
        couple_kernel,
        out_shape=(field, slab, slab, array(devices, 128)),
        in_specs=[SMEM] + [VMEM] * 9,
        out_specs=(VMEM,) * 4,
        input_output_aliases={9: 0},
        scratch_shapes=[
            x_buffer,
            x_buffer,
            y_buffer,
            y_buffer,
            pltpu.VMEM(field.shape, F32),
            pltpu.VMEM(halved.shape, BF16),
            pltpu.VMEM((2 * blocks, ROWS, TILE), F32),
            pltpu.VMEM((ROWS, 2 * markers), F32),
            *tile_scratch,
            pltpu.VMEM((128, 128), F32),
        ],
        compiler_params=params(16),
        name="couple",
    )(where, vel, got_xa, got_xb, got_ya, got_yb, rim, linear, sums, part)

    got_a, got_b = swap_x(send_a, send_b)
    everyone = lax.all_to_all(message, ("gx", "gy"), 0, 0, tiled=True)
    strip = array((nx + 8) * 18, nz)
    everyone, part = lax.optimization_barrier((everyone, part))
    strip_buffer = pltpu.VMEM(strip.shape, F32)
    to_ya, to_yb = pl.pallas_call(
        functools.partial(edges_kernel, tall=tall),
        out_shape=(strip, strip),
        in_specs=[SMEM] + [VMEM] * 3,
        out_specs=(VMEM,) * 2,
        compiler_params=params(4),
        name="edges",
    )(where, part, got_a, got_b)
    angular = jnp.concatenate([jnp.zeros((3, spheres), F32), sphere_motion[3:6]], axis=0).T
    new_motion = pl.pallas_call(
        functools.partial(motion_kernel, gx=gx, gy=gy, per_sphere=per_sphere),
        out_shape=array(spheres, 6),
        in_specs=[SMEM] * 3 + [VMEM] * 2,
        out_specs=VMEM,
        scratch_shapes=[pltpu.VMEM((devices, 128), F32)],
        compiler_params=params(4),
        name="motion",
    )(where, contact_sphere, contact_partner, angular, everyone).T
    got_ea, got_eb = swap_y(to_ya, to_yb)
    grown = pl.pallas_call(
        functools.partial(middle_kernel, tall=tall),
        out_shape=array(3, nx + 8, tall + 4, nz),
        in_specs=[SMEM] + [VMEM] * 3,
        out_specs=VMEM,
        compiler_params=params(4),
        cost_estimate=pl.CostEstimate(flops=2_000_000_000, bytes_accessed=0, transcendentals=0),
        name="middle",
    )(where, part, got_a, got_b)
    buffer = pltpu.VMEM(grown.shape, F32)
    state = pl.pallas_call(
        functools.partial(relax_kernel, rows=ny * gy),
        out_shape=array(3, nx, ny, nz),
        in_specs=[SMEM] + [VMEM] * 3,
        out_specs=HBM,
        scratch_shapes=[
            buffer,
            buffer,
            buffer,
            strip_buffer,
            strip_buffer,
            pltpu.VMEM((3, nx, ny, nz), F32),
            pltpu.SemaphoreType.DMA((3 * (nx // UNROLL),)),
        ],
        compiler_params=params(20),
        name="relax",
    )(where, grown, got_ea, got_eb)
    return (state, new_motion)


def solution(mesh):
    placed = (
        P(None, "gx", "gy", None),
        P(("gx", "gy"), None),
        P(("gx", "gy")),
        P(("gx", "gy")),
        P(("gx", "gy")),
        P(None, ("gx", "gy")),
        P(None, ("gx", "gy")),
        P(None, ("gx", "gy")),
        P(("gx", "gy")),
        P(("gx", "gy")),
    )
    return jax.shard_map(
        on_device,
        mesh=mesh,
        in_specs=placed,
        out_specs=(P(None, "gx", "gy", None), P(None, ("gx", "gy"))),
        check_vma=False,
    )
```

```python
import functools

import jax
import jax.numpy as jnp
from jax import lax
from jax.experimental import pallas as pl
from jax.experimental.pallas import tpu as pltpu
from jax.sharding import PartitionSpec as P

F32 = jnp.float32
BF16 = jnp.bfloat16
I32 = jnp.int32

ITERS = 4
DIFFUSION = 1.0
RESPONSE = 0.5
DASHPOT = 0.1

ROWS = 24
TILE = 256
UNROLLS = (11, 10, 9, 4)
UNROLL = UNROLLS[-1]
EARLY = 2
SIZES = (6, 7, 8, 9)
WIN = 10
CYR = 112


TRAVEL = ((0, 0), (-1, 0), (1, 0), (-1, -1), (0, -1), (1, -1), (-1, 1), (0, 1), (1, 1))

VMEM = pl.BlockSpec(memory_space=pltpu.VMEM)
SMEM = pl.BlockSpec(memory_space=pltpu.SMEM)
HBM = pl.BlockSpec(memory_space=pltpu.HBM)


def params(mib):
    return pltpu.CompilerParams(vmem_limit_bytes=mib * 1024 * 1024)


def split(value):
    high = value.astype(BF16)
    low = (value - high.astype(F32)).astype(BF16)
    return high, low


def counting_ranks(bin_of, start_of, bins_here):
    markers = bin_of.shape[1]
    bins = (lax.broadcasted_iota(I32, (32, markers), 0) == bin_of).astype(F32)
    bins16 = bins.astype(BF16)
    ramp_i = lax.broadcasted_iota(I32, (TILE, TILE), 0)
    ramp_j = lax.broadcasted_iota(I32, (TILE, TILE), 1)
    upper = (ramp_i < ramp_j).astype(F32).astype(BF16)
    totals = lax.dot_general(
        jnp.ones((8, markers), BF16), bins16, (((1,), (1,)), ((), ())), preferred_element_type=F32
    )
    row = lax.broadcasted_iota(I32, (32, 32), 0)
    col = lax.broadcasted_iota(I32, (32, 32), 1)
    before = jnp.where(jnp.logical_and(col < row, row < bins_here), totals[0:1, :], 0.0)
    bin_row = lax.broadcasted_iota(I32, (32, 1), 0)
    start = jnp.where(
        bin_row < bins_here, jnp.sum(before, axis=1, keepdims=True), start_of(bin_row).astype(F32)
    )
    slots = []
    for b in range(markers // TILE):
        mine = bins[:, b * TILE : (b + 1) * TILE]
        ranks = jnp.dot(bins16[:, b * TILE : (b + 1) * TILE], upper, preferred_element_type=F32)
        slots.append(jnp.sum(mine * (ranks + start), axis=0, keepdims=True))
        start = start + jnp.sum(mine, axis=1, keepdims=True)
    return jnp.concatenate(slots, axis=1).astype(I32)


def gather_tile(both, slot, tile):
    place = lax.broadcasted_iota(I32, (TILE, slot.shape[1]), 0).astype(F32).astype(BF16)
    local = jnp.clip(slot - tile * TILE, -1, TILE).astype(F32).astype(BF16)
    pick = jnp.where(place == local, jnp.ones((), BF16), jnp.zeros((), BF16))
    out = lax.dot_general(both, pick, (((1,), (1,)), ((), ())), preferred_element_type=F32)
    return out[0:ROWS] + out[ROWS : 2 * ROWS]


def sort_out(index, first, second, out_first, out_second):
    even = (index & 1) == 0
    out_first[...] = jnp.where(even, first[...], second[...])
    out_second[...] = jnp.where(even, second[...], first[...])


def halves(value):
    high, low = split(value)
    return jnp.concatenate([high.astype(F32), low.astype(F32)], axis=0).astype(BF16)


def route_kernel(
    where, motion_h, owner_h, bx_h, by_h, bz_h, weights_h, offset_h, velocity_h,
    to_a, to_b, middle, to_down, to_up, slot_out, both_out, linear, vel,
    motion, owner, bx, by, bz, weights, offset, rec, sems, edge_sem, *, gx, gy_shift
):
    markers = owner.shape[1]
    blocks = markers // TILE
    nx, ny = vel.shape[1:3]
    moves = []
    for k, (src, dst) in enumerate(
        (
            (owner_h, owner),
            (bx_h, bx),
            (by_h, by),
            (bz_h, bz),
            (weights_h, weights),
            (offset_h, offset),
            (motion_h, motion),
        )
    ):
        move = pltpu.make_async_copy(src, dst, sems.at[k])
        move.start()
        moves.append(move)
    whole = pltpu.make_async_copy(velocity_h, vel, edge_sem.at[0])
    whole.start()
    for move in moves:
        move.wait()
    own = owner[...]
    step_x = (lax.shift_right_logical(own, gy_shift) - where[0] + 1) & (gx - 1)
    step_y = (own & ((1 << gy_shift) - 1)) - where[1] + 1
    lane = step_x * 3 + step_y
    x_in = jnp.logical_and(bx[...] >= 2, bx[...] <= nx - 2)
    y_in = jnp.logical_and(by[...] >= 2, by[...] <= ny - 2)
    at_home = jnp.where(jnp.logical_and(x_in, y_in), bx[...], 17)
    bin_of = jnp.where(lane == 4, at_home, 18 + lane)
    slot = counting_ranks(
        bin_of, lambda b: jnp.where(b == 17, markers, 2 * markers + (b - 18) * TILE), 17
    )
    slot_out[...] = slot

    first = lax.broadcasted_iota(I32, (1, markers), 1) < markers // 2
    speed = [jnp.where(first, motion[0, c], motion[1, c]) for c in range(6)]
    off = [offset[c : c + 1, :] for c in range(3)]
    target = [
        speed[0] + (speed[4] * off[2] - speed[5] * off[1]),
        speed[1] + (speed[5] * off[0] - speed[3] * off[2]),
        speed[2] + (speed[3] * off[1] - speed[4] * off[0]),
    ]
    rec[0:12, :] = weights[...]
    rec[12:13, :] = bx[...].astype(F32)
    rec[13:14, :] = by[...].astype(F32)
    rec[14:15, :] = bz[...].astype(F32)
    for c in range(3):
        rec[15 + c : 16 + c, :] = target[c]
    rec[18:21, :] = offset[...]
    rec[21:22, :] = jnp.where(first, 0.0, 1.0)
    rec[22:23, :] = jnp.ones((1, markers), F32)
    rec[23:24, :] = jnp.zeros((1, markers), F32)
    both = halves(rec[...])
    both_out[...] = both
    base = 6 * ny
    even = (where[0] & 1) == 0
    for ref, up in ((to_a, even), (to_b, jnp.logical_not(even))):
        tile = 2 * blocks + jnp.where(up, 6, 0)
        for k in range(3):
            ref[base + k * ROWS : base + (k + 1) * ROWS, :] = gather_tile(both, slot, tile + k)
    middle[0] = gather_tile(both, slot, 2 * blocks + 3)
    middle[1] = gather_tile(both, slot, 2 * blocks + 5)

    lane_row = lax.broadcasted_iota(I32, (1, 128), 1)
    line = jnp.zeros((1, 128), F32)
    for s in range(2):
        for c in range(3):
            line = jnp.where(lane_row == 108 + 6 * s + c, motion[s, c], line)
    linear[...] = line
    whole.wait()
    for c in range(3):
        for x in range(2):
            rows = pl.ds((c * 2 + x) * ny, ny)
            to_a[rows, :] = vel[c, jnp.where(even, nx - 2, 0) + x]
            to_b[rows, :] = vel[c, jnp.where(even, 0, nx - 2) + x]

    for x in range(nx):
        for c in range(3):
            at = (x + 2) * 6 + c * 2
            to_down[at : at + 2, :] = vel[c, x, 0:2, :]
            to_up[at : at + 2, :] = vel[c, x, ny - 2 : ny, :]


def home_kernel(slot, both, vel, inner, rim, part, fcat, sums, tn, tt, sacc):
    markers = slot.shape[1]
    blocks = inner.shape[0]
    below = (slot[...] < markers).astype(F32)
    upto = (slot[...] < 2 * markers).astype(F32)
    count_inner = jnp.sum(below).astype(I32)
    count_rim = jnp.sum(upto - below).astype(I32)
    for t in range(blocks):
        inner[t] = jnp.zeros((ROWS, TILE), F32)
        rim[t] = jnp.zeros((ROWS, TILE), F32)

    def inner_tile(t, carry):
        inner[t] = gather_tile(both[...], slot[...], t)
        return carry

    def rim_tile(t, carry):
        rim[t] = gather_tile(both[...], slot[...], blocks + t)
        return carry

    lax.fori_loop(0, (count_inner + TILE - 1) // TILE, inner_tile, 0)
    lax.fori_loop(0, (count_rim + TILE - 1) // TILE, rim_tile, 0)

    nx = part.shape[0]
    cells = vel.shape[2]
    tall = cells + 4
    blank = jnp.zeros(part.shape[1:], F32)
    for x in range(nx):
        part[x] = blank
    fill_own(vel, part)

    def halve(x, carry):
        to_halves(part, fcat, x)
        return carry

    lax.fori_loop(0, nx, halve, 0, unroll=5)
    sums[...] = jnp.zeros(sums.shape, F32)
    process_tiles(0, EARLY, inner, fcat, part, sums, tn, tt, sacc, tall=tall)


def fill_own(vel, field):
    cells = vel.shape[2]

    def layer(x, carry):
        for c in range(3):
            field[x + 2, c * (cells + 4) + 2 : c * (cells + 4) + 2 + cells, :] = vel[c, x]
        return carry

    lax.fori_loop(0, vel.shape[1], layer, 0, unroll=4)


def to_halves(field, fcat, x):
    high, low = split(field[x])
    fcat[x, :, 0:256] = high
    fcat[x, :, 256:512] = low


def turn_kernel(
    where, got_a, got_b, middle, own_down, own_up, to_a, to_b, got_left, got_right, down, up, *, nx, ny
):
    sort_out(where[0], got_a, got_b, got_left, got_right)
    base = 6 * ny
    lists = (nx + 4) * 6
    for out, own, cut, pick, mid in (
        (down, own_down, 0, 0, 0),
        (up, own_up, ny - 2, 2, 1),
    ):
        out[0:lists, :] = own[0:lists, :]
        for x in range(2):
            for c in range(3):
                at = (c * 2 + x) * ny + cut
                to = x * 6 + c * 2
                out[to : to + 2, :] = got_right[at : at + 2, :]
                to = (nx + 2 + x) * 6 + c * 2
                out[to : to + 2, :] = got_left[at : at + 2, :]
        out[lists : lists + ROWS, :] = got_left[base + pick * ROWS : base + (pick + 1) * ROWS, :]
        out[lists + ROWS : lists + 2 * ROWS, :] = middle[mid]
        out[lists + 2 * ROWS : lists + 3 * ROWS, :] = (
            got_right[base + pick * ROWS : base + (pick + 1) * ROWS, :]
        )
    sort_out(where[1], up, down, to_a, to_b)


def chain(distance, rows):
    value = jnp.where(distance == 3, rows[3], jnp.zeros((), rows[3].dtype))
    for k in (2, 1, 0):
        value = jnp.where(distance == k, rows[k], value)
    return value


def process_tiles(first_tile, stop, lists, fcat, part, sums, tn, tt, sacc, *, tall):
    nx = part.shape[0]
    row = lax.broadcasted_iota(I32, (CYR, 1), 0)
    comp = (row >= tall).astype(I32) + (row >= 2 * tall).astype(I32)
    y_of = jnp.where(row < 3 * tall, row - comp * tall, -100)
    comp = jnp.where(row < 3 * tall, comp, 3)
    z_of = lax.broadcasted_iota(I32, (256, TILE), 0).astype(F32).astype(BF16)
    win_row = lax.broadcasted_iota(I32, (16, TILE), 0)
    group_of = lax.broadcasted_iota(I32, (128, TILE), 0)

    def tile_body(t, carry):
        rec = lists[t]
        valid = rec[22:23] > 0.5
        bxf = rec[12:13]
        x_first = jnp.min(jnp.where(valid, bxf, 99.0)).astype(I32)
        x_last = jnp.max(jnp.where(valid, bxf, -9.0)).astype(I32)
        layers = x_last - x_first + 4
        windows = jnp.where(x_last < 0, 0, (layers + WIN - 1) // WIN)

        @pl.when(windows > 0)
        def _():
            bxi = bxf.astype(I32)
            byi = rec[13:14].astype(I32)
            ahead = z_of - rec[14:15].astype(BF16)
            ahead = jnp.where(ahead < 0, ahead + 256, ahead)
            parts = [split(rec[8 + k : 9 + k]) for k in range(4)]
            high = chain(ahead, [p[0] for p in parts])
            low = chain(ahead, [p[1] for p in parts])
            tn[0:256, :] = high
            tn[256:512, :] = low
            tt[:, 0:256] = high
            tt[:, 256:512] = low
            table_y = chain(y_of - byi, [rec[4 + k : 5 + k] for k in range(4)])
            sacc[...] = jnp.zeros(sacc.shape, F32)

            def window(w, size):
                begin = x_first + w * size
                x0 = jnp.minimum(begin, nx - size)
                x_at = win_row + x0
                table_x = chain(x_at - bxi, [rec[k : k + 1] for k in range(4)])
                return x0, jnp.where(x_at >= begin, table_x, 0.0)

            def sample(w, size):
                x0, table_x = window(w, size)
                block_h = fcat[pl.ds(x0, size), :, 0:256].reshape(size * CYR, 256)
                block_l = fcat[pl.ds(x0, size), :, 256:512].reshape(size * CYR, 256)
                got = (
                    jnp.dot(block_h, tn[0:256], preferred_element_type=F32)
                    + jnp.dot(block_l, tn[0:256], preferred_element_type=F32)
                    + jnp.dot(block_h, tn[256:512], preferred_element_type=F32)
                )
                total = sacc[...]
                for i in range(size):
                    total = total + table_x[i : i + 1] * got[i * CYR : (i + 1) * CYR]
                sacc[...] = total

            def by_size(step):
                for size in SIZES:
                    fits = layers <= size
                    if size > SIZES[0]:
                        fits = jnp.logical_and(fits, layers > size - 1)
                    pl.when(fits)(functools.partial(step, 0, size))

                @pl.when(layers > SIZES[-1])
                def _():
                    def loop(w, c):
                        step(w, WIN)
                        return c

                    lax.fori_loop(0, windows, loop, 0)

            by_size(sample)
            weighted = sacc[...] * table_y
            force = [
                rec[15 + c : 16 + c]
                - jnp.sum(jnp.where(comp == c, weighted, 0.0), axis=0, keepdims=True)
                for c in range(3)
            ]
            by_row = jnp.where(comp == 0, force[0], jnp.where(comp == 1, force[1], force[2]))
            plane = table_y * by_row

            def deposit(w, size):
                x0, table_x = window(w, size)
                pieces = [split(table_x[i : i + 1] * plane) for i in range(size)]
                high_s = jnp.concatenate([p[0] for p in pieces], axis=0)
                low_s = jnp.concatenate([p[1] for p in pieces], axis=0)
                nt = (((1,), (1,)), ((), ()))
                made = (
                    lax.dot_general(high_s, tt[:, 0:256], nt, preferred_element_type=F32)
                    + lax.dot_general(low_s, tt[:, 0:256], nt, preferred_element_type=F32)
                    + lax.dot_general(high_s, tt[:, 256:512], nt, preferred_element_type=F32)
                )
                part[pl.ds(x0, size)] += made.reshape(size, CYR, 256)

            by_size(deposit)
            off = [rec[18 + c : 19 + c] for c in range(3)]
            turn = [
                off[1] * force[2] - off[2] * force[1],
                off[2] * force[0] - off[0] * force[2],
                off[0] * force[1] - off[1] * force[0],
            ]
            stack = jnp.concatenate(force + turn + [jnp.zeros((2, TILE), F32)], axis=0)
            group = (2.0 * rec[23:24] + rec[21:22]).astype(I32)
            member = (group_of == group).astype(F32).astype(BF16)
            found = lax.dot_general(
                member, halves(stack), (((1,), (1,)), ((), ())), preferred_element_type=F32
            )
            sums[:, 0:16] += found

        return carry

    lax.fori_loop(first_tile, stop, tile_body, 0)


def inner_kernel(lists, fcat, part_in, sums_in, part, sums, tn, tt, sacc, *, tall):
    del part_in
    del sums_in
    process_tiles(EARLY, lists.shape[0], lists, fcat, part, sums, tn, tt, sacc, tall=tall)


def couple_kernel(
    where, vel, got_xa, got_xb, got_ya, got_yb, rim, linear, sums_in, part_in,
    part, send_a, send_b, message,
    got_left, got_right, got_down, got_up, field, fcat, lists, arrived, tn, tt, sacc, sums,
):
    del part_in
    nx = vel.shape[1] + 4
    cells = vel.shape[2]
    tall = cells + 4
    sort_out(where[0], got_xa, got_xb, got_left, got_right)
    sort_out(where[1], got_ya, got_yb, got_down, got_up)
    zero_pad = jnp.zeros((CYR - 3 * tall, vel.shape[3]), F32)
    fill_own(vel, field)
    for x in range(2):
        for c in range(3):
            rows = pl.ds((c * 2 + x) * cells, cells)
            field[x, c * tall + 2 : c * tall + 2 + cells, :] = got_right[rows, :]
            field[nx - 2 + x, c * tall + 2 : c * tall + 2 + cells, :] = got_left[rows, :]
    for x in range(nx):
        for c in range(3):
            rows = pl.ds(x * 6 + c * 2, 2)
            field[x, c * tall : c * tall + 2, :] = got_up[rows, :]
            field[x, c * tall + 2 + cells : (c + 1) * tall, :] = got_down[rows, :]
        field[x, 3 * tall : CYR, :] = zero_pad

    def halve(x, carry):
        to_halves(field, fcat, x)
        return carry

    lax.fori_loop(0, nx, halve, 0, unroll=5)

    base = 6 * cells + ROWS
    after = nx * 6
    blocks = rim.shape[0]
    arrived[:, 0:TILE] = got_left[base : base + ROWS, :]
    arrived[:, TILE : 2 * TILE] = got_right[base : base + ROWS, :]
    for k in range(3):
        rows = pl.ds(after + k * ROWS, ROWS)
        arrived[:, (2 + k) * TILE : (3 + k) * TILE] = got_down[rows, :]
        arrived[:, (5 + k) * TILE : (6 + k) * TILE] = got_up[rows, :]
    for t in range(blocks):
        arrived[:, (8 + t) * TILE : (9 + t) * TILE] = rim[t]
    total_lanes = arrived.shape[1]
    lane_at = lax.broadcasted_iota(I32, (1, total_lanes), 1)
    list_at = 1 + lax.shift_right_logical(lane_at, TILE.bit_length() - 1)
    arrived[23:24, :] = jnp.where(list_at > 8, 0, list_at).astype(F32)
    valid_all = arrived[22:23, :] > 0.5
    count = jnp.sum(arrived[22:23, :]).astype(I32)
    used = 8 + (jnp.sum(arrived[22:23, 8 * TILE : total_lanes]).astype(I32) + TILE - 1) // TILE
    bin_all = jnp.where(valid_all, arrived[12:13, :].astype(I32), 17)
    slot = counting_ranks(bin_all, lambda b: 0 * b + total_lanes, 17)
    both = halves(arrived[...])
    for t in range(lists.shape[0]):
        lists[t] = jnp.zeros((ROWS, TILE), F32)
    tiles = (count + TILE - 1) // TILE

    reach = 0
    for size in (9, 10, 11, 12, 16):
        wanted = jnp.logical_and(used > reach, used <= size)
        reach = size

        def gather_some(t, carry, lanes=size * TILE):
            lists[t] = gather_tile(both[:, 0:lanes], slot[:, 0:lanes], t)
            return carry

        lax.fori_loop(0, jnp.where(wanted, tiles, 0), gather_some, 0)
    sums[...] = sums_in[...]
    process_tiles(0, tiles, lists, fcat, part, sums, tn, tt, sacc, tall=tall)
    lane_of = lax.broadcasted_iota(I32, (128, 128), 1)
    low_part = pltpu.roll(sums[...], 120, axis=1)
    joined = jnp.where(lane_of < 6, sums[...] + low_part, 0.0)
    line = linear[...] + joined[0:1]
    for k in range(1, 18):
        line = line + pltpu.roll(joined[k : k + 1], 6 * k, axis=1)
    message[...] = jnp.broadcast_to(line, message.shape)
    even = (where[0] & 1) == 0
    for x in range(6):
        rows = pl.ds(x * 3 * tall, 3 * tall)
        send_a[rows, :] = part[jnp.where(even, nx - 6, 0) + x, 0 : 3 * tall, :]
        send_b[rows, :] = part[jnp.where(even, 0, nx - 6) + x, 0 : 3 * tall, :]


def motion_kernel(
    where, contact_own, contact_other, angular, got, out, moved, *, gx, gy, per_sphere
):
    here = where[0] * gy + where[1]
    data = got[...]
    total = jnp.zeros(data.shape, F32)
    devices = gx * gy
    for k, (dx, dy) in enumerate(TRAVEL):
        piece = data
        shift = (-(gy * dx + dy)) % devices
        if shift:
            piece = pltpu.roll(piece, shift, axis=0)
        if k:
            piece = pltpu.roll(piece, 128 - 12 * k, axis=1)
        total = total + piece
    linear = pltpu.roll(data, 128 - 108, axis=1)
    moved[...] = linear - (RESPONSE / per_sphere) * total
    lane = lax.broadcasted_iota(I32, (1, 128), 1)
    mine = moved[pl.ds(here, 1), :]
    spring = jnp.zeros((1, 128), F32)
    for k in range(contact_own.shape[0]):
        partner = contact_other[k]
        line = moved[pl.ds(lax.shift_right_logical(partner, 1), 1), :]
        local = contact_own[k] - here * 2
        which = partner & 1
        same = jnp.where(which == local, line, 0.0)
        higher = jnp.where(which < local, pltpu.roll(line, 6, axis=1), 0.0)
        lower = jnp.where(which > local, pltpu.roll(line, 122, axis=1), 0.0)
        of_own = jnp.logical_and(lane >= local * 6, lane < local * 6 + 3)
        spring = spring + jnp.where(of_own, same + higher + lower - mine, 0.0)
    result = mine + DASHPOT * spring
    out[0:1, :] = result[:, 0:6] + angular[0:1, :]
    out[1:2, :] = pltpu.roll(result, 122, axis=1)[:, 0:6] + angular[1:2, :]


def edges_kernel(where, part, got_a, got_b, to_a, to_b, *, tall):
    nx = part.shape[0]
    even = (where[0] & 1) == 0
    even_y = (where[1] & 1) == 0
    for x in range(nx + 4):
        for c in range(3):
            values = []
            for at in (c * tall, (c + 1) * tall - 6):
                rows = pl.ds(at, 6)
                pieces = []
                if 2 <= x < nx + 2:
                    pieces.append(part[x - 2, rows, :])
                if x < 6:
                    slab = pl.ds(x * 3 * tall + at, 6)
                    pieces.append(jnp.where(even, got_b[slab, :], got_a[slab, :]))
                if x >= nx - 2:
                    slab = pl.ds((x - (nx - 2)) * 3 * tall + at, 6)
                    pieces.append(jnp.where(even, got_a[slab, :], got_b[slab, :]))
                total = pieces[0]
                for piece in pieces[1:]:
                    total = total + piece
                values.append(total)
            to = pl.ds(x * 18 + c * 6, 6)
            to_a[to, :] = jnp.where(even_y, values[1], values[0])
            to_b[to, :] = jnp.where(even_y, values[0], values[1])


def middle_kernel(where, part, got_a, got_b, rhs, *, tall):
    nx = part.shape[0]
    long = nx + 4
    high_y = tall + 4
    even = (where[0] & 1) == 0
    zero2 = jnp.zeros((2, 256), F32)

    def fill(x, sources):
        for c in range(3):
            rows_of = pl.ds(c * tall, tall)
            total = sources[0](rows_of)
            for source in sources[1:]:
                total = total + source(rows_of)
            rhs[c, x, 0:2, :] = zero2
            rhs[c, x, high_y - 2 : high_y, :] = zero2
            rhs[c, x, 2 : 2 + tall, :] = total

    def from_part(at):
        return lambda rows_of: part[at, rows_of, :]

    def chosen(at, first, second):
        def source(rows_of):
            slab = pl.ds(at * 3 * tall + rows_of.start, tall)
            return jnp.where(even, first[slab, :], second[slab, :])

        return source

    for x in range(6):
        fill(x, [chosen(x, got_b, got_a)] + ([from_part(x - 2)] if x >= 2 else []))
        fill(
            long - 6 + x,
            [chosen(x, got_a, got_b)] + ([from_part(nx - 4 + x)] if x < 4 else []),
        )

    def centre(x, carry):
        fill(x, [from_part(x - 2)])
        return carry

    lax.fori_loop(6, long - 6, centre, 0)


def relax_kernel(where, grown, got_a, got_b, out_h, rhs, va, vb, low, high, out, sems, *, rows):
    long, high_y = grown.shape[1:3]
    span = high_y - 8
    nx = long - 8
    sort_out(where[1], got_b, got_a, low, high)
    y_at = lax.broadcasted_iota(I32, (high_y, 1), 0) - 4 + where[1] * span
    inside = jnp.logical_and(y_at >= 0, y_at < rows)
    mask = jnp.broadcast_to(inside.astype(F32), (high_y, 256))
    factor = jnp.broadcast_to(
        jnp.where(inside, 1.0 / (1.0 + 6.0 * DIFFUSION), 0.0), (high_y, 256)
    )
    gap = jnp.zeros((high_y - 12, 256), F32)
    for x in range(long):
        for c in range(3):
            at = pl.ds(x * 18 + c * 6, 6)
            edge = jnp.concatenate([low[at, :], gap, high[at, :]], axis=0)
            rhs[c, x] = (grown[c, x] + edge) * mask

    state = rhs
    for sweep in range(ITERS):
        target = (va, vb)[sweep % 2]
        last = sweep == ITERS - 1
        size = UNROLLS[sweep]

        def layer(x, state=state, target=target, last=last):
            for c in range(3):
                here = state[c, x]
                near = state[c, x - 1] + state[c, x + 1]
                near = near + (pltpu.roll(here, 1, axis=1) + pltpu.roll(here, 255, axis=1))
                near = near + (pltpu.roll(here, 1, axis=0) + pltpu.roll(here, high_y - 1, axis=0))
                new = (rhs[c, x] + DIFFUSION * near) * factor
                if last:
                    out[c, x - 4] = new[4 : high_y - 4]
                else:
                    target[c, x] = new

        def group(g, carry, sweep=sweep, layer=layer, last=last, size=size):
            for k in range(size):
                layer(jnp.minimum(sweep + 1 + g * size + k, long - 2 - sweep))
            if last:
                for c in range(3):
                    part = pl.ds(g * UNROLL, UNROLL)
                    pltpu.make_async_copy(out.at[c, part], out_h.at[c, part], sems.at[g * 3 + c]).start()
            return carry

        lax.fori_loop(0, (long - 2 - 2 * sweep + size - 1) // size, group, 0)
        state = target
    for g in range(nx // UNROLL):
        for c in range(3):
            part = pl.ds(g * UNROLL, UNROLL)
            pltpu.make_async_copy(out.at[c, part], out_h.at[c, part], sems.at[g * 3 + c]).wait()


def on_device(
    velocity,
    owner_block,
    base_x,
    base_y,
    base_z,
    delta_weights,
    marker_offset,
    sphere_motion,
    contact_sphere,
    contact_partner,
):
    nx, ny, nz = velocity.shape[1:]
    gx = lax.axis_size("gx")
    gy = lax.axis_size("gy")
    where = jnp.stack([lax.axis_index("gx"), lax.axis_index("gy")]).astype(I32)
    markers = base_x.shape[0]
    spheres = sphere_motion.shape[1]
    per_sphere = markers // spheres
    blocks = markers // TILE
    tall = ny + 4

    def pairs(size, first, wrap):
        both_ways = []
        for i in range(first, size, 2):
            j = (i + 1) % size
            if j or wrap:
                both_ways += [(i, j), (j, i)]
        return both_ways

    def swap_x(first, second):
        return (
            lax.ppermute(first, "gx", pairs(gx, 0, True)),
            lax.ppermute(second, "gx", pairs(gx, 1, True)),
        )

    def swap_y(first, second):
        return (
            lax.ppermute(first, "gy", pairs(gy, 0, False)),
            lax.ppermute(second, "gy", pairs(gy, 1, False)),
        )


    def array(*shape, dtype=F32):
        return jax.ShapeDtypeStruct(shape, dtype)

    x_rows = 6 * ny + 3 * ROWS
    y_rows = 6 * (nx + 4) + 3 * ROWS
    to_a, to_b, middle, own_down, own_up, slot, both, linear, vel = pl.pallas_call(
        functools.partial(route_kernel, gx=gx, gy_shift=gy.bit_length() - 1),
        out_shape=(
            array(x_rows, nz),
            array(x_rows, nz),
            array(2, ROWS, TILE),
            array(y_rows, nz),
            array(y_rows, nz),
            array(1, markers, dtype=I32),
            array(2 * ROWS, markers, dtype=BF16),
            array(1, 128),
            array(3, nx, ny, nz),
        ),
        in_specs=[SMEM] + [HBM] * 8,
        out_specs=(VMEM,) * 9,
        scratch_shapes=[
            pltpu.SMEM((spheres, 6), F32),
            pltpu.VMEM((1, markers), I32),
            pltpu.VMEM((1, markers), I32),
            pltpu.VMEM((1, markers), I32),
            pltpu.VMEM((1, markers), I32),
            pltpu.VMEM((12, markers), F32),
            pltpu.VMEM((3, markers), F32),
            pltpu.VMEM((ROWS, markers), F32),
            pltpu.SemaphoreType.DMA((7,)),
            pltpu.SemaphoreType.DMA((1,)),
        ],
        compiler_params=params(16),
        name="route",
    )(
        where,
        *(
            pltpu.with_memory_space_constraint(a, pltpu.HBM)
            for a in (
                sphere_motion.T,
                owner_block.reshape(1, markers),
                base_x.reshape(1, markers),
                base_y.reshape(1, markers),
                base_z.reshape(1, markers),
                delta_weights,
                marker_offset,
                velocity,
            )
        ),
    )
    got_xa, got_xb = swap_x(to_a, to_b)
    field = array(nx + 4, CYR, nz)
    halved = array(nx + 4, CYR, 2 * nz, dtype=BF16)
    lists = array(blocks, ROWS, TILE)
    tile_scratch = [
        pltpu.VMEM((2 * nz, TILE), BF16),
        pltpu.VMEM((nz, 2 * TILE), BF16),
        pltpu.VMEM((CYR, TILE), F32),
    ]
    inner, rim, part, fcat, sums = pl.pallas_call(
        home_kernel,
        out_shape=(lists, lists, field, halved, array(128, 128)),
        in_specs=[VMEM] * 3,
        out_specs=(VMEM,) * 5,
        scratch_shapes=tile_scratch,
        compiler_params=params(8),
        cost_estimate=pl.CostEstimate(flops=2_000_000_000, bytes_accessed=0, transcendentals=0),
        name="home",
    )(slot, both, vel)
    part, sums = pl.pallas_call(
        functools.partial(inner_kernel, tall=tall),
        out_shape=(field, array(128, 128)),
        in_specs=[VMEM] * 4,
        out_specs=(VMEM,) * 2,
        input_output_aliases={2: 0, 3: 1},
        scratch_shapes=tile_scratch,
        compiler_params=params(8),
        cost_estimate=pl.CostEstimate(flops=4_000_000_000, bytes_accessed=0, transcendentals=0),
        name="inner",
    )(inner, fcat, part, sums)
    x_buffer = pltpu.VMEM((x_rows, nz), F32)
    y_buffer = pltpu.VMEM((y_rows, nz), F32)
    got_ya, got_yb = swap_y(
        *pl.pallas_call(
            functools.partial(turn_kernel, nx=nx, ny=ny),
            out_shape=(array(y_rows, nz),) * 2,
            in_specs=[SMEM] + [VMEM] * 5,
            out_specs=(VMEM,) * 2,
            scratch_shapes=[x_buffer, x_buffer, y_buffer, y_buffer],
            compiler_params=params(4),
            name="turn",
        )(where, got_xa, got_xb, middle, own_down, own_up)
    )

    devices = gx * gy
    slab = array(6 * 3 * tall, nz)
    part, send_a, send_b, message = pl.pallas_call(
        couple_kernel,
        out_shape=(field, slab, slab, array(devices, 128)),
        in_specs=[SMEM] + [VMEM] * 9,
        out_specs=(VMEM,) * 4,
        input_output_aliases={9: 0},
        scratch_shapes=[
            x_buffer,
            x_buffer,
            y_buffer,
            y_buffer,
            pltpu.VMEM(field.shape, F32),
            pltpu.VMEM(halved.shape, BF16),
            pltpu.VMEM((2 * blocks, ROWS, TILE), F32),
            pltpu.VMEM((ROWS, 2 * markers), F32),
            *tile_scratch,
            pltpu.VMEM((128, 128), F32),
        ],
        compiler_params=params(16),
        name="couple",
    )(where, vel, got_xa, got_xb, got_ya, got_yb, rim, linear, sums, part)

    got_a, got_b = swap_x(send_a, send_b)
    everyone = lax.all_to_all(message, ("gx", "gy"), 0, 0, tiled=True)
    strip = array((nx + 8) * 18, nz)
    everyone, part = lax.optimization_barrier((everyone, part))
    strip_buffer = pltpu.VMEM(strip.shape, F32)
    to_ya, to_yb = pl.pallas_call(
        functools.partial(edges_kernel, tall=tall),
        out_shape=(strip, strip),
        in_specs=[SMEM] + [VMEM] * 3,
        out_specs=(VMEM,) * 2,
        compiler_params=params(4),
        name="edges",
    )(where, part, got_a, got_b)
    angular = jnp.concatenate([jnp.zeros((3, spheres), F32), sphere_motion[3:6]], axis=0).T
    new_motion = pl.pallas_call(
        functools.partial(motion_kernel, gx=gx, gy=gy, per_sphere=per_sphere),
        out_shape=array(spheres, 6),
        in_specs=[SMEM] * 3 + [VMEM] * 2,
        out_specs=VMEM,
        scratch_shapes=[pltpu.VMEM((devices, 128), F32)],
        compiler_params=params(4),
        name="motion",
    )(where, contact_sphere, contact_partner, angular, everyone).T
    got_ea, got_eb = swap_y(to_ya, to_yb)
    grown = pl.pallas_call(
        functools.partial(middle_kernel, tall=tall),
        out_shape=array(3, nx + 8, tall + 4, nz),
        in_specs=[SMEM] + [VMEM] * 3,
        out_specs=VMEM,
        compiler_params=params(4),
        cost_estimate=pl.CostEstimate(flops=2_000_000_000, bytes_accessed=0, transcendentals=0),
        name="middle",
    )(where, part, got_a, got_b)
    buffer = pltpu.VMEM(grown.shape, F32)
    state = pl.pallas_call(
        functools.partial(relax_kernel, rows=ny * gy),
        out_shape=array(3, nx, ny, nz),
        in_specs=[SMEM] + [VMEM] * 3,
        out_specs=HBM,
        scratch_shapes=[
            buffer,
            buffer,
            buffer,
            strip_buffer,
            strip_buffer,
            pltpu.VMEM((3, nx, ny, nz), F32),
            pltpu.SemaphoreType.DMA((3 * (nx // UNROLL),)),
        ],
        compiler_params=params(20),
        name="relax",
    )(where, grown, got_ea, got_eb)
    return (state, new_motion)


def solution(mesh):
    placed = (
        P(None, "gx", "gy", None),
        P(("gx", "gy"), None),
        P(("gx", "gy")),
        P(("gx", "gy")),
        P(("gx", "gy")),
        P(None, ("gx", "gy")),
        P(None, ("gx", "gy")),
        P(None, ("gx", "gy")),
        P(("gx", "gy")),
        P(("gx", "gy")),
    )
    return jax.shard_map(
        on_device,
        mesh=mesh,
        in_specs=placed,
        out_specs=(P(None, "gx", "gy", None), P(None, ("gx", "gy"))),
        check_vma=False,
    )
```
